32 devices in a mesh: gx: 4 (over z), gy: 8 (over y, x, core).
Axes of the slice: x: 2, y: 2, z: 4, core: 2. Of those that a mesh axis runs over, the one named last changes fastest.
Arguments:
- right_side: float32 [512, 2048], P('gx', 'gy'), may hold values from -1.2 to 1.2
- shift: float32 [512, 2048], P('gx', 'gy'), may hold values from 0.0001 to 0.004
Outputs:
- solution: float32 [512, 2048], P('gx', 'gy')
- residual: float32 [512, 2048], P('gx', 'gy')
The draws below stay inside these ranges and needn't reach their ends.
All inputs are finite; a program needn't handle non-finite values.
Results may differ from the reference program's by a relative error of at most 0.0003.
Values sent between devices are 32-bit elements; how exact they have to be, the bound alone decides.
A program may use at most 128 MiB of HBM per device.

```python
import math
import jax
import jax.numpy as jnp

LEVELS = 4
COARSE_SWEEPS = 6
NX = 512
NY = 2048


def draw_right_side(key, part):
    return jnp.clip(0.2 * jax.random.normal(key, (NX, NY), jnp.float32), -1.2, 1.2)


def steps_of(own_key, shape, shards, smallest, largest):
    def one(position, shards_of):
        draws = jax.random.uniform(jax.random.fold_in(jax.random.fold_in(own_key, 6), position), (shards_of,), jnp.float32, smallest / len(shards), largest / len(shards))
        return jnp.repeat(jnp.exp(draws), shape[position] // shards_of).reshape((-1,) + (1,) * (len(shape) - position - 1))

    factor_of = one(*shards[0])
    for cut in shards[1:]:
        factor_of = factor_of * one(*cut)
    return factor_of


def setup_inputs(seed: int = 0) -> dict:
    key_list = jax.random.split(jax.random.key(seed), 3)
    right_side = draw_right_side(jax.random.fold_in(key_list[2], 71), 0)
    shift = jnp.clip(jnp.exp(math.log(0.004) - 3.6888795 * jax.random.uniform(key_list[1], (NX, NY), jnp.float32) ** steps_of(key_list[1], (NX, NY), ((0, 4), (1, 8)), -0.2, 0.2)), 0.0001, 0.004)
    return dict(right_side=right_side, shift=shift)


damping = 0.8


def restrict(values):
    rows, columns = values.shape
    blocks = values.reshape(rows // 2, 2, columns // 2, 2)
    return 0.25 * (blocks[:, 0, :, 0] + blocks[:, 1, :, 0] + blocks[:, 0, :, 1] + blocks[:, 1, :, 1])


def prolong(values):
    rows, columns = values.shape
    copies = jnp.broadcast_to(values[:, None, :, None], (rows, 2, columns, 2))
    return copies.reshape(2 * rows, 2 * columns)


def operate_padded(padded, shifts, level):
    centre = padded[1:-1, 1:-1]
    beside = padded[2:, 1:-1] + padded[:-2, 1:-1] + padded[1:-1, 2:] + padded[1:-1, :-2]
    return 4.0 ** (-level) * (4.0 * centre - beside) + shifts * centre


def apply_operator(field, shifts, level):
    return operate_padded(jnp.pad(field, 1), shifts, level)


def sweeps(iterate, source, shifts, level, count):
    diagonal = 4.0 ** (1 - level) + shifts
    for turn in range(count):
        if iterate is None:
            iterate = damping * source / diagonal
        else:
            iterate = iterate + damping * (source - apply_operator(iterate, shifts, level)) / diagonal
    return iterate


def coarse_solve(iterate, source, shifts):
    unit_total = jnp.sum(apply_operator(jnp.ones_like(source), shifts, LEVELS))
    if iterate is None:
        left = jnp.sum(source)
        iterate = jnp.zeros_like(source) + left / unit_total
    else:
        left = jnp.sum(source - apply_operator(iterate, shifts, LEVELS))
        iterate = iterate + left / unit_total
    return sweeps(iterate, source, shifts, LEVELS, COARSE_SWEEPS)


def vcycle(level, iterate, source, shift_list):
    shifts = shift_list[level]
    if level == LEVELS:
        return coarse_solve(iterate, source, shifts)
    iterate = sweeps(iterate, source, shifts, level, 2)
    coarse_rhs = restrict(source - apply_operator(iterate, shifts, level))
    iterate = iterate + prolong(vcycle(level + 1, None, coarse_rhs, shift_list))
    return sweeps(iterate, source, shifts, level, 2)


def fcycle(level, source, shift_list):
    shifts = shift_list[level]
    if level == LEVELS:
        return coarse_solve(None, source, shifts)
    iterate = sweeps(None, source, shifts, level, 2)
    coarse_rhs = restrict(source - apply_operator(iterate, shifts, level))
    correction = fcycle(level + 1, coarse_rhs, shift_list)
    correction = vcycle(level + 1, correction, coarse_rhs, shift_list)
    iterate = iterate + prolong(correction)
    return sweeps(iterate, source, shifts, level, 2)


def reference(right_side, shift):
    shift_list = [shift]
    for level in range(LEVELS):
        shift_list.append(restrict(shift_list[-1]))
    solution = fcycle(0, right_side, shift_list)
    residual = right_side - apply_operator(solution, shift, 0)
    return solution, residual
```

```python
import functools

import jax
import jax.numpy as jnp
from jax import lax
from jax.experimental import pallas as pl
from jax.experimental.pallas import tpu as pltpu
from jax.sharding import PartitionSpec as P

COARSE_SWEEPS = 6
DAMPING = 0.8
MESH = pl.DeviceIdType.MESH
F32 = jnp.float32
BF16 = jnp.bfloat16

ROWS_PAD = 8
HALO = 8
ROW_HALO = 32


def iota(shape, dim):
    return lax.broadcasted_iota(jnp.int32, shape, dim)


def put_strips(ref, at, values):
    for k in range(ref.shape[0]):
        ref[k, at, :] = values[:, k * 128 : (k + 1) * 128]


def get_strips(ref, at, count=None):
    return jnp.concatenate([ref[k, at, :] for k in range(count or ref.shape[0])], 1)


def exact_dot(values, selector):
    first = values.astype(BF16)
    rest = values - first.astype(F32)
    second = rest.astype(BF16)
    third = (rest - second.astype(F32)).astype(BF16)
    dot = functools.partial(jnp.dot, preferred_element_type=F32)
    return dot(first, selector) + (dot(second, selector) + dot(third, selector))


def kernel(
    gx_count, gy_count, g_hbm, s_hbm, out_ref,
    g_ref, s_ref, load_sem,
    gE, sE, wE, vA, vB, fine_add,
    gP, sP, wP, aP, bP,
    g1, s1, w1, a1, b1, r1,
    send_l, send_r, recv_l, recv_r,
    down0, up0, down1, spread, down_w, up_w,
    rbuf, cbuf, s2, w2, g2, a2, b2, s3, w3, g3, a3, b3, s4, w4, g4, a4, b4, picked,
    s2w, w2w, s3w, w3w,
    halo_send, halo_recv, row_send, row_recv, all_send, all_recv, coarse_sems,
):
    gx, gy = lax.axis_index("gx"), lax.axis_index("gy")
    total = gx_count * gy_count
    me = gx * gy_count + gy
    rows, cols = g_hbm.shape
    base = ROWS_PAD + HALO
    base1 = ROWS_PAD + (ROWS_PAD + HALO) // 2
    ext, width = gE.shape
    ext1, width1 = ext // 2, g1.shape[1]
    half_rows = rows // 2
    base_w = ROWS_PAD + ROW_HALO
    near1 = slice(ROWS_PAD, ROWS_PAD + ext1)
    wide1 = slice(ROWS_PAD, base_w + half_rows + ROW_HALO)
    lanes = 128

    load_g = pltpu.make_async_copy(g_hbm, g_ref, load_sem.at[0])
    load_s = pltpu.make_async_copy(s_hbm, s_ref, load_sem.at[1])
    load_g.start()
    load_s.start()
    zero_halo = jnp.zeros((base, width), F32)
    for ref in (gE, sE):
        ref[0:base, :] = zero_halo
        ref[base + rows : ext, :] = zero_halo
    for ref in (recv_l, recv_r):
        ref[...] = jnp.zeros(ref.shape, F32)
    for ref in (g1, s1):
        ref[0:base_w, :] = jnp.zeros((base_w, width1), F32)
        ref[base_w + half_rows :, :] = jnp.zeros((base_w, width1), F32)
    barrier = pltpu.get_barrier_semaphore()

    @pl.loop(1, total)
    def _(k):
        peer = lax.rem(me + k, total)
        pl.semaphore_signal(
            barrier, inc=1, device_id=(peer // gy_count, lax.rem(peer, gy_count)), device_id_type=MESH
        )

    lane = iota((rows, lanes), 1)
    half = lanes // 2
    l0 = iota((width, width1), 0)
    col0 = jnp.where(l0 < cols + half, l0, l0 - width)
    down0[...] = jnp.where(
        ((col0 + 2 * width1) // 2) % width1 == iota((width, width1), 1), 1.0, 0.0
    ).astype(BF16)
    l0 = iota((width1, width), 1)
    col0 = jnp.where(l0 < cols + half, l0, l0 - width)
    up0[...] = jnp.where(
        ((col0 + 2 * width1) // 2) % width1 == iota((width1, width), 0), 1.0, 0.0
    ).astype(BF16)
    l1 = iota((width1, lanes), 0)
    j2 = l1 // 2
    place = (j2 % 4) * 16 + j2 // 4
    down1[...] = jnp.where(
        (l1 < lanes) & (iota((width1, lanes), 1) % half == place), 1.0, 0.0
    ).astype(BF16)
    q_count = s2.shape[2]
    p_count = s2.shape[1]
    m1 = iota((q_count, width1), 1)
    col1 = jnp.where(m1 < lanes + half // 2, m1, m1 - width1)
    wide = gy * half + (col1 + 512) // 2 - 256
    for r in range(4):
        spread[r * q_count : (r + 1) * q_count, :] = jnp.where(
            wide == 4 * iota((q_count, width1), 0) + r, 1.0, 0.0
        ).astype(BF16)

    load_g.wait()
    load_s.wait()
    send_l[...] = jnp.where(lane < half, g_ref[:, 0:lanes], pltpu.roll(s_ref[:, 0:lanes], half, 1))
    send_r[...] = jnp.where(
        lane < half, pltpu.roll(s_ref[:, cols - lanes : cols], half, 1), g_ref[:, cols - lanes : cols]
    )

    l1 = iota((width1, lanes), 0)
    at2 = (jnp.where(l1 < lanes + half // 2, l1, l1 - width1) + 2 * lanes) // 2
    at4 = at2 // 4 - 24
    down_w[...] = jnp.where(
        (at4 >= 0) & (at4 < 32) & (iota((width1, lanes), 1) == (at2 % 4) * 32 + at4), 1.0, 0.0
    ).astype(BF16)
    l1 = iota((lanes, width1), 1)
    at2 = (jnp.where(l1 < lanes + half // 2, l1, l1 - width1) + 2 * lanes) // 2
    at4 = at2 // 4 - 24
    up_w[...] = jnp.where(
        (at4 >= 0) & (at4 < 32) & (iota((lanes, width1), 0) == (at2 % 4) * 32 + at4), 1.0, 0.0
    ).astype(BF16)

    def pack_level2(source):
        parts = []
        for t in range(4):
            start = base1 + 2 * t
            parts.append(
                get_strips(source, pl.ds(start, 8, 8)) + get_strips(source, pl.ds(start + 1, 8, 8))
            )
        means = 0.25 * exact_dot(jnp.concatenate(parts, 0), down1[...])
        low = iota((16, lanes), 1) < half
        return jnp.where(low, means[0:16], means[16:32])

    own_strips = cols // lanes
    for k in range(own_strips):
        fine_add[k, base : base + rows, :] = s_ref[:, k * lanes : (k + 1) * lanes]
    own = get_strips(fine_add, pl.ds(base, half_rows, 2), own_strips)
    own = own + get_strips(fine_add, pl.ds(base + 1, half_rows, 2), own_strips)
    put_strips(r1, slice(base1, base1 + half_rows), 0.25 * exact_dot(own, down0[0:cols, :]))
    rbuf[0, me] = pack_level2(r1)
    gE[base : base + rows, 0:cols] = g_ref[...]
    sE[base : base + rows, 0:cols] = s_ref[...]

    pl.semaphore_wait(barrier, total - 1)

    top, bottom = slice(0, HALO), slice(rows - HALO, rows)
    above, below = slice(ROWS_PAD, base), slice(base + rows, base + rows + HALO)
    middle = slice(base, base + rows)
    sends = (
        (0, -1, send_l, recv_r.at[middle, :]),
        (0, 1, send_r, recv_l.at[middle, :]),
        (-1, -1, send_l.at[top, :], recv_r.at[below, :]),
        (1, -1, send_l.at[bottom, :], recv_r.at[above, :]),
        (-1, 1, send_r.at[top, :], recv_l.at[below, :]),
        (1, 1, send_r.at[bottom, :], recv_l.at[above, :]),
        (-1, 0, g_ref.at[top, :], gE.at[below, 0:cols]),
        (-1, 0, s_ref.at[top, :], sE.at[below, 0:cols]),
        (1, 0, g_ref.at[bottom, :], gE.at[above, 0:cols]),
        (1, 0, s_ref.at[bottom, :], sE.at[above, 0:cols]),
    )

    def inside(dx, dy):
        ok = None
        for step, at, count in ((dx, gx, gx_count), (dy, gy, gy_count)):
            if step:
                here = (at > 0) if step < 0 else (at < count - 1)
                ok = here if ok is None else ok & here
        return ok

    def halo_copy(n, dx, dy, source, target):
        return pltpu.make_async_remote_copy(
            src_ref=source, dst_ref=target, send_sem=halo_send.at[n], recv_sem=halo_recv.at[n],
            device_id=(gx + dx, gy + dy), device_id_type=MESH,
        )

    for n, (dx, dy, source, target) in enumerate(sends):
        @pl.when(inside(dx, dy))
        def _():
            halo_copy(n, dx, dy, source, target).start()

    core = lax.rem(gy, 2)
    per_row = gy_count // 2
    chips = total // 2
    chip = me // 2
    partner = (gx, gy + 1 - 2 * core)

    def zigzag(j):
        odd = lax.rem(j, 2)
        return odd * ((j + 1) // 2) + (1 - odd) * (chips - j // 2)

    def block_copy(turn, n, slot, peer):
        return pltpu.make_async_remote_copy(
            src_ref=rbuf.at[turn, slot], dst_ref=rbuf.at[turn, slot],
            send_sem=all_send.at[turn, n], recv_sem=all_recv.at[turn, slot],
            device_id=peer, device_id_type=MESH,
        )

    def direct(turn, j):
        other = lax.rem(chip + zigzag(j), chips)
        return block_copy(turn, j, me, (other // per_row, 2 * lax.rem(other, per_row) + core))

    def onward(turn, j):
        slot = 2 * lax.rem(chip + chips - zigzag(j), chips) + core
        return block_copy(turn, chips + j, slot, partner)

    def gather_start(turn):
        block_copy(turn, 0, me, partner).start()

        @pl.loop(1, chips)
        def _(j):
            direct(turn, chips - j).start()

    def gather_wait(turn):
        @pl.loop(1, chips)
        def _(j):
            copy = onward(turn, j)
            copy.wait_recv()
            copy.start()

        block_copy(turn, 0, me + 1 - 2 * core, partner).wait_recv()

        @pl.loop(1, chips)
        def _(j):
            slot = 2 * lax.rem(chip + chips - zigzag(j), chips) + 1 - core
            block_copy(turn, chips + j, slot, partner).wait_recv()

    def gather_sent(turn):
        block_copy(turn, 0, me, partner).wait_send()

        @pl.loop(1, chips)
        def _(j):
            direct(turn, j).wait_send()
            onward(turn, j).wait_send()

    gather_start(0)
    zero_tile = jnp.zeros((ROWS_PAD, width), F32)
    for ref in (vA, vB):
        ref[0:ROWS_PAD, :] = zero_tile
        ref[ext - ROWS_PAD : ext, :] = zero_tile
    for ref in (aP, bP, a1, b1):
        ref[0:ROWS_PAD, :] = jnp.zeros((ROWS_PAD, width1), F32)
        ref[ref.shape[0] - ROWS_PAD :, :] = jnp.zeros((ROWS_PAD, width1), F32)
    for ref in (a2, b2, a3, b3, a4, b4):
        for i in range(ref.shape[0]):
            ref[i, 0:8, :] = jnp.zeros((8, q_count), F32)
            ref[i, 8 + p_count : 16 + p_count, :] = jnp.zeros((8, q_count), F32)

    for n, (dx, dy, source, target) in enumerate(sends):
        @pl.when(inside(-dx, -dy))
        def _():
            halo_copy(n, -dx, -dy, source, target).wait_recv()

    lane_e = iota((ext, lanes), 1)
    gE[:, cols:width] = jnp.where(lane_e < half, recv_r[...], recv_l[...])
    sE[:, cols:width] = pltpu.roll(jnp.where(lane_e < half, recv_l[...], recv_r[...]), half, 1)

    def weight(shifts, first_row, own_rows, own_cols, split, level):
        shape = shifts.shape
        at_row = gx * own_rows + iota(shape, 0) + first_row
        lane_at = iota(shape, 1)
        at_col = gy * own_cols + jnp.where(lane_at < own_cols + split, lane_at, lane_at - shape[1])
        good = (at_row >= 0) & (at_row < gx_count * own_rows)
        good = good & (at_col >= 0) & (at_col < gy_count * own_cols)
        return jnp.where(good, DAMPING / (4.0 ** (1 - level) + shifts), 0.0)

    def around(v, lo, size):
        span = v.shape[1]
        mid = v[lo : lo + size, :]
        beside = pltpu.roll(mid, 1, 1) + pltpu.roll(mid, span - 1, 1)
        return mid, beside + (v[lo - 1 : lo - 1 + size, :] + v[lo + 1 : lo + 1 + size, :])

    def sweep_block(v, out, g, w, level, span=None):
        scale = 4.0 ** (-level)
        for lo in range(*(span or (ROWS_PAD, v.shape[0] - ROWS_PAD)), 8):
            mid, beside = around(v, lo, 8)
            at = slice(lo, lo + 8)
            out[at, :] = (1.0 - DAMPING) * mid + w[at, :] * (g[at, :] + scale * beside)

    def residual_block(v, out, g, s, level, span=None):
        scale = 4.0 ** (-level)
        for lo in range(*(span or (ROWS_PAD, v.shape[0] - ROWS_PAD)), 8):
            mid, beside = around(v, lo, 8)
            at = slice(lo, lo + 8)
            put_strips(out, at, g[at, :] - (scale * (4.0 * mid - beside) + s[at, :] * mid))

    row_moves = (
        (-1, sP.at[base1 : base1 + ROW_HALO, :], s1.at[base_w + half_rows : base_w + half_rows + ROW_HALO, :]),
        (1, sP.at[base1 + half_rows - ROW_HALO : base1 + half_rows, :], s1.at[ROWS_PAD:base_w, :]),
        (-1, gP.at[base1 : base1 + ROW_HALO, :], g1.at[base_w + half_rows : base_w + half_rows + ROW_HALO, :]),
        (1, gP.at[base1 + half_rows - ROW_HALO : base1 + half_rows, :], g1.at[ROWS_PAD:base_w, :]),
    )

    def row_copy(n, dx):
        _, source, target = row_moves[n]
        return pltpu.make_async_remote_copy(
            src_ref=source, dst_ref=target, send_sem=row_send.at[n], recv_sem=row_recv.at[n],
            device_id=(gx + dx, gy), device_id_type=MESH,
        )

    def rows_start(which):
        for n in which:
            dx = row_moves[n][0]
            @pl.when(inside(dx, 0))
            def _():
                row_copy(n, dx).start()

    def halved():
        pairs = get_strips(fine_add, pl.ds(0, ext1, 2)) + get_strips(fine_add, pl.ds(1, ext1, 2))
        return 0.25 * exact_dot(pairs, down0[...])

    put_strips(fine_add, slice(0, ext), sE[...])
    sP[near1, :] = halved()
    rows_start((0, 1))
    chunk = 16
    for lo in range(0, ext, chunk):
        at = slice(lo, lo + chunk)
        wE[at, :] = weight(sE[at, :], lo - base, rows, cols, half, 0)
    for lo in range(ROWS_PAD, ext - ROWS_PAD, 8):
        at = slice(lo, lo + 8)
        vA[at, :] = wE[at, :] * gE[at, :]
    sweep_block(vA, vB, gE, wE, 0)
    put_strips(fine_add, slice(0, ROWS_PAD), zero_tile)
    put_strips(fine_add, slice(ext - ROWS_PAD, ext), zero_tile)
    residual_block(vB, fine_add, gE, sE, 0)
    gP[near1, :] = halved()
    wP[near1, :] = weight(sP[near1, :], ROWS_PAD - base1, half_rows, cols // 2, half // 2, 1)
    aP[near1, :] = wP[near1, :] * gP[near1, :]
    sweep_block(aP, bP, gP, wP, 1)
    residual_block(bP, r1, gP, sP, 1, (base1, base1 + half_rows))
    rbuf[1, me] = pack_level2(r1)
    gather_start(1)
    rows_start((2, 3))

    block = (lane_e[0:8] // 16)

    def unpack(turn, target):
        for x in range(gx_count):
            for u in range(gy_count // 8):
                for tl in range(2):
                    tiles = [rbuf[turn, x * gy_count + u * 8 + g, tl * 8 : tl * 8 + 8, :] for g in range(8)]
                    for bit in (1, 2, 4):
                        keep = (block & bit) == 0
                        fresh = list(tiles)
                        for g in range(8):
                            if g & bit == 0:
                                lo, hi = tiles[g], tiles[g | bit]
                                fresh[g] = jnp.where(keep, lo, pltpu.roll(hi, 16 * bit, 1))
                                fresh[g | bit] = jnp.where(keep, pltpu.roll(lo, lanes - 16 * bit, 1), hi)
                        tiles = fresh
                    for b in range(8):
                        t, r = (b // 4) * 2 + tl, b % 4
                        target[t * 4 + r, 8 * x : 8 * x + 8, u * lanes : (u + 1) * lanes] = tiles[b]

    lane_q = iota((p_count, q_count), 1)
    rows_q = slice(8, 8 + p_count)

    def sides(v, n, t, r):
        mid = v[t * n + r, rows_q, :]
        if t > 0:
            north = v[(t - 1) * n + r, rows_q, :]
        else:
            north = v[(n - 1) * n + r, 7 : 7 + p_count, :]
        if t < n - 1:
            south = v[(t + 1) * n + r, rows_q, :]
        else:
            south = v[r, 9 : 9 + p_count, :]
        if r > 0:
            west = v[t * n + r - 1, rows_q, :]
        else:
            west = jnp.where(lane_q == 0, 0.0, pltpu.roll(v[t * n + n - 1, rows_q, :], 1, 1))
        if r < n - 1:
            east = v[t * n + r + 1, rows_q, :]
        else:
            east = jnp.where(
                lane_q == q_count - 1, 0.0, pltpu.roll(v[t * n, rows_q, :], q_count - 1, 1)
            )
        return mid, (north + south) + (west + east)

    level_refs = {2: (s2, w2, g2, a2, b2, 4), 3: (s3, w3, g3, a3, b3, 2), 4: (s4, w4, g4, a4, b4, 1)}

    def sweep(level, v, out):
        s, w, g, _, _, n = level_refs[level]
        for t in range(n):
            for r in range(n):
                i = t * n + r
                mid, beside = sides(v, n, t, r)
                out[i, rows_q, :] = (1.0 - DAMPING) * mid + w[i] * (g[i] + 4.0 ** (-level) * beside)

    def first_sweep(level, out):
        s, w, g, _, _, n = level_refs[level]
        for i in range(n * n):
            out[i, rows_q, :] = w[i] * g[i]

    def restricted(level, v):
        s, w, g, _, _, n = level_refs[level]
        coarse_g = level_refs[level + 1][2]
        for t in range(n // 2):
            for r in range(n // 2):
                sums = None
                for dt in range(2):
                    for dr in range(2):
                        i = (2 * t + dt) * n + 2 * r + dr
                        mid, beside = sides(v, n, 2 * t + dt, 2 * r + dr)
                        left = g[i] - (4.0 ** (-level) * (4.0 * mid - beside) + s[i] * mid)
                        sums = left if sums is None else sums + left
                coarse_g[t * (n // 2) + r] = 0.25 * sums

    def correct(level, v, e):
        n = level_refs[level][5]
        for t in range(n):
            for r in range(n):
                i = t * n + r
                v[i, rows_q, :] = v[i, rows_q, :] + e[(t // 2) * (n // 2) + r // 2, rows_q, :]

    def prepare(level):
        s, w, _, _, _, n = level_refs[level]
        for i in range(n * n):
            w[i] = DAMPING / (4.0 ** (1 - level) + s[i])
        if level < 4:
            coarse_s = level_refs[level + 1][0]
            m = n // 2
            for t in range(m):
                for r in range(m):
                    i = 2 * t * n + 2 * r
                    coarse_s[t * m + r] = 0.25 * ((s[i] + s[i + n]) + (s[i + 1] + s[i + n + 1]))

    def total_of(x):
        return jnp.sum(jnp.sum(x, axis=0, keepdims=True), axis=1, keepdims=True)

    gather_wait(0)
    unpack(0, s2)
    for level in (2, 3, 4):
        prepare(level)
    row_q = iota((p_count, q_count), 0)
    edges = jnp.where(row_q == 0, 1.0, 0.0) + jnp.where(row_q == p_count - 1, 1.0, 0.0)
    edges = edges + jnp.where(lane_q == 0, 1.0, 0.0) + jnp.where(lane_q == q_count - 1, 1.0, 0.0)
    per_unit = 1.0 / total_of(4.0 ** (-4) * edges + s4[0])

    def coarse(v, from_zero):
        if from_zero:
            shifted = jnp.zeros((p_count, q_count), F32) + total_of(g4[0]) * per_unit
        else:
            mid, beside = sides(v, 1, 0, 0)
            left = g4[0] - (4.0 ** (-4) * (4.0 * mid - beside) + s4[0] * mid)
            shifted = mid + total_of(left) * per_unit
        now, later = a4, b4
        now[0, rows_q, :] = shifted
        for _ in range(COARSE_SWEEPS):
            sweep(4, now, later)
            now, later = later, now
        return now

    def vcycle(level, v):
        if level == 4:
            return coarse(v, v is None)
        _, _, _, a, b, n = level_refs[level]
        if v is None:
            first_sweep(level, a)
            sweep(level, a, b)
            now, later = b, a
        else:
            later = b if v is a else a
            sweep(level, v, later)
            sweep(level, later, v)
            now = v
        restricted(level, now)
        correct(level, now, vcycle(level + 1, None))
        sweep(level, now, later)
        sweep(level, later, now)
        return now

    def fcycle(level):
        if level == 4:
            return coarse(None, True)
        _, _, _, a, b, n = level_refs[level]
        first_sweep(level, a)
        sweep(level, a, b)
        restricted(level, b)
        e = fcycle(level + 1)
        e = vcycle(level + 1, e)
        correct(level, b, e)
        sweep(level, b, a)
        sweep(level, a, b)
        return b

    window = picked.shape[1] - 8
    lane_w, row_w = iota((window, lanes), 1), iota((window, lanes), 0)

    def in_domain(period):
        at_p, at_q = gx * 8 - 4 + row_w, gy * 16 - 8 + lane_w % period
        good = (at_p >= 0) & (at_p < p_count) & (at_q >= 0) & (at_q < q_count)
        return good & (lane_w % period < 32)

    def put_window(t, values):
        for a in range(2):
            put_strips(r1, pl.ds(ROWS_PAD + 2 * t + a, window, 8), values)

    def add_level2(e, v):
        for t in range(4):
            tiles = [e[t * 4 + r, pl.ds(pl.multiple_of(gx * 8, 8), 24), :] for r in range(4)]
            picked[t] = exact_dot(jnp.concatenate(tiles, 1), spread[...])
        for t in range(4):
            put_window(t, picked[t, 4 : 4 + window, :])
        v[wide1, :] = v[wide1, :] + get_strips(r1, wide1)

    def pack_window(source):
        parts = []
        for t in range(4):
            start = ROWS_PAD + 2 * t
            parts.append(
                get_strips(source, pl.ds(start, window, 8)) + get_strips(source, pl.ds(start + 1, window, 8))
            )
        means = 0.25 * exact_dot(jnp.concatenate(parts, 0), down_w[...])
        return [means[t * window : (t + 1) * window] for t in range(4)]

    def joined(x, unit):
        return x + pltpu.roll(x, lanes - unit, 1)

    def halved_window(tiles, unit):
        return [0.25 * joined(tiles[2 * t] + tiles[2 * t + 1], unit) for t in range(len(tiles) // 2)]

    def beside_window(v, unit):
        n = len(v)
        out = []
        for t in range(n):
            north = v[t - 1] if t > 0 else pltpu.roll(v[n - 1], 1, 0)
            south = v[t + 1] if t < n - 1 else pltpu.roll(v[0], window - 1, 0)
            west = jnp.where(lane_w < unit, pltpu.roll(v[t], unit + 1, 1), pltpu.roll(v[t], unit, 1))
            east = jnp.where(
                lane_w >= lanes - unit,
                pltpu.roll(v[t], lanes - unit - 1, 1), pltpu.roll(v[t], lanes - unit, 1),
            )
            out.append((north + south) + (west + east))
        return out

    window_refs = {2: (s2w, w2w, 32), 3: (s3w, w3w, 64)}

    def sweep_window(level, v, g):
        _, w, unit = window_refs[level]
        beside = beside_window(v, unit)
        return [
            (1.0 - DAMPING) * v[t] + w[t] * (g[t] + 4.0 ** (-level) * beside[t]) for t in range(len(v))
        ]

    def residual_window(level, v, g):
        s, _, unit = window_refs[level]
        beside = beside_window(v, unit)
        return [
            g[t] - (4.0 ** (-level) * (4.0 * v[t] - beside[t]) + s[t] * v[t]) for t in range(len(v))
        ]

    for n, (dx, _, _) in enumerate(row_moves):
        @pl.when(inside(-dx, 0))
        def _():
            row_copy(n, -dx).wait_recv()

    own1, own_w = slice(base1, base1 + half_rows), slice(base_w, base_w + half_rows)
    g1[own_w, :] = gP[own1, :]
    s1[own_w, :] = sP[own1, :]
    w1[wide1, :] = weight(s1[wide1, :], ROWS_PAD - base_w, half_rows, cols // 2, half // 2, 1)
    a1[wide1, :] = w1[wide1, :] * g1[wide1, :]
    sweep_block(a1, b1, g1, w1, 1)
    put_strips(r1, wide1, s1[wide1, :])
    tiles = pack_window(r1)
    for t in range(4):
        s2w[t] = tiles[t]
        w2w[t] = jnp.where(in_domain(32), DAMPING / (4.0 ** (-1) + tiles[t]), 0.0)
    tiles = halved_window(tiles, 32)
    for t in range(2):
        s3w[t] = tiles[t]
        w3w[t] = jnp.where(in_domain(64), DAMPING / (4.0 ** (-2) + tiles[t]), 0.0)

    def coarse_copy(peer):
        return pltpu.make_async_remote_copy(
            src_ref=cbuf.at[me], dst_ref=cbuf.at[me], send_sem=coarse_sems.at[0], recv_sem=coarse_sems.at[1],
            device_id=(peer // gy_count, lax.rem(peer, gy_count)), device_id_type=MESH,
        )

    def coarse_wait(n):
        others = cbuf.at[pl.ds(0, total - 1)]
        pltpu.make_async_copy(others, others, coarse_sems.at[n]).wait()

    gather_wait(1)
    unpack(1, g2)
    e = fcycle(2)
    e = vcycle(2, e)
    add_level2(e, b1)
    sweep_block(b1, a1, g1, w1, 1)
    sweep_block(a1, b1, g1, w1, 1)
    sweep_block(b1, a1, g1, w1, 1)
    sweep_block(a1, b1, g1, w1, 1)
    residual_block(b1, r1, g1, s1, 1)
    source2 = pack_window(r1)
    v2 = sweep_window(2, [w2w[t] * source2[t] for t in range(4)], source2)
    source3 = halved_window(residual_window(2, v2, source2), 32)
    v3 = sweep_window(3, [w3w[t] * source3[t] for t in range(2)], source3)
    source4 = halved_window(residual_window(3, v3, source3), 64)[0]
    place = lax.rem(gy, 8) * 16
    mine = pltpu.roll(source4[4:12], lax.rem(place + lanes - 8, lanes), 1)
    lane_c = iota((8, lanes), 1)
    cbuf[me] = jnp.where((lane_c >= place) & (lane_c < place + 16), mine, 0.0)

    @pl.loop(0, total - 1)
    def _(k):
        odd = lax.rem(k, 2)
        coarse_copy(lax.rem(me + total + total // 2 + odd * ((k + 1) // 2) - (1 - odd) * (k // 2), total)).start()

    gather_sent(0)
    gather_sent(1)
    for n, (dx, dy, source, target) in enumerate(sends):
        @pl.when(inside(dx, dy))
        def _():
            halo_copy(n, dx, dy, source, target).wait_send()
    for n, (dx, _, _) in enumerate(row_moves):
        @pl.when(inside(dx, 0))
        def _():
            row_copy(n, dx).wait_send()
    coarse_wait(1)
    for x in range(gx_count):
        for u in range(gy_count // 8):
            first = x * gy_count + u * 8
            pairs = [cbuf[first + k] + cbuf[first + k + 1] for k in range(0, 8, 2)]
            g4[0, x * 8 : x * 8 + 8, u * lanes : (u + 1) * lanes] = (pairs[0] + pairs[1]) + (pairs[2] + pairs[3])
    e = coarse(None, True)
    e = e[0, pl.ds(pl.multiple_of(gx * 8, 8), 24), :][4 : 4 + window]
    e = pltpu.roll(e, lax.rem(q_count + 8 - gy * 16 + q_count, q_count), 1)[:, 0:lanes]
    e = jnp.where(in_domain(lanes), e, 0.0)
    e = e + pltpu.roll(e, 64, 1)
    v3 = [v3[t] + e for t in range(2)]
    v3 = sweep_window(3, sweep_window(3, v3, source3), source3)
    e = [v3[t] + pltpu.roll(v3[t], 32, 1) for t in range(2)]
    v2 = [v2[t] + e[t // 2] for t in range(4)]
    v2 = sweep_window(2, sweep_window(2, v2, source2), source2)
    raised = exact_dot(jnp.concatenate(v2, 0), up_w[...])
    for t in range(4):
        put_window(t, raised[t * window : (t + 1) * window])
    b1[wide1, :] = b1[wide1, :] + get_strips(r1, wide1)
    near_w = (base_w - 8, base_w + half_rows + 8)
    sweep_block(b1, a1, g1, w1, 1, near_w)
    sweep_block(a1, b1, g1, w1, 1, near_w)
    raised = exact_dot(b1[slice(*near_w), :], up0[...])
    put_strips(fine_add, pl.ds(0, ext1, 2), raised)
    put_strips(fine_add, pl.ds(1, ext1, 2), raised)
    for lo in range(ROWS_PAD, ext - ROWS_PAD, 8):
        at = slice(lo, lo + 8)
        vB[at, :] = vB[at, :] + get_strips(fine_add, at)
    sweep_block(vB, vA, gE, wE, 0)
    sweep_block(vA, vB, gE, wE, 0)
    for lo in range(0, rows, 8):
        mid, beside = around(vB, base + lo, 8)
        at = slice(base + lo, base + lo + 8)
        left = gE[at, :] - ((4.0 * mid - beside) + sE[at, :] * mid)
        out_ref[0, lo : lo + 8, :] = mid[:, 0:cols]
        out_ref[1, lo : lo + 8, :] = left[:, 0:cols]

    coarse_wait(0)


def solution(mesh):
    gx_count, gy_count = mesh.shape["gx"], mesh.shape["gy"]
    total = gx_count * gy_count

    def body(right_side, shift):
        rows, cols = right_side.shape
        assert cols == 256 and rows == 128 and gy_count % 8 == 0
        ext, width = rows + 2 * (HALO + ROWS_PAD), cols + 128
        ext1, width1 = ext // 2 + 2 * ROWS_PAD, 256
        wide1 = rows // 2 + 2 * (ROW_HALO + ROWS_PAD)
        window = rows // 16 + 8
        p, q = rows // 16 * gx_count, cols // 16 * gy_count
        V = pltpu.VMEM
        dma = pltpu.SemaphoreType.DMA
        big = [V((ext, width), F32)] * 5 + [V((width // 128, ext, 128), F32)]
        one = [V((ext1, width1), F32)] * 5
        one += [V((wide1, width1), F32)] * 5 + [V((width1 // 128, wide1, 128), F32)]
        levels = []
        for n in (16, 4, 1):
            levels += [V((n, p, q), F32)] * 3 + [V((n, p + 16, q), F32)] * 2
        scratch = (
            [V((rows, cols), F32)] * 2 + [dma((2,))]
            + big + one
            + [V((rows, 128), F32)] * 2 + [V((ext, 128), F32)] * 2
            + [V((width, width1), BF16), V((width1, width), BF16), V((width1, 128), BF16), V((4 * q, width1), BF16)]
            + [V((width1, 128), BF16), V((128, width1), BF16)]
            + [V((2, total, 16, 128), F32), V((total, 8, 128), F32)]
            + levels
            + [V((4, 24, width1), F32)]
            + [V((4, window, 128), F32)] * 2 + [V((2, window, 128), F32)] * 2
            + [dma((10,)), dma((10,)), dma((4,)), dma((4,)), dma((2, total)), dma((2, total)), dma((2,))]
        )
        out = jax.ShapeDtypeStruct((2,) + right_side.shape, F32)
        both = pl.pallas_call(
            functools.partial(kernel, gx_count, gy_count),
            out_shape=out,
            in_specs=[pl.BlockSpec(memory_space=pltpu.HBM)] * 2,
            out_specs=pl.BlockSpec(memory_space=pltpu.VMEM),
            scratch_shapes=scratch,
            compiler_params=pltpu.CompilerParams(
                collective_id=0, has_side_effects=True, vmem_limit_bytes=60*1024*1024
            ),
        )(right_side, shift)
        return both[0], both[1]

    spec = P("gx", "gy")
    return jax.shard_map(body, mesh=mesh, in_specs=(spec, spec), out_specs=(spec, spec), check_vma=False)
```

```python
import functools

import jax
import jax.numpy as jnp
from jax import lax
from jax.experimental import pallas as pl
from jax.experimental.pallas import tpu as pltpu
from jax.sharding import PartitionSpec as P

DAMPING = 0.8
MESH = pl.DeviceIdType.MESH
F32 = jnp.float32
BF16 = jnp.bfloat16

ROWS_PAD = 8
HALO = 8
ROW_HALO = 32


def iota(shape, dim):
    return lax.broadcasted_iota(jnp.int32, shape, dim)


def put_strips(ref, at, values):
    for k in range(ref.shape[0]):
        ref[k, at, :] = values[:, k * 128 : (k + 1) * 128]


def get_strips(ref, at, count=None):
    return jnp.concatenate([ref[k, at, :] for k in range(count or ref.shape[0])], 1)


def exact_dot(values, selector):
    first = values.astype(BF16)
    rest = values - first.astype(F32)
    second = rest.astype(BF16)
    third = (rest - second.astype(F32)).astype(BF16)
    dot = functools.partial(jnp.dot, preferred_element_type=F32)
    return dot(first, selector) + (dot(second, selector) + dot(third, selector))


def kernel(
    gx_count, gy_count, g_hbm, s_hbm, out_ref,
    g_ref, s_ref, load_sem,
    gE, sE, wE, vA, vB, fine_add,
    gP, sP, wP, aP, bP,
    g1, s1, w1, a1, b1, r1,
    send_l, send_r, recv_l, recv_r,
    down0, up0, down1, spread, down_w, up_w,
    rbuf, cbuf, s2, w2, g2, a2, b2, s3, w3, g3, a3, b3, s4, w4, g4, a4, picked,
    s2w, w2w, s3w, w3w, hw4, phi, beside4,
    halo_send, halo_recv, row_send, row_recv, all_send, all_recv, coarse_sems,
):
    gx, gy = lax.axis_index("gx"), lax.axis_index("gy")
    total = gx_count * gy_count
    me = gx * gy_count + gy
    rows, cols = g_hbm.shape
    base = ROWS_PAD + HALO
    base1 = ROWS_PAD + (ROWS_PAD + HALO) // 2
    ext, width = gE.shape
    ext1, width1 = ext // 2, g1.shape[1]
    half_rows = rows // 2
    base_w = ROWS_PAD + ROW_HALO
    near1 = slice(ROWS_PAD, ROWS_PAD + ext1)
    wide1 = slice(ROWS_PAD, base_w + half_rows + ROW_HALO)
    lanes = 128

    load_g = pltpu.make_async_copy(g_hbm, g_ref, load_sem.at[0])
    load_s = pltpu.make_async_copy(s_hbm, s_ref, load_sem.at[1])
    load_g.start()
    load_s.start()
    zero_halo = jnp.zeros((base, width), F32)
    for ref in (gE, sE):
        ref[0:base, :] = zero_halo
        ref[base + rows : ext, :] = zero_halo
    for ref in (recv_l, recv_r):
        ref[...] = jnp.zeros(ref.shape, F32)
    for ref in (g1, s1):
        ref[0:base_w, :] = jnp.zeros((base_w, width1), F32)
        ref[base_w + half_rows :, :] = jnp.zeros((base_w, width1), F32)
    barrier = pltpu.get_barrier_semaphore()

    @pl.loop(1, total)
    def _(k):
        peer = lax.rem(me + k, total)
        pl.semaphore_signal(
            barrier, inc=1, device_id=(peer // gy_count, lax.rem(peer, gy_count)), device_id_type=MESH
        )

    lane = iota((rows, lanes), 1)
    half = lanes // 2
    l0 = iota((width, width1), 0)
    col0 = jnp.where(l0 < cols + half, l0, l0 - width)
    down0[...] = jnp.where(
        ((col0 + 2 * width1) // 2) % width1 == iota((width, width1), 1), 1.0, 0.0
    ).astype(BF16)
    l0 = iota((width1, width), 1)
    col0 = jnp.where(l0 < cols + half, l0, l0 - width)
    up0[...] = jnp.where(
        ((col0 + 2 * width1) // 2) % width1 == iota((width1, width), 0), 1.0, 0.0
    ).astype(BF16)
    l1 = iota((width1, lanes), 0)
    j2 = l1 // 2
    place = (j2 % 4) * 16 + j2 // 4
    down1[...] = jnp.where(
        (l1 < lanes) & (iota((width1, lanes), 1) % half == place), 1.0, 0.0
    ).astype(BF16)
    q_count = s2.shape[2]
    p_count = s2.shape[1]
    m1 = iota((q_count, width1), 1)
    col1 = jnp.where(m1 < lanes + half // 2, m1, m1 - width1)
    wide = gy * half + (col1 + 512) // 2 - 256
    for r in range(4):
        spread[r * q_count : (r + 1) * q_count, :] = jnp.where(
            wide == 4 * iota((q_count, width1), 0) + r, 1.0, 0.0
        ).astype(BF16)

    load_g.wait()
    load_s.wait()
    send_l[...] = jnp.where(lane < half, g_ref[:, 0:lanes], pltpu.roll(s_ref[:, 0:lanes], half, 1))
    send_r[...] = jnp.where(
        lane < half, pltpu.roll(s_ref[:, cols - lanes : cols], half, 1), g_ref[:, cols - lanes : cols]
    )

    l1 = iota((width1, lanes), 0)
    at2 = (jnp.where(l1 < lanes + half // 2, l1, l1 - width1) + 2 * lanes) // 2
    at4 = at2 // 4 - 24
    down_w[...] = jnp.where(
        (at4 >= 0) & (at4 < 32) & (iota((width1, lanes), 1) == (at2 % 4) * 32 + at4), 1.0, 0.0
    ).astype(BF16)
    l1 = iota((lanes, width1), 1)
    at2 = (jnp.where(l1 < lanes + half // 2, l1, l1 - width1) + 2 * lanes) // 2
    at4 = at2 // 4 - 24
    up_w[...] = jnp.where(
        (at4 >= 0) & (at4 < 32) & (iota((lanes, width1), 0) == (at2 % 4) * 32 + at4), 1.0, 0.0
    ).astype(BF16)

    def pack_level2(source):
        parts = []
        for t in range(4):
            start = base1 + 2 * t
            parts.append(
                get_strips(source, pl.ds(start, 8, 8)) + get_strips(source, pl.ds(start + 1, 8, 8))
            )
        means = 0.25 * exact_dot(jnp.concatenate(parts, 0), down1[...])
        low = iota((16, lanes), 1) < half
        return jnp.where(low, means[0:16], means[16:32])

    own_strips = cols // lanes
    for k in range(own_strips):
        fine_add[k, base : base + rows, :] = s_ref[:, k * lanes : (k + 1) * lanes]
    own = get_strips(fine_add, pl.ds(base, half_rows, 2), own_strips)
    own = own + get_strips(fine_add, pl.ds(base + 1, half_rows, 2), own_strips)
    put_strips(r1, slice(base1, base1 + half_rows), 0.25 * exact_dot(own, down0[0:cols, :]))
    rbuf[0, me] = pack_level2(r1)
    gE[base : base + rows, 0:cols] = g_ref[...]
    sE[base : base + rows, 0:cols] = s_ref[...]

    pl.semaphore_wait(barrier, total - 1)

    top, bottom = slice(0, HALO), slice(rows - HALO, rows)
    above, below = slice(ROWS_PAD, base), slice(base + rows, base + rows + HALO)
    middle = slice(base, base + rows)
    sends = (
        (0, -1, send_l, recv_r.at[middle, :]),
        (0, 1, send_r, recv_l.at[middle, :]),
        (-1, -1, send_l.at[top, :], recv_r.at[below, :]),
        (1, -1, send_l.at[bottom, :], recv_r.at[above, :]),
        (-1, 1, send_r.at[top, :], recv_l.at[below, :]),
        (1, 1, send_r.at[bottom, :], recv_l.at[above, :]),
        (-1, 0, g_ref.at[top, :], gE.at[below, 0:cols]),
        (-1, 0, s_ref.at[top, :], sE.at[below, 0:cols]),
        (1, 0, g_ref.at[bottom, :], gE.at[above, 0:cols]),
        (1, 0, s_ref.at[bottom, :], sE.at[above, 0:cols]),
    )

    def inside(dx, dy):
        ok = None
        for step, at, count in ((dx, gx, gx_count), (dy, gy, gy_count)):
            if step:
                here = (at > 0) if step < 0 else (at < count - 1)
                ok = here if ok is None else ok & here
        return ok

    def halo_copy(n, dx, dy, source, target):
        return pltpu.make_async_remote_copy(
            src_ref=source, dst_ref=target, send_sem=halo_send.at[n], recv_sem=halo_recv.at[n],
            device_id=(gx + dx, gy + dy), device_id_type=MESH,
        )

    for n, (dx, dy, source, target) in enumerate(sends):
        @pl.when(inside(dx, dy))
        def _():
            halo_copy(n, dx, dy, source, target).start()

    core = lax.rem(gy, 2)
    per_row = gy_count // 2
    chips = total // 2
    chip = me // 2
    partner = (gx, gy + 1 - 2 * core)

    def zigzag(j):
        odd = lax.rem(j, 2)
        return odd * ((j + 1) // 2) + (1 - odd) * (chips - j // 2)

    def block_copy(turn, n, slot, peer):
        return pltpu.make_async_remote_copy(
            src_ref=rbuf.at[turn, slot], dst_ref=rbuf.at[turn, slot],
            send_sem=all_send.at[turn, n], recv_sem=all_recv.at[turn, slot],
            device_id=peer, device_id_type=MESH,
        )

    def direct(turn, j):
        other = lax.rem(chip + zigzag(j), chips)
        return block_copy(turn, j, me, (other // per_row, 2 * lax.rem(other, per_row) + core))

    def onward(turn, j):
        slot = 2 * lax.rem(chip + chips - zigzag(j), chips) + core
        return block_copy(turn, chips + j, slot, partner)

    def gather_start(turn):
        block_copy(turn, 0, me, partner).start()

        @pl.loop(1, chips)
        def _(j):
            direct(turn, chips - j).start()

    def gather_wait(turn):
        @pl.loop(1, chips)
        def _(j):
            copy = onward(turn, j)
            copy.wait_recv()
            copy.start()

        block_copy(turn, 0, me + 1 - 2 * core, partner).wait_recv()

        @pl.loop(1, chips)
        def _(j):
            slot = 2 * lax.rem(chip + chips - zigzag(j), chips) + 1 - core
            block_copy(turn, chips + j, slot, partner).wait_recv()

    def gather_sent(turn):
        block_copy(turn, 0, me, partner).wait_send()

        @pl.loop(1, chips)
        def _(j):
            direct(turn, j).wait_send()
            onward(turn, j).wait_send()

    gather_start(0)
    zero_tile = jnp.zeros((ROWS_PAD, width), F32)
    for ref in (vA, vB):
        ref[0:ROWS_PAD, :] = zero_tile
        ref[ext - ROWS_PAD : ext, :] = zero_tile
    for ref in (aP, bP, a1, b1):
        ref[0:ROWS_PAD, :] = jnp.zeros((ROWS_PAD, width1), F32)
        ref[ref.shape[0] - ROWS_PAD :, :] = jnp.zeros((ROWS_PAD, width1), F32)
    for ref in (a2, b2, a3, b3, a4):
        for i in range(ref.shape[0]):
            ref[i, 0:8, :] = jnp.zeros((8, q_count), F32)
            ref[i, 8 + p_count : 16 + p_count, :] = jnp.zeros((8, q_count), F32)

    for n, (dx, dy, source, target) in enumerate(sends):
        @pl.when(inside(-dx, -dy))
        def _():
            halo_copy(n, -dx, -dy, source, target).wait_recv()

    lane_e = iota((ext, lanes), 1)
    gE[:, cols:width] = jnp.where(lane_e < half, recv_r[...], recv_l[...])
    sE[:, cols:width] = pltpu.roll(jnp.where(lane_e < half, recv_l[...], recv_r[...]), half, 1)

    def weight(shifts, first_row, own_rows, own_cols, split, level):
        shape = shifts.shape
        at_row = gx * own_rows + iota(shape, 0) + first_row
        lane_at = iota(shape, 1)
        at_col = gy * own_cols + jnp.where(lane_at < own_cols + split, lane_at, lane_at - shape[1])
        good = (at_row >= 0) & (at_row < gx_count * own_rows)
        good = good & (at_col >= 0) & (at_col < gy_count * own_cols)
        return jnp.where(good, DAMPING / (4.0 ** (1 - level) + shifts), 0.0)

    def around(v, lo, size):
        span = v.shape[1]
        mid = v[lo : lo + size, :]
        beside = pltpu.roll(mid, 1, 1) + pltpu.roll(mid, span - 1, 1)
        return mid, beside + (v[lo - 1 : lo - 1 + size, :] + v[lo + 1 : lo + 1 + size, :])

    def sweep_block(v, out, g, w, level, span=None):
        scale = 4.0 ** (-level)
        for lo in range(*(span or (ROWS_PAD, v.shape[0] - ROWS_PAD)), 8):
            mid, beside = around(v, lo, 8)
            at = slice(lo, lo + 8)
            out[at, :] = (1.0 - DAMPING) * mid + w[at, :] * (g[at, :] + scale * beside)

    def residual_block(v, out, g, s, level, span=None):
        scale = 4.0 ** (-level)
        for lo in range(*(span or (ROWS_PAD, v.shape[0] - ROWS_PAD)), 8):
            mid, beside = around(v, lo, 8)
            at = slice(lo, lo + 8)
            put_strips(out, at, g[at, :] - (scale * (4.0 * mid - beside) + s[at, :] * mid))

    row_moves = (
        (-1, sP.at[base1 : base1 + ROW_HALO, :], s1.at[base_w + half_rows : base_w + half_rows + ROW_HALO, :]),
        (1, sP.at[base1 + half_rows - ROW_HALO : base1 + half_rows, :], s1.at[ROWS_PAD:base_w, :]),
        (-1, gP.at[base1 : base1 + ROW_HALO, :], g1.at[base_w + half_rows : base_w + half_rows + ROW_HALO, :]),
        (1, gP.at[base1 + half_rows - ROW_HALO : base1 + half_rows, :], g1.at[ROWS_PAD:base_w, :]),
    )

    def row_copy(n, dx):
        _, source, target = row_moves[n]
        return pltpu.make_async_remote_copy(
            src_ref=source, dst_ref=target, send_sem=row_send.at[n], recv_sem=row_recv.at[n],
            device_id=(gx + dx, gy), device_id_type=MESH,
        )

    def rows_start(which):
        for n in which:
            dx = row_moves[n][0]
            @pl.when(inside(dx, 0))
            def _():
                row_copy(n, dx).start()

    def halved():
        pairs = get_strips(fine_add, pl.ds(0, ext1, 2)) + get_strips(fine_add, pl.ds(1, ext1, 2))
        return 0.25 * exact_dot(pairs, down0[...])

    put_strips(fine_add, slice(0, ext), sE[...])
    sP[near1, :] = halved()
    rows_start((0, 1))
    chunk = 16
    for lo in range(0, ext, chunk):
        at = slice(lo, lo + chunk)
        wE[at, :] = weight(sE[at, :], lo - base, rows, cols, half, 0)
    for lo in range(ROWS_PAD, ext - ROWS_PAD, 8):
        at = slice(lo, lo + 8)
        vA[at, :] = wE[at, :] * gE[at, :]
    sweep_block(vA, vB, gE, wE, 0)
    put_strips(fine_add, slice(0, ROWS_PAD), zero_tile)
    put_strips(fine_add, slice(ext - ROWS_PAD, ext), zero_tile)
    residual_block(vB, fine_add, gE, sE, 0)
    gP[near1, :] = halved()
    wP[near1, :] = weight(sP[near1, :], ROWS_PAD - base1, half_rows, cols // 2, half // 2, 1)
    aP[near1, :] = wP[near1, :] * gP[near1, :]
    sweep_block(aP, bP, gP, wP, 1)
    residual_block(bP, r1, gP, sP, 1, (base1, base1 + half_rows))
    rbuf[1, me] = pack_level2(r1)
    gather_start(1)
    rows_start((2, 3))

    block = (lane_e[0:8] // 16)

    def unpack(turn, target):
        for x in range(gx_count):
            for u in range(gy_count // 8):
                for tl in range(2):
                    tiles = [rbuf[turn, x * gy_count + u * 8 + g, tl * 8 : tl * 8 + 8, :] for g in range(8)]
                    for bit in (1, 2, 4):
                        keep = (block & bit) == 0
                        fresh = list(tiles)
                        for g in range(8):
                            if g & bit == 0:
                                lo, hi = tiles[g], tiles[g | bit]
                                fresh[g] = jnp.where(keep, lo, pltpu.roll(hi, 16 * bit, 1))
                                fresh[g | bit] = jnp.where(keep, pltpu.roll(lo, lanes - 16 * bit, 1), hi)
                        tiles = fresh
                    for b in range(8):
                        t, r = (b // 4) * 2 + tl, b % 4
                        target[t * 4 + r, 8 * x : 8 * x + 8, u * lanes : (u + 1) * lanes] = tiles[b]

    lane_q = iota((p_count, q_count), 1)
    rows_q = slice(8, 8 + p_count)

    def sides(v, n, t, r):
        mid = v[t * n + r, rows_q, :]
        if t > 0:
            north = v[(t - 1) * n + r, rows_q, :]
        else:
            north = v[(n - 1) * n + r, 7 : 7 + p_count, :]
        if t < n - 1:
            south = v[(t + 1) * n + r, rows_q, :]
        else:
            south = v[r, 9 : 9 + p_count, :]
        if r > 0:
            west = v[t * n + r - 1, rows_q, :]
        else:
            west = jnp.where(lane_q == 0, 0.0, pltpu.roll(v[t * n + n - 1, rows_q, :], 1, 1))
        if r < n - 1:
            east = v[t * n + r + 1, rows_q, :]
        else:
            east = jnp.where(
                lane_q == q_count - 1, 0.0, pltpu.roll(v[t * n, rows_q, :], q_count - 1, 1)
            )
        return mid, (north + south) + (west + east)

    level_refs = {2: (s2, w2, g2, a2, b2, 4), 3: (s3, w3, g3, a3, b3, 2), 4: (s4, w4, g4, a4, None, 1)}

    def sweep(level, v, out):
        s, w, g, _, _, n = level_refs[level]
        for t in range(n):
            for r in range(n):
                i = t * n + r
                mid, beside = sides(v, n, t, r)
                out[i, rows_q, :] = (1.0 - DAMPING) * mid + w[i] * (g[i] + 4.0 ** (-level) * beside)

    def first_sweep(level, out):
        s, w, g, _, _, n = level_refs[level]
        for i in range(n * n):
            out[i, rows_q, :] = w[i] * g[i]

    def restricted(level, v):
        s, w, g, _, _, n = level_refs[level]
        coarse_g = level_refs[level + 1][2]
        for t in range(n // 2):
            for r in range(n // 2):
                sums = None
                for dt in range(2):
                    for dr in range(2):
                        i = (2 * t + dt) * n + 2 * r + dr
                        mid, beside = sides(v, n, 2 * t + dt, 2 * r + dr)
                        left = g[i] - (4.0 ** (-level) * (4.0 * mid - beside) + s[i] * mid)
                        sums = left if sums is None else sums + left
                coarse_g[t * (n // 2) + r] = 0.25 * sums

    def correct(level, v, e):
        n = level_refs[level][5]
        for t in range(n):
            for r in range(n):
                i = t * n + r
                v[i, rows_q, :] = v[i, rows_q, :] + e[(t // 2) * (n // 2) + r // 2, rows_q, :]

    def prepare(level):
        s, w, _, _, _, n = level_refs[level]
        for i in range(n * n):
            w[i] = DAMPING / (4.0 ** (1 - level) + s[i])
        if level < 4:
            coarse_s = level_refs[level + 1][0]
            m = n // 2
            for t in range(m):
                for r in range(m):
                    i = 2 * t * n + 2 * r
                    coarse_s[t * m + r] = 0.25 * ((s[i] + s[i + n]) + (s[i + 1] + s[i + n + 1]))

    def total_of(x):
        return jnp.sum(jnp.sum(x, axis=0, keepdims=True), axis=1, keepdims=True)

    gather_wait(0)
    unpack(0, s2)
    for level in (2, 3, 4):
        prepare(level)
    row_q = iota((p_count, q_count), 0)
    edges = jnp.where(row_q == 0, 1.0, 0.0) + jnp.where(row_q == p_count - 1, 1.0, 0.0)
    edges = edges + jnp.where(lane_q == 0, 1.0, 0.0) + jnp.where(lane_q == q_count - 1, 1.0, 0.0)
    unit4 = 4.0 ** (-4) * edges + s4[0]
    per_unit = 1.0 / total_of(unit4)

    def shifted(x, reach):
        out = {0: x}
        for k in range(1, reach + 1):
            out[k] = jnp.where(lane_q < q_count - k, pltpu.roll(x, q_count - k, 1), 0.0)
            out[-k] = jnp.where(lane_q >= k, pltpu.roll(x, k, 1), 0.0)
        return out

    reach4 = 2
    for k, values in shifted(4.0 ** (-4) * w4[0], reach4).items():
        hw4[k + reach4] = values
    for i in range(beside4.shape[0]):
        beside4[i, 0:8, :] = jnp.zeros((8, q_count), F32)
        beside4[i, 8 + p_count : 16 + p_count, :] = jnp.zeros((8, q_count), F32)

    def fused_sweeps(v, source, count):
        for turn in range(count):
            reach = count - 1 - turn
            new = {}
            for k in range(-reach, reach + 1):
                slot = (turn % 2) * 5 + k + reach4
                beside4[slot, rows_q, :] = v[k]
                along = beside4[slot, 7 : 7 + p_count, :] + beside4[slot, 9 : 9 + p_count, :]
                value = (1.0 - DAMPING) * v[k] + hw4[k + reach4] * ((v[k - 1] + v[k + 1]) + along)
                new[k] = value if source is None else value + source[k]
            v = new
        return v[0]

    def six_sweeps(v, source):
        return fused_sweeps(shifted(fused_sweeps(shifted(v, 3), source, 3), 3), source, 3)

    phi[0] = six_sweeps(jnp.ones((p_count, q_count), F32), None)
    phi[1] = six_sweeps(phi[0], None)
    kept = 1.0 - per_unit * total_of(unit4 * phi[0])

    def coarse(twice=False):
        source = shifted(w4[0] * g4[0], 3)
        v = fused_sweeps(source, source, 3)
        v = fused_sweeps(shifted(v, 2), source, 2)
        add = total_of(g4[0]) * per_unit
        if twice:
            again = add * kept - total_of(unit4 * v) * per_unit
            v = six_sweeps(v, source) + add * phi[1] + again * phi[0]
        else:
            v = v + add * phi[0]
        a4[0, rows_q, :] = v
        return a4

    def vcycle(level, v):
        if level == 4:
            return coarse()
        _, _, _, a, b, n = level_refs[level]
        if v is None:
            first_sweep(level, a)
            sweep(level, a, b)
            now, later = b, a
        else:
            later = b if v is a else a
            sweep(level, v, later)
            sweep(level, later, v)
            now = v
        restricted(level, now)
        correct(level, now, vcycle(level + 1, None))
        sweep(level, now, later)
        sweep(level, later, now)
        return now

    def fcycle(level):
        _, _, _, a, b, n = level_refs[level]
        first_sweep(level, a)
        sweep(level, a, b)
        restricted(level, b)
        if level == 3:
            e = coarse(True)
        else:
            e = vcycle(level + 1, fcycle(level + 1))
        correct(level, b, e)
        sweep(level, b, a)
        sweep(level, a, b)
        return b

    window = picked.shape[1] - 8
    lane_w, row_w = iota((window, lanes), 1), iota((window, lanes), 0)

    def in_domain(period):
        at_p, at_q = gx * 8 - 4 + row_w, gy * 16 - 8 + lane_w % period
        good = (at_p >= 0) & (at_p < p_count) & (at_q >= 0) & (at_q < q_count)
        return good & (lane_w % period < 32)

    def put_window(t, values):
        for a in range(2):
            put_strips(r1, pl.ds(ROWS_PAD + 2 * t + a, window, 8), values)

    def add_level2(e, v):
        for t in range(4):
            tiles = [e[t * 4 + r, pl.ds(pl.multiple_of(gx * 8, 8), 24), :] for r in range(4)]
            picked[t] = exact_dot(jnp.concatenate(tiles, 1), spread[...])
        for t in range(4):
            put_window(t, picked[t, 4 : 4 + window, :])
        v[wide1, :] = v[wide1, :] + get_strips(r1, wide1)

    def pack_window(source):
        parts = []
        for t in range(4):
            start = ROWS_PAD + 2 * t
            parts.append(
                get_strips(source, pl.ds(start, window, 8)) + get_strips(source, pl.ds(start + 1, window, 8))
            )
        means = 0.25 * exact_dot(jnp.concatenate(parts, 0), down_w[...])
        return [means[t * window : (t + 1) * window] for t in range(4)]

    def joined(x, unit):
        return x + pltpu.roll(x, lanes - unit, 1)

    def halved_window(tiles, unit):
        return [0.25 * joined(tiles[2 * t] + tiles[2 * t + 1], unit) for t in range(len(tiles) // 2)]

    def beside_window(v, unit):
        n = len(v)
        out = []
        for t in range(n):
            north = v[t - 1] if t > 0 else pltpu.roll(v[n - 1], 1, 0)
            south = v[t + 1] if t < n - 1 else pltpu.roll(v[0], window - 1, 0)
            west = jnp.where(lane_w < unit, pltpu.roll(v[t], unit + 1, 1), pltpu.roll(v[t], unit, 1))
            east = jnp.where(
                lane_w >= lanes - unit,
                pltpu.roll(v[t], lanes - unit - 1, 1), pltpu.roll(v[t], lanes - unit, 1),
            )
            out.append((north + south) + (west + east))
        return out

    window_refs = {2: (s2w, w2w, 32), 3: (s3w, w3w, 64)}

    def sweep_window(level, v, g):
        _, w, unit = window_refs[level]
        beside = beside_window(v, unit)
        return [
            (1.0 - DAMPING) * v[t] + w[t] * (g[t] + 4.0 ** (-level) * beside[t]) for t in range(len(v))
        ]

    def residual_window(level, v, g):
        s, _, unit = window_refs[level]
        beside = beside_window(v, unit)
        return [
            g[t] - (4.0 ** (-level) * (4.0 * v[t] - beside[t]) + s[t] * v[t]) for t in range(len(v))
        ]

    for n, (dx, _, _) in enumerate(row_moves):
        @pl.when(inside(-dx, 0))
        def _():
            row_copy(n, -dx).wait_recv()

    own1, own_w = slice(base1, base1 + half_rows), slice(base_w, base_w + half_rows)
    g1[own_w, :] = gP[own1, :]
    s1[own_w, :] = sP[own1, :]
    w1[wide1, :] = weight(s1[wide1, :], ROWS_PAD - base_w, half_rows, cols // 2, half // 2, 1)
    a1[wide1, :] = w1[wide1, :] * g1[wide1, :]
    sweep_block(a1, b1, g1, w1, 1)
    put_strips(r1, wide1, s1[wide1, :])
    tiles = pack_window(r1)
    for t in range(4):
        s2w[t] = tiles[t]
        w2w[t] = jnp.where(in_domain(32), DAMPING / (4.0 ** (-1) + tiles[t]), 0.0)
    tiles = halved_window(tiles, 32)
    for t in range(2):
        s3w[t] = tiles[t]
        w3w[t] = jnp.where(in_domain(64), DAMPING / (4.0 ** (-2) + tiles[t]), 0.0)

    def coarse_copy(peer):
        return pltpu.make_async_remote_copy(
            src_ref=cbuf.at[me], dst_ref=cbuf.at[me], send_sem=coarse_sems.at[0], recv_sem=coarse_sems.at[1],
            device_id=(peer // gy_count, lax.rem(peer, gy_count)), device_id_type=MESH,
        )

    def coarse_wait(n):
        others = cbuf.at[pl.ds(0, total - 1)]
        pltpu.make_async_copy(others, others, coarse_sems.at[n]).wait()

    gather_wait(1)
    unpack(1, g2)
    e = fcycle(2)
    e = vcycle(2, e)
    add_level2(e, b1)
    sweep_block(b1, a1, g1, w1, 1)
    sweep_block(a1, b1, g1, w1, 1)
    sweep_block(b1, a1, g1, w1, 1)
    sweep_block(a1, b1, g1, w1, 1)
    residual_block(b1, r1, g1, s1, 1)
    source2 = pack_window(r1)
    v2 = sweep_window(2, [w2w[t] * source2[t] for t in range(4)], source2)
    source3 = halved_window(residual_window(2, v2, source2), 32)
    v3 = sweep_window(3, [w3w[t] * source3[t] for t in range(2)], source3)
    source4 = halved_window(residual_window(3, v3, source3), 64)[0]
    place = lax.rem(gy, 8) * 16
    mine = pltpu.roll(source4[4:12], lax.rem(place + lanes - 8, lanes), 1)
    lane_c = iota((8, lanes), 1)
    cbuf[me] = jnp.where((lane_c >= place) & (lane_c < place + 16), mine, 0.0)

    @pl.loop(0, total - 1)
    def _(k):
        odd = lax.rem(k, 2)
        coarse_copy(lax.rem(me + total + total // 2 + odd * ((k + 1) // 2) - (1 - odd) * (k // 2), total)).start()

    gather_sent(0)
    gather_sent(1)
    for n, (dx, dy, source, target) in enumerate(sends):
        @pl.when(inside(dx, dy))
        def _():
            halo_copy(n, dx, dy, source, target).wait_send()
    for n, (dx, _, _) in enumerate(row_moves):
        @pl.when(inside(dx, 0))
        def _():
            row_copy(n, dx).wait_send()
    coarse_wait(1)
    for x in range(gx_count):
        for u in range(gy_count // 8):
            first = x * gy_count + u * 8
            pairs = [cbuf[first + k] + cbuf[first + k + 1] for k in range(0, 8, 2)]
            g4[0, x * 8 : x * 8 + 8, u * lanes : (u + 1) * lanes] = (pairs[0] + pairs[1]) + (pairs[2] + pairs[3])
    e = coarse()
    e = e[0, pl.ds(pl.multiple_of(gx * 8, 8), 24), :][4 : 4 + window]
    e = pltpu.roll(e, lax.rem(q_count + 8 - gy * 16 + q_count, q_count), 1)[:, 0:lanes]
    e = jnp.where(in_domain(lanes), e, 0.0)
    e = e + pltpu.roll(e, 64, 1)
    v3 = [v3[t] + e for t in range(2)]
    v3 = sweep_window(3, sweep_window(3, v3, source3), source3)
    e = [v3[t] + pltpu.roll(v3[t], 32, 1) for t in range(2)]
    v2 = [v2[t] + e[t // 2] for t in range(4)]
    v2 = sweep_window(2, sweep_window(2, v2, source2), source2)
    raised = exact_dot(jnp.concatenate(v2, 0), up_w[...])
    for t in range(4):
        put_window(t, raised[t * window : (t + 1) * window])
    b1[wide1, :] = b1[wide1, :] + get_strips(r1, wide1)
    near_w = (base_w - 8, base_w + half_rows + 8)
    sweep_block(b1, a1, g1, w1, 1, near_w)
    sweep_block(a1, b1, g1, w1, 1, near_w)
    raised = exact_dot(b1[slice(*near_w), :], up0[...])
    put_strips(fine_add, pl.ds(0, ext1, 2), raised)
    put_strips(fine_add, pl.ds(1, ext1, 2), raised)
    for lo in range(ROWS_PAD, ext - ROWS_PAD, 8):
        at = slice(lo, lo + 8)
        vB[at, :] = vB[at, :] + get_strips(fine_add, at)
    sweep_block(vB, vA, gE, wE, 0)
    sweep_block(vA, vB, gE, wE, 0)
    for lo in range(0, rows, 8):
        mid, beside = around(vB, base + lo, 8)
        at = slice(base + lo, base + lo + 8)
        left = gE[at, :] - ((4.0 * mid - beside) + sE[at, :] * mid)
        out_ref[0, lo : lo + 8, :] = mid[:, 0:cols]
        out_ref[1, lo : lo + 8, :] = left[:, 0:cols]

    coarse_wait(0)


def solution(mesh):
    gx_count, gy_count = mesh.shape["gx"], mesh.shape["gy"]
    total = gx_count * gy_count

    def body(right_side, shift):
        rows, cols = right_side.shape
        assert cols == 256 and rows == 128 and gy_count % 8 == 0
        ext, width = rows + 2 * (HALO + ROWS_PAD), cols + 128
        ext1, width1 = ext // 2 + 2 * ROWS_PAD, 256
        wide1 = rows // 2 + 2 * (ROW_HALO + ROWS_PAD)
        window = rows // 16 + 8
        p, q = rows // 16 * gx_count, cols // 16 * gy_count
        V = pltpu.VMEM
        dma = pltpu.SemaphoreType.DMA
        big = [V((ext, width), F32)] * 5 + [V((width // 128, ext, 128), F32)]
        one = [V((ext1, width1), F32)] * 5
        one += [V((wide1, width1), F32)] * 5 + [V((width1 // 128, wide1, 128), F32)]
        levels = []
        for n in (16, 4, 1):
            levels += [V((n, p, q), F32)] * 3 + [V((n, p + 16, q), F32)] * (2 if n > 1 else 1)
        scratch = (
            [V((rows, cols), F32)] * 2 + [dma((2,))]
            + big + one
            + [V((rows, 128), F32)] * 2 + [V((ext, 128), F32)] * 2
            + [V((width, width1), BF16), V((width1, width), BF16), V((width1, 128), BF16), V((4 * q, width1), BF16)]
            + [V((width1, 128), BF16), V((128, width1), BF16)]
            + [V((2, total, 16, 128), F32), V((total, 8, 128), F32)]
            + levels
            + [V((4, 24, width1), F32)]
            + [V((4, window, 128), F32)] * 2 + [V((2, window, 128), F32)] * 2
            + [V((5, p, q), F32), V((2, p, q), F32), V((10, p + 16, q), F32)]
            + [dma((10,)), dma((10,)), dma((4,)), dma((4,)), dma((2, total)), dma((2, total)), dma((2,))]
        )
        out = pltpu.VMEM((2,) + right_side.shape, F32)
        both = pl.pallas_call(
            functools.partial(kernel, gx_count, gy_count),
            out_shape=out,
            in_specs=[pl.BlockSpec(memory_space=pltpu.HBM)] * 2,
            out_specs=pl.BlockSpec(memory_space=pltpu.VMEM),
            scratch_shapes=scratch,
            compiler_params=pltpu.CompilerParams(
                collective_id=0, has_side_effects=True, vmem_limit_bytes=60*1024*1024
            ),
        )(right_side, shift)
        return both[0], both[1]

    spec = P("gx", "gy")
    return jax.shard_map(body, mesh=mesh, in_specs=(spec, spec), out_specs=(spec, spec), check_vma=False)
```

```python
import functools

import jax
import jax.numpy as jnp
from jax import lax
from jax.experimental import pallas as pl
from jax.experimental.pallas import tpu as pltpu
from jax.sharding import PartitionSpec as P

DAMPING = 0.8
MESH = pl.DeviceIdType.MESH
F32 = jnp.float32
BF16 = jnp.bfloat16

ROWS_PAD = 8
HALO = 8
ROW_HALO = 32


def iota(shape, dim):
    return lax.broadcasted_iota(jnp.int32, shape, dim)


def put_strips(ref, at, values):
    for k in range(ref.shape[0]):
        ref[k, at, :] = values[:, k * 128 : (k + 1) * 128]


def get_strips(ref, at, count=None):
    return jnp.concatenate([ref[k, at, :] for k in range(count or ref.shape[0])], 1)


def exact_dot(values, selector):
    first = values.astype(BF16)
    rest = values - first.astype(F32)
    second = rest.astype(BF16)
    third = (rest - second.astype(F32)).astype(BF16)
    dot = functools.partial(jnp.dot, preferred_element_type=F32)
    return dot(first, selector) + (dot(second, selector) + dot(third, selector))


def kernel(
    gx_count, gy_count, g_hbm, s_hbm, out_ref,
    g_ref, s_ref, load_sem,
    gE, sE, wE, vA, vB, fine_add,
    gP, sP, wP, aP, bP,
    g1, s1, w1, a1, b1, r1,
    send_l, send_r, recv_l, recv_r,
    down0, up0, down1, spread, down_w, up_w,
    rbuf, cbuf, s2, w2, g2, a2, b2, s3, w3, g3, a3, b3, s4, w4, g4, a4, picked,
    s2w, w2w, s3w, w3w, hw4, phi, beside4,
    halo_send, halo_recv, row_send, row_recv, all_send, all_recv, coarse_sems, row_wave,
):
    gx, gy = lax.axis_index("gx"), lax.axis_index("gy")
    total = gx_count * gy_count
    me = gx * gy_count + gy
    rows, cols = g_hbm.shape
    base = ROWS_PAD + HALO
    base1 = ROWS_PAD + (ROWS_PAD + HALO) // 2
    ext, width = gE.shape
    ext1, width1 = ext // 2, g1.shape[1]
    half_rows = rows // 2
    base_w = ROWS_PAD + ROW_HALO
    near1 = slice(ROWS_PAD, ROWS_PAD + ext1)
    wide1 = slice(ROWS_PAD, base_w + half_rows + ROW_HALO)
    lanes = 128

    load_g = pltpu.make_async_copy(g_hbm, g_ref, load_sem.at[0])
    load_s = pltpu.make_async_copy(s_hbm, s_ref, load_sem.at[1])
    load_g.start()
    load_s.start()
    zero_halo = jnp.zeros((base, width), F32)
    for ref in (gE, sE):
        ref[0:base, :] = zero_halo
        ref[base + rows : ext, :] = zero_halo
    for ref in (recv_l, recv_r):
        ref[...] = jnp.zeros(ref.shape, F32)
    for ref in (g1, s1):
        ref[0:base_w, :] = jnp.zeros((base_w, width1), F32)
        ref[base_w + half_rows :, :] = jnp.zeros((base_w, width1), F32)
    def inside(dx, dy):
        ok = None
        for step, at, count in ((dx, gx, gx_count), (dy, gy, gy_count)):
            if step:
                here = (at > 0) if step < 0 else (at < count - 1)
                ok = here if ok is None else ok & here
        return ok

    def wrap(at, step, count):
        return lax.rem(at + count + step, count)

    def each(count, body):
        if count <= 64:
            for j in range(1, count):
                body(j)
        else:
            pl.loop(1, count)(body)

    barrier = pltpu.get_barrier_semaphore()
    beyond = [(dx, dy) for dx in (-1, 1) for dy in (0, -1, 1)]

    def greet(x, y):
        pl.semaphore_signal(barrier, inc=1, device_id=(x, y), device_id_type=MESH)

    for dx, dy in beyond:
        @pl.when(inside(dx, dy))
        def _():
            greet(gx + dx, gy + dy)

    each(gy_count, lambda k: greet(gx, wrap(gy, k, gy_count)))

    lane = iota((rows, lanes), 1)
    half = lanes // 2
    l0 = iota((width, width1), 0)
    col0 = jnp.where(l0 < cols + half, l0, l0 - width)
    down0[...] = jnp.where(
        ((col0 + 2 * width1) // 2) % width1 == iota((width, width1), 1), 1.0, 0.0
    ).astype(BF16)
    l0 = iota((width1, width), 1)
    col0 = jnp.where(l0 < cols + half, l0, l0 - width)
    up0[...] = jnp.where(
        ((col0 + 2 * width1) // 2) % width1 == iota((width1, width), 0), 1.0, 0.0
    ).astype(BF16)
    l1 = iota((width1, lanes), 0)
    j2 = l1 // 2
    place = (j2 % 4) * 16 + j2 // 4
    down1[...] = jnp.where(
        (l1 < lanes) & (iota((width1, lanes), 1) % half == place), 1.0, 0.0
    ).astype(BF16)
    q_count = s2.shape[2]
    p_count = s2.shape[1]
    m1 = iota((q_count, width1), 1)
    col1 = jnp.where(m1 < lanes + half // 2, m1, m1 - width1)
    wide = gy * half + (col1 + 512) // 2 - 256
    for r in range(4):
        spread[r * q_count : (r + 1) * q_count, :] = jnp.where(
            wide == 4 * iota((q_count, width1), 0) + r, 1.0, 0.0
        ).astype(BF16)

    load_g.wait()
    load_s.wait()
    send_l[...] = jnp.where(lane < half, g_ref[:, 0:lanes], pltpu.roll(s_ref[:, 0:lanes], half, 1))
    send_r[...] = jnp.where(
        lane < half, pltpu.roll(s_ref[:, cols - lanes : cols], half, 1), g_ref[:, cols - lanes : cols]
    )

    l1 = iota((width1, lanes), 0)
    at2 = (jnp.where(l1 < lanes + half // 2, l1, l1 - width1) + 2 * lanes) // 2
    at4 = at2 // 4 - 24
    down_w[...] = jnp.where(
        (at4 >= 0) & (at4 < 32) & (iota((width1, lanes), 1) == (at2 % 4) * 32 + at4), 1.0, 0.0
    ).astype(BF16)
    l1 = iota((lanes, width1), 1)
    at2 = (jnp.where(l1 < lanes + half // 2, l1, l1 - width1) + 2 * lanes) // 2
    at4 = at2 // 4 - 24
    up_w[...] = jnp.where(
        (at4 >= 0) & (at4 < 32) & (iota((lanes, width1), 0) == (at2 % 4) * 32 + at4), 1.0, 0.0
    ).astype(BF16)

    def pack_level2(source):
        parts = []
        for t in range(4):
            start = base1 + 2 * t
            parts.append(
                get_strips(source, pl.ds(start, 8, 8)) + get_strips(source, pl.ds(start + 1, 8, 8))
            )
        means = 0.25 * exact_dot(jnp.concatenate(parts, 0), down1[...])
        low = iota((16, lanes), 1) < half
        return jnp.where(low, means[0:16], means[16:32])

    own_strips = cols // lanes
    for k in range(own_strips):
        fine_add[k, base : base + rows, :] = s_ref[:, k * lanes : (k + 1) * lanes]
    own = get_strips(fine_add, pl.ds(base, half_rows, 2), own_strips)
    own = own + get_strips(fine_add, pl.ds(base + 1, half_rows, 2), own_strips)
    put_strips(r1, slice(base1, base1 + half_rows), 0.25 * exact_dot(own, down0[0:cols, :]))
    rbuf[0, me] = pack_level2(r1)
    gE[base : base + rows, 0:cols] = g_ref[...]
    sE[base : base + rows, 0:cols] = s_ref[...]

    def beside_count(at, count):
        return (at + count - 1) // count + 1 - (at + 1) // count

    pl.semaphore_wait(
        barrier, gy_count - 1 + beside_count(gx, gx_count) * (1 + beside_count(gy, gy_count))
    )

    top, bottom = slice(0, HALO), slice(rows - HALO, rows)
    above, below = slice(ROWS_PAD, base), slice(base + rows, base + rows + HALO)
    middle = slice(base, base + rows)
    sends = (
        (0, -1, send_l, recv_r.at[middle, :]),
        (0, 1, send_r, recv_l.at[middle, :]),
        (-1, -1, send_l.at[top, :], recv_r.at[below, :]),
        (1, -1, send_l.at[bottom, :], recv_r.at[above, :]),
        (-1, 1, send_r.at[top, :], recv_l.at[below, :]),
        (1, 1, send_r.at[bottom, :], recv_l.at[above, :]),
        (-1, 0, g_ref.at[top, :], gE.at[below, 0:cols]),
        (-1, 0, s_ref.at[top, :], sE.at[below, 0:cols]),
        (1, 0, g_ref.at[bottom, :], gE.at[above, 0:cols]),
        (1, 0, s_ref.at[bottom, :], sE.at[above, 0:cols]),
    )

    def halo_copy(n, dx, dy, source, target):
        return pltpu.make_async_remote_copy(
            src_ref=source, dst_ref=target, send_sem=halo_send.at[n], recv_sem=halo_recv.at[n],
            device_id=(gx + dx, gy + dy), device_id_type=MESH,
        )

    for n, (dx, dy, source, target) in enumerate(sends):
        @pl.when(inside(dx, dy))
        def _():
            halo_copy(n, dx, dy, source, target).start()

    def pass_on(n, step):
        @pl.when(inside(-step, 0))
        def _():
            pl.semaphore_wait(row_wave.at[n], 1)

        @pl.when(inside(step, 0))
        def _():
            pl.semaphore_signal(row_wave.at[n], inc=1, device_id=(gx + step, gy), device_id_type=MESH)

    @pl.when(gx < gx_count // 2)
    def _():
        pass_on(0, 1)
        pass_on(1, -1)

    @pl.when(gx >= gx_count // 2)
    def _():
        pass_on(1, -1)
        pass_on(0, 1)

    core = lax.rem(gy, 2)
    per_row = gy_count // 2
    chips = total // 2
    partner = (gx, gy + 1 - 2 * core)

    def zigzag(j, count):
        odd = j % 2
        return odd * ((j + 1) // 2) + (1 - odd) * (count - j // 2)

    def block_copy(turn, n, slot, peer):
        return pltpu.make_async_remote_copy(
            src_ref=rbuf.at[turn, slot], dst_ref=rbuf.at[turn, slot],
            send_sem=all_send.at[turn, n], recv_sem=all_recv.at[turn, slot],
            device_id=peer, device_id_type=MESH,
        )

    def direct(turn, j):
        n = zigzag(j, chips)
        peer = (wrap(gx, n // per_row, gx_count), wrap(gy, 2 * (n % per_row), gy_count))
        return block_copy(turn, j, me, peer)

    def sender(j):
        n = zigzag(j, chips)
        return wrap(gx, -(n // per_row), gx_count) * gy_count + wrap(gy, -2 * (n % per_row), gy_count)

    def onward(turn, j):
        return block_copy(turn, chips + j, sender(j), partner)

    def gather_start(turn):
        block_copy(turn, 0, me, partner).start()
        each(chips, lambda j: direct(turn, chips - j).start())

    def gather_wait(turn):
        def pass_block(j):
            copy = onward(turn, j)
            copy.wait_recv()
            copy.start()

        each(chips, pass_block)
        block_copy(turn, 0, me + 1 - 2 * core, partner).wait_recv()
        each(chips, lambda j: block_copy(turn, chips + j, sender(j) + 1 - 2 * core, partner).wait_recv())

    def gather_sent(turn):
        def sent(j):
            direct(turn, j).wait_send()
            onward(turn, j).wait_send()

        block_copy(turn, 0, me, partner).wait_send()
        each(chips, sent)

    gather_start(0)
    zero_tile = jnp.zeros((ROWS_PAD, width), F32)
    for ref in (vA, vB):
        ref[0:ROWS_PAD, :] = zero_tile
        ref[ext - ROWS_PAD : ext, :] = zero_tile
    for ref in (aP, bP, a1, b1):
        ref[0:ROWS_PAD, :] = jnp.zeros((ROWS_PAD, width1), F32)
        ref[ref.shape[0] - ROWS_PAD :, :] = jnp.zeros((ROWS_PAD, width1), F32)
    for ref in (a2, b2, a3, b3, a4):
        for i in range(ref.shape[0]):
            ref[i, 0:8, :] = jnp.zeros((8, q_count), F32)
            ref[i, 8 + p_count : 16 + p_count, :] = jnp.zeros((8, q_count), F32)

    for n, (dx, dy, source, target) in enumerate(sends):
        @pl.when(inside(-dx, -dy))
        def _():
            halo_copy(n, -dx, -dy, source, target).wait_recv()

    lane_e = iota((ext, lanes), 1)
    gE[:, cols:width] = jnp.where(lane_e < half, recv_r[...], recv_l[...])
    sE[:, cols:width] = pltpu.roll(jnp.where(lane_e < half, recv_l[...], recv_r[...]), half, 1)

    def weight(shifts, first_row, own_rows, own_cols, split, level):
        shape = shifts.shape
        at_row = gx * own_rows + iota(shape, 0) + first_row
        lane_at = iota(shape, 1)
        at_col = gy * own_cols + jnp.where(lane_at < own_cols + split, lane_at, lane_at - shape[1])
        good = (at_row >= 0) & (at_row < gx_count * own_rows)
        good = good & (at_col >= 0) & (at_col < gy_count * own_cols)
        return jnp.where(good, DAMPING / (4.0 ** (1 - level) + shifts), 0.0)

    def around(v, lo, size):
        span = v.shape[1]
        mid = v[lo : lo + size, :]
        beside = pltpu.roll(mid, 1, 1) + pltpu.roll(mid, span - 1, 1)
        return mid, beside + (v[lo - 1 : lo - 1 + size, :] + v[lo + 1 : lo + 1 + size, :])

    def sweep_block(v, out, g, w, level, span=None):
        scale = 4.0 ** (-level)
        for lo in range(*(span or (ROWS_PAD, v.shape[0] - ROWS_PAD)), 8):
            mid, beside = around(v, lo, 8)
            at = slice(lo, lo + 8)
            out[at, :] = (1.0 - DAMPING) * mid + w[at, :] * (g[at, :] + scale * beside)

    def residual_block(v, out, g, s, level, span=None):
        scale = 4.0 ** (-level)
        for lo in range(*(span or (ROWS_PAD, v.shape[0] - ROWS_PAD)), 8):
            mid, beside = around(v, lo, 8)
            at = slice(lo, lo + 8)
            put_strips(out, at, g[at, :] - (scale * (4.0 * mid - beside) + s[at, :] * mid))

    row_moves = (
        (-1, sP.at[base1 : base1 + ROW_HALO, :], s1.at[base_w + half_rows : base_w + half_rows + ROW_HALO, :]),
        (1, sP.at[base1 + half_rows - ROW_HALO : base1 + half_rows, :], s1.at[ROWS_PAD:base_w, :]),
        (-1, gP.at[base1 : base1 + ROW_HALO, :], g1.at[base_w + half_rows : base_w + half_rows + ROW_HALO, :]),
        (1, gP.at[base1 + half_rows - ROW_HALO : base1 + half_rows, :], g1.at[ROWS_PAD:base_w, :]),
    )

    def row_copy(n, dx):
        _, source, target = row_moves[n]
        return pltpu.make_async_remote_copy(
            src_ref=source, dst_ref=target, send_sem=row_send.at[n], recv_sem=row_recv.at[n],
            device_id=(gx + dx, gy), device_id_type=MESH,
        )

    def rows_start(which):
        for n in which:
            dx = row_moves[n][0]
            @pl.when(inside(dx, 0))
            def _():
                row_copy(n, dx).start()

    def halved():
        pairs = get_strips(fine_add, pl.ds(0, ext1, 2)) + get_strips(fine_add, pl.ds(1, ext1, 2))
        return 0.25 * exact_dot(pairs, down0[...])

    put_strips(fine_add, slice(0, ext), sE[...])
    sP[near1, :] = halved()
    rows_start((0, 1))
    chunk = 16
    for lo in range(0, ext, chunk):
        at = slice(lo, lo + chunk)
        wE[at, :] = weight(sE[at, :], lo - base, rows, cols, half, 0)
    for lo in range(ROWS_PAD, ext - ROWS_PAD, 8):
        at = slice(lo, lo + 8)
        vA[at, :] = wE[at, :] * gE[at, :]
    sweep_block(vA, vB, gE, wE, 0)
    put_strips(fine_add, slice(0, ROWS_PAD), zero_tile)
    put_strips(fine_add, slice(ext - ROWS_PAD, ext), zero_tile)
    residual_block(vB, fine_add, gE, sE, 0)
    gP[near1, :] = halved()
    wP[near1, :] = weight(sP[near1, :], ROWS_PAD - base1, half_rows, cols // 2, half // 2, 1)
    aP[near1, :] = wP[near1, :] * gP[near1, :]
    sweep_block(aP, bP, gP, wP, 1)
    residual_block(bP, r1, gP, sP, 1, (base1, base1 + half_rows))
    rbuf[1, me] = pack_level2(r1)
    gather_start(1)
    rows_start((2, 3))

    block = (lane_e[0:8] // 16)

    def unpack(turn, target):
        for x in range(gx_count):
            for u in range(gy_count // 8):
                for tl in range(2):
                    tiles = [rbuf[turn, x * gy_count + u * 8 + g, tl * 8 : tl * 8 + 8, :] for g in range(8)]
                    for bit in (1, 2, 4):
                        keep = (block & bit) == 0
                        fresh = list(tiles)
                        for g in range(8):
                            if g & bit == 0:
                                lo, hi = tiles[g], tiles[g | bit]
                                fresh[g] = jnp.where(keep, lo, pltpu.roll(hi, 16 * bit, 1))
                                fresh[g | bit] = jnp.where(keep, pltpu.roll(lo, lanes - 16 * bit, 1), hi)
                        tiles = fresh
                    for b in range(8):
                        t, r = (b // 4) * 2 + tl, b % 4
                        target[t * 4 + r, 8 * x : 8 * x + 8, u * lanes : (u + 1) * lanes] = tiles[b]

    lane_q = iota((p_count, q_count), 1)
    rows_q = slice(8, 8 + p_count)

    def sides(v, n, t, r):
        mid = v[t * n + r, rows_q, :]
        if t > 0:
            north = v[(t - 1) * n + r, rows_q, :]
        else:
            north = v[(n - 1) * n + r, 7 : 7 + p_count, :]
        if t < n - 1:
            south = v[(t + 1) * n + r, rows_q, :]
        else:
            south = v[r, 9 : 9 + p_count, :]
        if r > 0:
            west = v[t * n + r - 1, rows_q, :]
        else:
            west = jnp.where(lane_q == 0, 0.0, pltpu.roll(v[t * n + n - 1, rows_q, :], 1, 1))
        if r < n - 1:
            east = v[t * n + r + 1, rows_q, :]
        else:
            east = jnp.where(
                lane_q == q_count - 1, 0.0, pltpu.roll(v[t * n, rows_q, :], q_count - 1, 1)
            )
        return mid, (north + south) + (west + east)

    level_refs = {2: (s2, w2, g2, a2, b2, 4), 3: (s3, w3, g3, a3, b3, 2), 4: (s4, w4, g4, a4, None, 1)}

    def sweep(level, v, out):
        s, w, g, _, _, n = level_refs[level]
        for t in range(n):
            for r in range(n):
                i = t * n + r
                mid, beside = sides(v, n, t, r)
                out[i, rows_q, :] = (1.0 - DAMPING) * mid + w[i] * (g[i] + 4.0 ** (-level) * beside)

    def first_sweep(level, out):
        s, w, g, _, _, n = level_refs[level]
        for i in range(n * n):
            out[i, rows_q, :] = w[i] * g[i]

    def restricted(level, v):
        s, w, g, _, _, n = level_refs[level]
        coarse_g = level_refs[level + 1][2]
        for t in range(n // 2):
            for r in range(n // 2):
                sums = None
                for dt in range(2):
                    for dr in range(2):
                        i = (2 * t + dt) * n + 2 * r + dr
                        mid, beside = sides(v, n, 2 * t + dt, 2 * r + dr)
                        left = g[i] - (4.0 ** (-level) * (4.0 * mid - beside) + s[i] * mid)
                        sums = left if sums is None else sums + left
                coarse_g[t * (n // 2) + r] = 0.25 * sums

    def correct(level, v, e):
        n = level_refs[level][5]
        for t in range(n):
            for r in range(n):
                i = t * n + r
                v[i, rows_q, :] = v[i, rows_q, :] + e[(t // 2) * (n // 2) + r // 2, rows_q, :]

    def prepare(level):
        s, w, _, _, _, n = level_refs[level]
        for i in range(n * n):
            w[i] = DAMPING / (4.0 ** (1 - level) + s[i])
        if level < 4:
            coarse_s = level_refs[level + 1][0]
            m = n // 2
            for t in range(m):
                for r in range(m):
                    i = 2 * t * n + 2 * r
                    coarse_s[t * m + r] = 0.25 * ((s[i] + s[i + n]) + (s[i + 1] + s[i + n + 1]))

    def total_of(x):
        return jnp.sum(jnp.sum(x, axis=0, keepdims=True), axis=1, keepdims=True)

    gather_wait(0)
    unpack(0, s2)
    for level in (2, 3, 4):
        prepare(level)
    row_q = iota((p_count, q_count), 0)
    edges = jnp.where(row_q == 0, 1.0, 0.0) + jnp.where(row_q == p_count - 1, 1.0, 0.0)
    edges = edges + jnp.where(lane_q == 0, 1.0, 0.0) + jnp.where(lane_q == q_count - 1, 1.0, 0.0)
    unit4 = 4.0 ** (-4) * edges + s4[0]
    per_unit = 1.0 / total_of(unit4)

    def shifted(x, reach):
        out = {0: x}
        for k in range(1, reach + 1):
            out[k] = jnp.where(lane_q < q_count - k, pltpu.roll(x, q_count - k, 1), 0.0)
            out[-k] = jnp.where(lane_q >= k, pltpu.roll(x, k, 1), 0.0)
        return out

    reach4 = 2
    for k, values in shifted(4.0 ** (-4) * w4[0], reach4).items():
        hw4[k + reach4] = values
    for i in range(beside4.shape[0]):
        beside4[i, 0:8, :] = jnp.zeros((8, q_count), F32)
        beside4[i, 8 + p_count : 16 + p_count, :] = jnp.zeros((8, q_count), F32)

    def fused_sweeps(v, source, count):
        for turn in range(count):
            reach = count - 1 - turn
            new = {}
            for k in range(-reach, reach + 1):
                slot = (turn % 2) * 5 + k + reach4
                beside4[slot, rows_q, :] = v[k]
                along = beside4[slot, 7 : 7 + p_count, :] + beside4[slot, 9 : 9 + p_count, :]
                value = (1.0 - DAMPING) * v[k] + hw4[k + reach4] * ((v[k - 1] + v[k + 1]) + along)
                new[k] = value if source is None else value + source[k]
            v = new
        return v[0]

    def six_sweeps(v, source):
        return fused_sweeps(shifted(fused_sweeps(shifted(v, 3), source, 3), 3), source, 3)

    phi[0] = six_sweeps(jnp.ones((p_count, q_count), F32), None)
    phi[1] = six_sweeps(phi[0], None)
    kept = 1.0 - per_unit * total_of(unit4 * phi[0])

    def coarse(twice=False):
        source = shifted(w4[0] * g4[0], 3)
        v = fused_sweeps(source, source, 3)
        v = fused_sweeps(shifted(v, 2), source, 2)
        add = total_of(g4[0]) * per_unit
        if twice:
            again = add * kept - total_of(unit4 * v) * per_unit
            v = six_sweeps(v, source) + add * phi[1] + again * phi[0]
        else:
            v = v + add * phi[0]
        a4[0, rows_q, :] = v
        return a4

    def vcycle(level, v):
        if level == 4:
            return coarse()
        _, _, _, a, b, n = level_refs[level]
        if v is None:
            first_sweep(level, a)
            sweep(level, a, b)
            now, later = b, a
        else:
            later = b if v is a else a
            sweep(level, v, later)
            sweep(level, later, v)
            now = v
        restricted(level, now)
        correct(level, now, vcycle(level + 1, None))
        sweep(level, now, later)
        sweep(level, later, now)
        return now

    def fcycle(level):
        _, _, _, a, b, n = level_refs[level]
        first_sweep(level, a)
        sweep(level, a, b)
        restricted(level, b)
        if level == 3:
            e = coarse(True)
        else:
            e = vcycle(level + 1, fcycle(level + 1))
        correct(level, b, e)
        sweep(level, b, a)
        sweep(level, a, b)
        return b

    window = picked.shape[1] - 8
    lane_w, row_w = iota((window, lanes), 1), iota((window, lanes), 0)

    def in_domain(period):
        at_p, at_q = gx * 8 - 4 + row_w, gy * 16 - 8 + lane_w % period
        good = (at_p >= 0) & (at_p < p_count) & (at_q >= 0) & (at_q < q_count)
        return good & (lane_w % period < 32)

    def put_window(t, values):
        for a in range(2):
            put_strips(r1, pl.ds(ROWS_PAD + 2 * t + a, window, 8), values)

    def add_level2(e, v):
        for t in range(4):
            tiles = [e[t * 4 + r, pl.ds(pl.multiple_of(gx * 8, 8), 24), :] for r in range(4)]
            picked[t] = exact_dot(jnp.concatenate(tiles, 1), spread[...])
        for t in range(4):
            put_window(t, picked[t, 4 : 4 + window, :])
        v[wide1, :] = v[wide1, :] + get_strips(r1, wide1)

    def pack_window(source):
        parts = []
        for t in range(4):
            start = ROWS_PAD + 2 * t
            parts.append(
                get_strips(source, pl.ds(start, window, 8)) + get_strips(source, pl.ds(start + 1, window, 8))
            )
        means = 0.25 * exact_dot(jnp.concatenate(parts, 0), down_w[...])
        return [means[t * window : (t + 1) * window] for t in range(4)]

    def joined(x, unit):
        return x + pltpu.roll(x, lanes - unit, 1)

    def halved_window(tiles, unit):
        return [0.25 * joined(tiles[2 * t] + tiles[2 * t + 1], unit) for t in range(len(tiles) // 2)]

    def beside_window(v, unit):
        n = len(v)
        out = []
        for t in range(n):
            north = v[t - 1] if t > 0 else pltpu.roll(v[n - 1], 1, 0)
            south = v[t + 1] if t < n - 1 else pltpu.roll(v[0], window - 1, 0)
            west = jnp.where(lane_w < unit, pltpu.roll(v[t], unit + 1, 1), pltpu.roll(v[t], unit, 1))
            east = jnp.where(
                lane_w >= lanes - unit,
                pltpu.roll(v[t], lanes - unit - 1, 1), pltpu.roll(v[t], lanes - unit, 1),
            )
            out.append((north + south) + (west + east))
        return out

    window_refs = {2: (s2w, w2w, 32), 3: (s3w, w3w, 64)}

    def sweep_window(level, v, g):
        _, w, unit = window_refs[level]
        beside = beside_window(v, unit)
        return [
            (1.0 - DAMPING) * v[t] + w[t] * (g[t] + 4.0 ** (-level) * beside[t]) for t in range(len(v))
        ]

    def residual_window(level, v, g):
        s, _, unit = window_refs[level]
        beside = beside_window(v, unit)
        return [
            g[t] - (4.0 ** (-level) * (4.0 * v[t] - beside[t]) + s[t] * v[t]) for t in range(len(v))
        ]

    for n, (dx, _, _) in enumerate(row_moves):
        @pl.when(inside(-dx, 0))
        def _():
            row_copy(n, -dx).wait_recv()

    own1, own_w = slice(base1, base1 + half_rows), slice(base_w, base_w + half_rows)
    g1[own_w, :] = gP[own1, :]
    s1[own_w, :] = sP[own1, :]
    w1[wide1, :] = weight(s1[wide1, :], ROWS_PAD - base_w, half_rows, cols // 2, half // 2, 1)
    a1[wide1, :] = w1[wide1, :] * g1[wide1, :]
    sweep_block(a1, b1, g1, w1, 1)
    put_strips(r1, wide1, s1[wide1, :])
    tiles = pack_window(r1)
    for t in range(4):
        s2w[t] = tiles[t]
        w2w[t] = jnp.where(in_domain(32), DAMPING / (4.0 ** (-1) + tiles[t]), 0.0)
    tiles = halved_window(tiles, 32)
    for t in range(2):
        s3w[t] = tiles[t]
        w3w[t] = jnp.where(in_domain(64), DAMPING / (4.0 ** (-2) + tiles[t]), 0.0)

    def coarse_send(k):
        n = zigzag(total - k, total)
        pltpu.make_async_remote_copy(
            src_ref=cbuf.at[me], dst_ref=cbuf.at[me], send_sem=coarse_sems.at[0], recv_sem=coarse_sems.at[1],
            device_id=(wrap(gx, n // gy_count, gx_count), wrap(gy, n % gy_count, gy_count)), device_id_type=MESH,
        ).start()

    def coarse_wait(n):
        others = cbuf.at[pl.ds(0, total - 1)]
        pltpu.make_async_copy(others, others, coarse_sems.at[n]).wait()

    gather_wait(1)
    unpack(1, g2)
    e = fcycle(2)
    e = vcycle(2, e)
    add_level2(e, b1)
    sweep_block(b1, a1, g1, w1, 1)
    sweep_block(a1, b1, g1, w1, 1)
    sweep_block(b1, a1, g1, w1, 1)
    sweep_block(a1, b1, g1, w1, 1)
    residual_block(b1, r1, g1, s1, 1)
    source2 = pack_window(r1)
    v2 = sweep_window(2, [w2w[t] * source2[t] for t in range(4)], source2)
    source3 = halved_window(residual_window(2, v2, source2), 32)
    v3 = sweep_window(3, [w3w[t] * source3[t] for t in range(2)], source3)
    source4 = halved_window(residual_window(3, v3, source3), 64)[0]
    place = lax.rem(gy, 8) * 16
    mine = pltpu.roll(source4[4:12], lax.rem(place + lanes - 8, lanes), 1)
    lane_c = iota((8, lanes), 1)
    cbuf[me] = jnp.where((lane_c >= place) & (lane_c < place + 16), mine, 0.0)

    each(total, coarse_send)
    gather_sent(0)
    gather_sent(1)
    for n, (dx, dy, source, target) in enumerate(sends):
        @pl.when(inside(dx, dy))
        def _():
            halo_copy(n, dx, dy, source, target).wait_send()
    for n, (dx, _, _) in enumerate(row_moves):
        @pl.when(inside(dx, 0))
        def _():
            row_copy(n, dx).wait_send()
    coarse_wait(1)
    for x in range(gx_count):
        for u in range(gy_count // 8):
            first = x * gy_count + u * 8
            pairs = [cbuf[first + k] + cbuf[first + k + 1] for k in range(0, 8, 2)]
            g4[0, x * 8 : x * 8 + 8, u * lanes : (u + 1) * lanes] = (pairs[0] + pairs[1]) + (pairs[2] + pairs[3])
    e = coarse()
    e = e[0, pl.ds(pl.multiple_of(gx * 8, 8), 24), :][4 : 4 + window]
    e = pltpu.roll(e, lax.rem(q_count + 8 - gy * 16 + q_count, q_count), 1)[:, 0:lanes]
    e = jnp.where(in_domain(lanes), e, 0.0)
    e = e + pltpu.roll(e, 64, 1)
    v3 = [v3[t] + e for t in range(2)]
    v3 = sweep_window(3, sweep_window(3, v3, source3), source3)
    e = [v3[t] + pltpu.roll(v3[t], 32, 1) for t in range(2)]
    v2 = [v2[t] + e[t // 2] for t in range(4)]
    v2 = sweep_window(2, sweep_window(2, v2, source2), source2)
    raised = exact_dot(jnp.concatenate(v2, 0), up_w[...])
    for t in range(4):
        put_window(t, raised[t * window : (t + 1) * window])
    b1[wide1, :] = b1[wide1, :] + get_strips(r1, wide1)
    near_w = (base_w - 8, base_w + half_rows + 8)
    sweep_block(b1, a1, g1, w1, 1, near_w)
    sweep_block(a1, b1, g1, w1, 1, near_w)
    raised = exact_dot(b1[slice(*near_w), :], up0[...])
    put_strips(fine_add, pl.ds(0, ext1, 2), raised)
    put_strips(fine_add, pl.ds(1, ext1, 2), raised)
    for lo in range(ROWS_PAD, ext - ROWS_PAD, 8):
        at = slice(lo, lo + 8)
        vB[at, :] = vB[at, :] + get_strips(fine_add, at)
    sweep_block(vB, vA, gE, wE, 0)
    sweep_block(vA, vB, gE, wE, 0)
    for lo in range(0, rows, 8):
        mid, beside = around(vB, base + lo, 8)
        at = slice(base + lo, base + lo + 8)
        left = gE[at, :] - ((4.0 * mid - beside) + sE[at, :] * mid)
        out_ref[0, lo : lo + 8, :] = mid[:, 0:cols]
        out_ref[1, lo : lo + 8, :] = left[:, 0:cols]

    coarse_wait(0)


def solution(mesh):
    gx_count, gy_count = mesh.shape["gx"], mesh.shape["gy"]
    total = gx_count * gy_count

    def body(right_side, shift):
        rows, cols = right_side.shape
        assert cols == 256 and rows == 128 and gy_count % 8 == 0
        ext, width = rows + 2 * (HALO + ROWS_PAD), cols + 128
        ext1, width1 = ext // 2 + 2 * ROWS_PAD, 256
        wide1 = rows // 2 + 2 * (ROW_HALO + ROWS_PAD)
        window = rows // 16 + 8
        p, q = rows // 16 * gx_count, cols // 16 * gy_count
        V = pltpu.VMEM
        dma = pltpu.SemaphoreType.DMA
        big = [V((ext, width), F32)] * 5 + [V((width // 128, ext, 128), F32)]
        one = [V((ext1, width1), F32)] * 5
        one += [V((wide1, width1), F32)] * 5 + [V((width1 // 128, wide1, 128), F32)]
        levels = []
        for n in (16, 4, 1):
            levels += [V((n, p, q), F32)] * 3 + [V((n, p + 16, q), F32)] * (2 if n > 1 else 1)
        scratch = (
            [V((rows, cols), F32)] * 2 + [dma((2,))]
            + big + one
            + [V((rows, 128), F32)] * 2 + [V((ext, 128), F32)] * 2
            + [V((width, width1), BF16), V((width1, width), BF16), V((width1, 128), BF16), V((4 * q, width1), BF16)]
            + [V((width1, 128), BF16), V((128, width1), BF16)]
            + [V((2, total, 16, 128), F32), V((total, 8, 128), F32)]
            + levels
            + [V((4, 24, width1), F32)]
            + [V((4, window, 128), F32)] * 2 + [V((2, window, 128), F32)] * 2
            + [V((5, p, q), F32), V((2, p, q), F32), V((10, p + 16, q), F32)]
            + [dma((10,)), dma((10,)), dma((4,)), dma((4,)), dma((2, total)), dma((2, total)), dma((2,))]
            + [pltpu.SemaphoreType.REGULAR((2,))]
        )
        out = pltpu.VMEM((2,) + right_side.shape, F32)
        both = pl.pallas_call(
            functools.partial(kernel, gx_count, gy_count),
            out_shape=out,
            in_specs=[pl.BlockSpec(memory_space=pltpu.HBM)] * 2,
            out_specs=pl.BlockSpec(memory_space=pltpu.VMEM),
            scratch_shapes=scratch,
            compiler_params=pltpu.CompilerParams(
                collective_id=0, has_side_effects=True, vmem_limit_bytes=60*1024*1024
            ),
        )(right_side, shift)
        return both[0], both[1]

    spec = P("gx", "gy")
    return jax.shard_map(body, mesh=mesh, in_specs=(spec, spec), out_specs=(spec, spec), check_vma=False)
```

```python
import functools

import jax
import jax.numpy as jnp
from jax import lax
from jax.experimental import pallas as pl
from jax.experimental.pallas import tpu as pltpu
from jax.sharding import PartitionSpec as P

DAMPING = 0.8
MESH = pl.DeviceIdType.MESH
F32 = jnp.float32
BF16 = jnp.bfloat16

ROWS_PAD = 8
HALO = 8
ROW_HALO = 32


def iota(shape, dim):
    return lax.broadcasted_iota(jnp.int32, shape, dim)


def put_strips(ref, at, values):
    for k in range(ref.shape[0]):
        ref[k, at, :] = values[:, k * 128 : (k + 1) * 128]


def get_strips(ref, at, count=None):
    return jnp.concatenate([ref[k, at, :] for k in range(count or ref.shape[0])], 1)


def exact_dot(values, selector):
    first = values.astype(BF16)
    rest = values - first.astype(F32)
    second = rest.astype(BF16)
    third = (rest - second.astype(F32)).astype(BF16)
    dot = functools.partial(jnp.dot, preferred_element_type=F32)
    return dot(first, selector) + (dot(second, selector) + dot(third, selector))


def kernel(
    gx_count, gy_count, g_hbm, s_hbm, out_ref,
    g_ref, s_ref, load_sem,
    gE, sE, wE, vA, vB, fine_add,
    gP, sP, wP, aP, bP,
    g1, s1, w1, a1, b1, r1,
    send_l, send_r, recv_l, recv_r,
    down0, up0, down1, spread, down_w, up_w,
    rbuf, cbuf, s2, w2, g2, a2, b2, s3, w3, g3, a3, b3, s4, w4, g4, a4, picked,
    s2w, w2w, s3w, w3w, hw4, phi, beside4,
    halo_send, halo_recv, row_send, row_recv, all_send, all_recv, coarse_sems, row_wave,
):
    gx, gy = lax.axis_index("gx"), lax.axis_index("gy")
    total = gx_count * gy_count
    me = gx * gy_count + gy
    rows, cols = g_hbm.shape
    base = ROWS_PAD + HALO
    base1 = ROWS_PAD + (ROWS_PAD + HALO) // 2
    ext, width = gE.shape
    ext1, width1 = ext // 2, g1.shape[1]
    half_rows = rows // 2
    base_w = ROWS_PAD + ROW_HALO
    near1 = slice(ROWS_PAD, ROWS_PAD + ext1)
    wide1 = slice(ROWS_PAD, base_w + half_rows + ROW_HALO)
    lanes = 128

    load_g = pltpu.make_async_copy(g_hbm, g_ref, load_sem.at[0])
    load_s = pltpu.make_async_copy(s_hbm, s_ref, load_sem.at[1])
    load_g.start()
    load_s.start()
    zero_halo = jnp.zeros((base, width), F32)
    for ref in (gE, sE):
        ref[0:base, :] = zero_halo
        ref[base + rows : ext, :] = zero_halo
    for ref in (recv_l, recv_r):
        ref[...] = jnp.zeros(ref.shape, F32)
    for ref in (g1, s1):
        ref[0:base_w, :] = jnp.zeros((base_w, width1), F32)
        ref[base_w + half_rows :, :] = jnp.zeros((base_w, width1), F32)
    def inside(dx, dy):
        ok = None
        for step, at, count in ((dx, gx, gx_count), (dy, gy, gy_count)):
            if step:
                here = (at > 0) if step < 0 else (at < count - 1)
                ok = here if ok is None else ok & here
        return ok

    def wrap(at, step, count):
        return lax.rem(at + count + step, count)

    def each(count, body):
        if count <= 64:
            for j in range(1, count):
                body(j)
        else:
            pl.loop(1, count)(body)

    barrier = pltpu.get_barrier_semaphore()
    corners = [(dx, dy) for dx in (-1, 1) for dy in (-1, 1)]

    def greet(x, y):
        pl.semaphore_signal(barrier, inc=1, device_id=(x, y), device_id_type=MESH)

    each(gx_count, lambda k: greet(wrap(gx, k, gx_count), gy))
    for dx, dy in corners:
        @pl.when(inside(dx, dy))
        def _():
            greet(gx + dx, gy + dy)

    each(gy_count, lambda k: greet(gx, wrap(gy, k, gy_count)))

    lane = iota((rows, lanes), 1)
    half = lanes // 2
    l0 = iota((width, width1), 0)
    col0 = jnp.where(l0 < cols + half, l0, l0 - width)
    down0[...] = jnp.where(
        ((col0 + 2 * width1) // 2) % width1 == iota((width, width1), 1), 1.0, 0.0
    ).astype(BF16)
    l0 = iota((width1, width), 1)
    col0 = jnp.where(l0 < cols + half, l0, l0 - width)
    up0[...] = jnp.where(
        ((col0 + 2 * width1) // 2) % width1 == iota((width1, width), 0), 1.0, 0.0
    ).astype(BF16)
    l1 = iota((width1, lanes), 0)
    j2 = l1 // 2
    place = (j2 % 4) * 16 + j2 // 4
    down1[...] = jnp.where(
        (l1 < lanes) & (iota((width1, lanes), 1) % half == place), 1.0, 0.0
    ).astype(BF16)
    q_count = s2.shape[2]
    p_count = s2.shape[1]
    m1 = iota((q_count, width1), 1)
    col1 = jnp.where(m1 < lanes + half // 2, m1, m1 - width1)
    wide = gy * half + (col1 + 512) // 2 - 256
    for r in range(4):
        spread[r * q_count : (r + 1) * q_count, :] = jnp.where(
            wide == 4 * iota((q_count, width1), 0) + r, 1.0, 0.0
        ).astype(BF16)

    load_g.wait()
    load_s.wait()
    send_l[...] = jnp.where(lane < half, g_ref[:, 0:lanes], pltpu.roll(s_ref[:, 0:lanes], half, 1))
    send_r[...] = jnp.where(
        lane < half, pltpu.roll(s_ref[:, cols - lanes : cols], half, 1), g_ref[:, cols - lanes : cols]
    )

    l1 = iota((width1, lanes), 0)
    at2 = (jnp.where(l1 < lanes + half // 2, l1, l1 - width1) + 2 * lanes) // 2
    at4 = at2 // 4 - 24
    down_w[...] = jnp.where(
        (at4 >= 0) & (at4 < 32) & (iota((width1, lanes), 1) == (at2 % 4) * 32 + at4), 1.0, 0.0
    ).astype(BF16)
    l1 = iota((lanes, width1), 1)
    at2 = (jnp.where(l1 < lanes + half // 2, l1, l1 - width1) + 2 * lanes) // 2
    at4 = at2 // 4 - 24
    up_w[...] = jnp.where(
        (at4 >= 0) & (at4 < 32) & (iota((lanes, width1), 0) == (at2 % 4) * 32 + at4), 1.0, 0.0
    ).astype(BF16)

    def pack_level2(source):
        parts = []
        for t in range(4):
            start = base1 + 2 * t
            parts.append(
                get_strips(source, pl.ds(start, 8, 8)) + get_strips(source, pl.ds(start + 1, 8, 8))
            )
        means = 0.25 * exact_dot(jnp.concatenate(parts, 0), down1[...])
        low = iota((16, lanes), 1) < half
        return jnp.where(low, means[0:16], means[16:32])

    def beside_count(at, count):
        return (at + count - 1) // count + 1 - (at + 1) // count

    pl.semaphore_wait(
        barrier, gx_count + gy_count - 2 + beside_count(gx, gx_count) * beside_count(gy, gy_count)
    )

    def tell_row(k):
        pl.semaphore_signal(row_wave, inc=1, device_id=(wrap(gx, k, gx_count), gy), device_id_type=MESH)

    each(gx_count, tell_row)

    top, bottom = slice(0, HALO), slice(rows - HALO, rows)
    above, below = slice(ROWS_PAD, base), slice(base + rows, base + rows + HALO)
    middle = slice(base, base + rows)
    sends = (
        (-1, -1, send_l.at[top, :], recv_r.at[below, :]),
        (1, -1, send_l.at[bottom, :], recv_r.at[above, :]),
        (-1, 1, send_r.at[top, :], recv_l.at[below, :]),
        (1, 1, send_r.at[bottom, :], recv_l.at[above, :]),
        (-1, 0, g_ref.at[top, :], gE.at[below, 0:cols]),
        (-1, 0, s_ref.at[top, :], sE.at[below, 0:cols]),
        (1, 0, g_ref.at[bottom, :], gE.at[above, 0:cols]),
        (1, 0, s_ref.at[bottom, :], sE.at[above, 0:cols]),
        (0, -1, send_l, recv_r.at[middle, :]),
        (0, 1, send_r, recv_l.at[middle, :]),
    )

    def halo_copy(n, dx, dy, source, target):
        return pltpu.make_async_remote_copy(
            src_ref=source, dst_ref=target, send_sem=halo_send.at[n], recv_sem=halo_recv.at[n],
            device_id=(gx + dx, gy + dy), device_id_type=MESH,
        )

    for n, (dx, dy, source, target) in enumerate(sends):
        @pl.when(inside(dx, dy))
        def _():
            halo_copy(n, dx, dy, source, target).start()

    core = lax.rem(gy, 2)
    per_row = gy_count // 2
    chips = total // 2
    partner = (gx, gy + 1 - 2 * core)

    def zigzag(j, count):
        odd = j % 2
        return odd * ((j + 1) // 2) + (1 - odd) * (count - j // 2)

    def block_copy(turn, n, slot, peer):
        return pltpu.make_async_remote_copy(
            src_ref=rbuf.at[turn, slot], dst_ref=rbuf.at[turn, slot],
            send_sem=all_send.at[turn, n], recv_sem=all_recv.at[turn, slot],
            device_id=peer, device_id_type=MESH,
        )

    def direct(turn, j):
        n = zigzag(j, chips)
        peer = (wrap(gx, n // per_row, gx_count), wrap(gy, 2 * (n % per_row), gy_count))
        return block_copy(turn, j, me, peer)

    def sender(j):
        n = zigzag(j, chips)
        return wrap(gx, -(n // per_row), gx_count) * gy_count + wrap(gy, -2 * (n % per_row), gy_count)

    def onward(turn, j):
        return block_copy(turn, chips + j, sender(j), partner)

    def gather_start(turn):
        block_copy(turn, 0, me, partner).start()
        each(chips, lambda j: direct(turn, chips - j).start())

    def gather_wait(turn):
        def pass_block(j):
            copy = onward(turn, j)
            copy.wait_recv()
            copy.start()

        each(chips, pass_block)
        block_copy(turn, 0, me + 1 - 2 * core, partner).wait_recv()
        each(chips, lambda j: block_copy(turn, chips + j, sender(j) + 1 - 2 * core, partner).wait_recv())

    def gather_sent(turn):
        def sent(j):
            direct(turn, j).wait_send()
            onward(turn, j).wait_send()

        block_copy(turn, 0, me, partner).wait_send()
        each(chips, sent)

    def slot_of(d, j):
        return wrap(gx, -d, gx_count) * gy_count + wrap(gy, -2 * j, gy_count)

    def each_block(first_d, first_j, body):
        if total <= 64:
            for d in range(first_d, gx_count):
                for j in range(first_j, per_row):
                    body(d, j)
        else:
            pl.loop(first_d, gx_count)(lambda d: pl.loop(first_j, per_row)(lambda j: body(d, j)))

    def along_line(turn, d):
        return block_copy(turn, d, me, (wrap(gx, d, gx_count), gy))

    def across(turn, d, j):
        n = gx_count + d * (per_row - 1) + j - 1
        return block_copy(turn, n, slot_of(d, 0), (gx, wrap(gy, 2 * j, gy_count)))

    def to_partner(turn, d, j):
        return block_copy(turn, chips + d * per_row + j, slot_of(d, j), partner)

    def from_partner(turn, d, j):
        return block_copy(turn, 0, slot_of(d, j) + 1 - 2 * core, partner)

    def line_start(turn):
        block_copy(turn, 0, me, partner).start()
        each(gx_count, lambda d: along_line(turn, gx_count - d).start())
        each(per_row, lambda j: across(turn, 0, per_row - j).start())

    def line_pass(turn):
        def pass_line(d):
            block_copy(turn, 0, slot_of(d, 0), partner).wait_recv()
            each(per_row, lambda j: across(turn, d, per_row - j).start())
            to_partner(turn, d, 0).start()

        each(gx_count, pass_line)

    def line_wait(turn):
        def pass_block(d, j):
            copy = to_partner(turn, d, j)
            copy.wait_recv()
            copy.start()

        each_block(0, 1, pass_block)
        each_block(0, 0, lambda d, j: from_partner(turn, d, j).wait_recv())

    def line_sent(turn):
        block_copy(turn, 0, me, partner).wait_send()
        each(gx_count, lambda d: along_line(turn, d).wait_send())
        each_block(0, 1, lambda d, j: across(turn, d, j).wait_send())
        each_block(1, 0, lambda d, j: to_partner(turn, d, j).wait_send())
        each(per_row, lambda j: to_partner(turn, 0, j).wait_send())

    gE[base : base + rows, 0:cols] = g_ref[...]
    sE[base : base + rows, 0:cols] = s_ref[...]

    own_strips = cols // lanes
    for k in range(own_strips):
        fine_add[k, base : base + rows, :] = s_ref[:, k * lanes : (k + 1) * lanes]
    own = get_strips(fine_add, pl.ds(base, half_rows, 2), own_strips)
    own = own + get_strips(fine_add, pl.ds(base + 1, half_rows, 2), own_strips)
    put_strips(r1, slice(base1, base1 + half_rows), 0.25 * exact_dot(own, down0[0:cols, :]))
    rbuf[0, me] = pack_level2(r1)
    line_start(0)
    zero_tile = jnp.zeros((ROWS_PAD, width), F32)
    for ref in (vA, vB):
        ref[0:ROWS_PAD, :] = zero_tile
        ref[ext - ROWS_PAD : ext, :] = zero_tile
    for ref in (aP, bP, a1, b1):
        ref[0:ROWS_PAD, :] = jnp.zeros((ROWS_PAD, width1), F32)
        ref[ref.shape[0] - ROWS_PAD :, :] = jnp.zeros((ROWS_PAD, width1), F32)
    for ref in (a2, b2, a3, b3, a4):
        for i in range(ref.shape[0]):
            ref[i, 0:8, :] = jnp.zeros((8, q_count), F32)
            ref[i, 8 + p_count : 16 + p_count, :] = jnp.zeros((8, q_count), F32)

    for n, (dx, dy, source, target) in enumerate(sends):
        @pl.when(inside(-dx, -dy))
        def _():
            halo_copy(n, -dx, -dy, source, target).wait_recv()

    lane_e = iota((ext, lanes), 1)
    gE[:, cols:width] = jnp.where(lane_e < half, recv_r[...], recv_l[...])
    sE[:, cols:width] = pltpu.roll(jnp.where(lane_e < half, recv_l[...], recv_r[...]), half, 1)

    def weight(shifts, first_row, own_rows, own_cols, split, level):
        shape = shifts.shape
        at_row = gx * own_rows + iota(shape, 0) + first_row
        lane_at = iota(shape, 1)
        at_col = gy * own_cols + jnp.where(lane_at < own_cols + split, lane_at, lane_at - shape[1])
        good = (at_row >= 0) & (at_row < gx_count * own_rows)
        good = good & (at_col >= 0) & (at_col < gy_count * own_cols)
        return jnp.where(good, DAMPING / (4.0 ** (1 - level) + shifts), 0.0)

    def around(v, lo, size):
        span = v.shape[1]
        mid = v[lo : lo + size, :]
        beside = pltpu.roll(mid, 1, 1) + pltpu.roll(mid, span - 1, 1)
        return mid, beside + (v[lo - 1 : lo - 1 + size, :] + v[lo + 1 : lo + 1 + size, :])

    def sweep_block(v, out, g, w, level, span=None):
        scale = 4.0 ** (-level)
        for lo in range(*(span or (ROWS_PAD, v.shape[0] - ROWS_PAD)), 8):
            mid, beside = around(v, lo, 8)
            at = slice(lo, lo + 8)
            out[at, :] = (1.0 - DAMPING) * mid + w[at, :] * (g[at, :] + scale * beside)

    def residual_block(v, out, g, s, level, span=None):
        scale = 4.0 ** (-level)
        for lo in range(*(span or (ROWS_PAD, v.shape[0] - ROWS_PAD)), 8):
            mid, beside = around(v, lo, 8)
            at = slice(lo, lo + 8)
            put_strips(out, at, g[at, :] - (scale * (4.0 * mid - beside) + s[at, :] * mid))

    row_moves = (
        (-1, sP.at[base1 : base1 + ROW_HALO, :], s1.at[base_w + half_rows : base_w + half_rows + ROW_HALO, :]),
        (1, sP.at[base1 + half_rows - ROW_HALO : base1 + half_rows, :], s1.at[ROWS_PAD:base_w, :]),
        (-1, gP.at[base1 : base1 + ROW_HALO, :], g1.at[base_w + half_rows : base_w + half_rows + ROW_HALO, :]),
        (1, gP.at[base1 + half_rows - ROW_HALO : base1 + half_rows, :], g1.at[ROWS_PAD:base_w, :]),
    )

    def row_copy(n, dx):
        _, source, target = row_moves[n]
        return pltpu.make_async_remote_copy(
            src_ref=source, dst_ref=target, send_sem=row_send.at[n], recv_sem=row_recv.at[n],
            device_id=(gx + dx, gy), device_id_type=MESH,
        )

    def rows_start(which):
        for n in which:
            dx = row_moves[n][0]
            @pl.when(inside(dx, 0))
            def _():
                row_copy(n, dx).start()

    def halved():
        pairs = get_strips(fine_add, pl.ds(0, ext1, 2)) + get_strips(fine_add, pl.ds(1, ext1, 2))
        return 0.25 * exact_dot(pairs, down0[...])

    put_strips(fine_add, slice(0, ext), sE[...])
    sP[near1, :] = halved()
    rows_start((0, 1))
    chunk = 16
    for lo in range(0, ext, chunk):
        at = slice(lo, lo + chunk)
        wE[at, :] = weight(sE[at, :], lo - base, rows, cols, half, 0)
    for lo in range(ROWS_PAD, ext - ROWS_PAD, 8):
        at = slice(lo, lo + 8)
        vA[at, :] = wE[at, :] * gE[at, :]
    sweep_block(vA, vB, gE, wE, 0)
    put_strips(fine_add, slice(0, ROWS_PAD), zero_tile)
    put_strips(fine_add, slice(ext - ROWS_PAD, ext), zero_tile)
    residual_block(vB, fine_add, gE, sE, 0)
    gP[near1, :] = halved()
    wP[near1, :] = weight(sP[near1, :], ROWS_PAD - base1, half_rows, cols // 2, half // 2, 1)
    aP[near1, :] = wP[near1, :] * gP[near1, :]
    sweep_block(aP, bP, gP, wP, 1)
    residual_block(bP, r1, gP, sP, 1, (base1, base1 + half_rows))
    rbuf[1, me] = pack_level2(r1)
    pl.semaphore_wait(row_wave, gx_count - 1)
    gather_start(1)
    line_pass(0)

    block = (lane_e[0:8] // 16)

    def unpack(turn, target):
        for x in range(gx_count):
            for u in range(gy_count // 8):
                for tl in range(2):
                    tiles = [rbuf[turn, x * gy_count + u * 8 + g, tl * 8 : tl * 8 + 8, :] for g in range(8)]
                    for bit in (1, 2, 4):
                        keep = (block & bit) == 0
                        fresh = list(tiles)
                        for g in range(8):
                            if g & bit == 0:
                                lo, hi = tiles[g], tiles[g | bit]
                                fresh[g] = jnp.where(keep, lo, pltpu.roll(hi, 16 * bit, 1))
                                fresh[g | bit] = jnp.where(keep, pltpu.roll(lo, lanes - 16 * bit, 1), hi)
                        tiles = fresh
                    for b in range(8):
                        t, r = (b // 4) * 2 + tl, b % 4
                        target[t * 4 + r, 8 * x : 8 * x + 8, u * lanes : (u + 1) * lanes] = tiles[b]

    lane_q = iota((p_count, q_count), 1)
    rows_q = slice(8, 8 + p_count)

    def sides(v, n, t, r):
        mid = v[t * n + r, rows_q, :]
        if t > 0:
            north = v[(t - 1) * n + r, rows_q, :]
        else:
            north = v[(n - 1) * n + r, 7 : 7 + p_count, :]
        if t < n - 1:
            south = v[(t + 1) * n + r, rows_q, :]
        else:
            south = v[r, 9 : 9 + p_count, :]
        if r > 0:
            west = v[t * n + r - 1, rows_q, :]
        else:
            west = jnp.where(lane_q == 0, 0.0, pltpu.roll(v[t * n + n - 1, rows_q, :], 1, 1))
        if r < n - 1:
            east = v[t * n + r + 1, rows_q, :]
        else:
            east = jnp.where(
                lane_q == q_count - 1, 0.0, pltpu.roll(v[t * n, rows_q, :], q_count - 1, 1)
            )
        return mid, (north + south) + (west + east)

    level_refs = {2: (s2, w2, g2, a2, b2, 4), 3: (s3, w3, g3, a3, b3, 2), 4: (s4, w4, g4, a4, None, 1)}

    def sweep(level, v, out):
        s, w, g, _, _, n = level_refs[level]
        for t in range(n):
            for r in range(n):
                i = t * n + r
                mid, beside = sides(v, n, t, r)
                out[i, rows_q, :] = (1.0 - DAMPING) * mid + w[i] * (g[i] + 4.0 ** (-level) * beside)

    def first_sweep(level, out):
        s, w, g, _, _, n = level_refs[level]
        for i in range(n * n):
            out[i, rows_q, :] = w[i] * g[i]

    def restricted(level, v):
        s, w, g, _, _, n = level_refs[level]
        coarse_g = level_refs[level + 1][2]
        for t in range(n // 2):
            for r in range(n // 2):
                sums = None
                for dt in range(2):
                    for dr in range(2):
                        i = (2 * t + dt) * n + 2 * r + dr
                        mid, beside = sides(v, n, 2 * t + dt, 2 * r + dr)
                        left = g[i] - (4.0 ** (-level) * (4.0 * mid - beside) + s[i] * mid)
                        sums = left if sums is None else sums + left
                coarse_g[t * (n // 2) + r] = 0.25 * sums

    def correct(level, v, e):
        n = level_refs[level][5]
        for t in range(n):
            for r in range(n):
                i = t * n + r
                v[i, rows_q, :] = v[i, rows_q, :] + e[(t // 2) * (n // 2) + r // 2, rows_q, :]

    def prepare(level):
        s, w, _, _, _, n = level_refs[level]
        for i in range(n * n):
            w[i] = DAMPING / (4.0 ** (1 - level) + s[i])
        if level < 4:
            coarse_s = level_refs[level + 1][0]
            m = n // 2
            for t in range(m):
                for r in range(m):
                    i = 2 * t * n + 2 * r
                    coarse_s[t * m + r] = 0.25 * ((s[i] + s[i + n]) + (s[i + 1] + s[i + n + 1]))

    def total_of(x):
        return jnp.sum(jnp.sum(x, axis=0, keepdims=True), axis=1, keepdims=True)

    window = picked.shape[1] - 8
    lane_w, row_w = iota((window, lanes), 1), iota((window, lanes), 0)

    def in_domain(period):
        at_p, at_q = gx * 8 - 4 + row_w, gy * 16 - 8 + lane_w % period
        good = (at_p >= 0) & (at_p < p_count) & (at_q >= 0) & (at_q < q_count)
        return good & (lane_w % period < 32)

    def put_window(t, values):
        for a in range(2):
            put_strips(r1, pl.ds(ROWS_PAD + 2 * t + a, window, 8), values)

    def add_level2(e, v):
        for t in range(4):
            tiles = [e[t * 4 + r, pl.ds(pl.multiple_of(gx * 8, 8), 24), :] for r in range(4)]
            picked[t] = exact_dot(jnp.concatenate(tiles, 1), spread[...])
        for t in range(4):
            put_window(t, picked[t, 4 : 4 + window, :])
        v[wide1, :] = v[wide1, :] + get_strips(r1, wide1)

    def pack_window(source):
        parts = []
        for t in range(4):
            start = ROWS_PAD + 2 * t
            parts.append(
                get_strips(source, pl.ds(start, window, 8)) + get_strips(source, pl.ds(start + 1, window, 8))
            )
        means = 0.25 * exact_dot(jnp.concatenate(parts, 0), down_w[...])
        return [means[t * window : (t + 1) * window] for t in range(4)]

    def joined(x, unit):
        return x + pltpu.roll(x, lanes - unit, 1)

    def halved_window(tiles, unit):
        return [0.25 * joined(tiles[2 * t] + tiles[2 * t + 1], unit) for t in range(len(tiles) // 2)]

    def beside_window(v, unit):
        n = len(v)
        out = []
        for t in range(n):
            north = v[t - 1] if t > 0 else pltpu.roll(v[n - 1], 1, 0)
            south = v[t + 1] if t < n - 1 else pltpu.roll(v[0], window - 1, 0)
            west = jnp.where(lane_w < unit, pltpu.roll(v[t], unit + 1, 1), pltpu.roll(v[t], unit, 1))
            east = jnp.where(
                lane_w >= lanes - unit,
                pltpu.roll(v[t], lanes - unit - 1, 1), pltpu.roll(v[t], lanes - unit, 1),
            )
            out.append((north + south) + (west + east))
        return out

    window_refs = {2: (s2w, w2w, 32), 3: (s3w, w3w, 64)}

    def sweep_window(level, v, g):
        _, w, unit = window_refs[level]
        beside = beside_window(v, unit)
        return [
            (1.0 - DAMPING) * v[t] + w[t] * (g[t] + 4.0 ** (-level) * beside[t]) for t in range(len(v))
        ]

    def residual_window(level, v, g):
        s, _, unit = window_refs[level]
        beside = beside_window(v, unit)
        return [
            g[t] - (4.0 ** (-level) * (4.0 * v[t] - beside[t]) + s[t] * v[t]) for t in range(len(v))
        ]

    def rows_wait(which):
        for n in which:
            dx = row_moves[n][0]
            @pl.when(inside(-dx, 0))
            def _():
                row_copy(n, -dx).wait_recv()

    own1, own_w = slice(base1, base1 + half_rows), slice(base_w, base_w + half_rows)
    rows_wait((0, 1))
    s1[own_w, :] = sP[own1, :]
    w1[wide1, :] = weight(s1[wide1, :], ROWS_PAD - base_w, half_rows, cols // 2, half // 2, 1)
    put_strips(r1, wide1, s1[wide1, :])
    tiles = pack_window(r1)
    for t in range(4):
        s2w[t] = tiles[t]
        w2w[t] = jnp.where(in_domain(32), DAMPING / (4.0 ** (-1) + tiles[t]), 0.0)
    tiles = halved_window(tiles, 32)
    for t in range(2):
        s3w[t] = tiles[t]
        w3w[t] = jnp.where(in_domain(64), DAMPING / (4.0 ** (-2) + tiles[t]), 0.0)

    line_wait(0)
    unpack(0, s2)
    for level in (2, 3, 4):
        prepare(level)
    row_q = iota((p_count, q_count), 0)
    edges = jnp.where(row_q == 0, 1.0, 0.0) + jnp.where(row_q == p_count - 1, 1.0, 0.0)
    edges = edges + jnp.where(lane_q == 0, 1.0, 0.0) + jnp.where(lane_q == q_count - 1, 1.0, 0.0)
    unit4 = 4.0 ** (-4) * edges + s4[0]
    per_unit = 1.0 / total_of(unit4)

    def shifted(x, reach):
        out = {0: x}
        for k in range(1, reach + 1):
            out[k] = jnp.where(lane_q < q_count - k, pltpu.roll(x, q_count - k, 1), 0.0)
            out[-k] = jnp.where(lane_q >= k, pltpu.roll(x, k, 1), 0.0)
        return out

    reach4 = 2
    for k, values in shifted(4.0 ** (-4) * w4[0], reach4).items():
        hw4[k + reach4] = values
    for i in range(beside4.shape[0]):
        beside4[i, 0:8, :] = jnp.zeros((8, q_count), F32)
        beside4[i, 8 + p_count : 16 + p_count, :] = jnp.zeros((8, q_count), F32)

    def fused_sweeps(v, source, count, first_slot=0):
        for turn in range(count):
            reach = count - 1 - turn
            new = {}
            for k in range(-reach, reach + 1):
                slot = first_slot + (turn % 2) * 5 + k + reach4
                beside4[slot, rows_q, :] = v[k]
                along = beside4[slot, 7 : 7 + p_count, :] + beside4[slot, 9 : 9 + p_count, :]
                value = (1.0 - DAMPING) * v[k] + hw4[k + reach4] * ((v[k - 1] + v[k + 1]) + along)
                new[k] = value if source is None else value + source[k]
            v = new
        return v[0]

    def six_sweeps(v, source, first_slot=0):
        v = fused_sweeps(shifted(v, 3), source, 3, first_slot)
        return fused_sweeps(shifted(v, 3), source, 3, first_slot)

    def coarse(twice=False):
        source = shifted(w4[0] * g4[0], 3)
        v = fused_sweeps(source, source, 3)
        v = fused_sweeps(shifted(v, 2), source, 2)
        add = total_of(g4[0]) * per_unit
        if twice:
            phi[0] = six_sweeps(jnp.ones((p_count, q_count), F32), None, 10)
            phi[1] = six_sweeps(phi[0], None, 10)
            kept = 1.0 - per_unit * total_of(unit4 * phi[0])
            again = add * kept - total_of(unit4 * v) * per_unit
            v = six_sweeps(v, source) + add * phi[1] + again * phi[0]
        else:
            v = v + add * phi[0]
        a4[0, rows_q, :] = v
        return a4

    def vcycle(level, v):
        if level == 4:
            return coarse()
        _, _, _, a, b, n = level_refs[level]
        if v is None:
            first_sweep(level, a)
            sweep(level, a, b)
            now, later = b, a
        else:
            later = b if v is a else a
            sweep(level, v, later)
            sweep(level, later, v)
            now = v
        restricted(level, now)
        correct(level, now, vcycle(level + 1, None))
        sweep(level, now, later)
        sweep(level, later, now)
        return now

    def fcycle(level):
        _, _, _, a, b, n = level_refs[level]
        first_sweep(level, a)
        sweep(level, a, b)
        restricted(level, b)
        if level == 3:
            e = coarse(True)
        else:
            e = vcycle(level + 1, fcycle(level + 1))
        correct(level, b, e)
        sweep(level, b, a)
        sweep(level, a, b)
        return b

    def coarse_send(k):
        n = zigzag(total - k, total)
        pltpu.make_async_remote_copy(
            src_ref=cbuf.at[me], dst_ref=cbuf.at[me], send_sem=coarse_sems.at[0], recv_sem=coarse_sems.at[1],
            device_id=(wrap(gx, n // gy_count, gx_count), wrap(gy, n % gy_count, gy_count)), device_id_type=MESH,
        ).start()

    def coarse_wait(n):
        others = cbuf.at[pl.ds(0, total - 1)]
        pltpu.make_async_copy(others, others, coarse_sems.at[n]).wait()

    gather_wait(1)
    rows_start((2, 3))
    unpack(1, g2)
    e = fcycle(2)
    e = vcycle(2, e)
    rows_wait((2, 3))
    g1[own_w, :] = gP[own1, :]
    a1[wide1, :] = w1[wide1, :] * g1[wide1, :]
    sweep_block(a1, b1, g1, w1, 1)
    add_level2(e, b1)
    sweep_block(b1, a1, g1, w1, 1)
    sweep_block(a1, b1, g1, w1, 1)
    sweep_block(b1, a1, g1, w1, 1)
    sweep_block(a1, b1, g1, w1, 1)
    residual_block(b1, r1, g1, s1, 1)
    source2 = pack_window(r1)
    v2 = sweep_window(2, [w2w[t] * source2[t] for t in range(4)], source2)
    source3 = halved_window(residual_window(2, v2, source2), 32)
    v3 = sweep_window(3, [w3w[t] * source3[t] for t in range(2)], source3)
    source4 = halved_window(residual_window(3, v3, source3), 64)[0]
    place = lax.rem(gy, 8) * 16
    mine = pltpu.roll(source4[4:12], lax.rem(place + lanes - 8, lanes), 1)
    lane_c = iota((8, lanes), 1)
    cbuf[me] = jnp.where((lane_c >= place) & (lane_c < place + 16), mine, 0.0)

    each(total, coarse_send)
    line_sent(0)
    gather_sent(1)
    for n, (dx, dy, source, target) in enumerate(sends):
        @pl.when(inside(dx, dy))
        def _():
            halo_copy(n, dx, dy, source, target).wait_send()
    for n, (dx, _, _) in enumerate(row_moves):
        @pl.when(inside(dx, 0))
        def _():
            row_copy(n, dx).wait_send()
    coarse_wait(1)
    for x in range(gx_count):
        for u in range(gy_count // 8):
            first = x * gy_count + u * 8
            pairs = [cbuf[first + k] + cbuf[first + k + 1] for k in range(0, 8, 2)]
            g4[0, x * 8 : x * 8 + 8, u * lanes : (u + 1) * lanes] = (pairs[0] + pairs[1]) + (pairs[2] + pairs[3])
    e = coarse()
    e = e[0, pl.ds(pl.multiple_of(gx * 8, 8), 24), :][4 : 4 + window]
    e = pltpu.roll(e, lax.rem(q_count + 8 - gy * 16 + q_count, q_count), 1)[:, 0:lanes]
    e = jnp.where(in_domain(lanes), e, 0.0)
    e = e + pltpu.roll(e, 64, 1)
    v3 = [v3[t] + e for t in range(2)]
    v3 = sweep_window(3, sweep_window(3, v3, source3), source3)
    e = [v3[t] + pltpu.roll(v3[t], 32, 1) for t in range(2)]
    v2 = [v2[t] + e[t // 2] for t in range(4)]
    v2 = sweep_window(2, sweep_window(2, v2, source2), source2)
    raised = exact_dot(jnp.concatenate(v2, 0), up_w[...])
    for t in range(4):
        put_window(t, raised[t * window : (t + 1) * window])
    b1[wide1, :] = b1[wide1, :] + get_strips(r1, wide1)
    near_w = (base_w - 8, base_w + half_rows + 8)
    sweep_block(b1, a1, g1, w1, 1, near_w)
    sweep_block(a1, b1, g1, w1, 1, near_w)
    raised = exact_dot(b1[slice(*near_w), :], up0[...])
    put_strips(fine_add, pl.ds(0, ext1, 2), raised)
    put_strips(fine_add, pl.ds(1, ext1, 2), raised)
    for lo in range(ROWS_PAD, ext - ROWS_PAD, 8):
        at = slice(lo, lo + 8)
        vB[at, :] = vB[at, :] + get_strips(fine_add, at)
    sweep_block(vB, vA, gE, wE, 0)
    sweep_block(vA, vB, gE, wE, 0)
    for lo in range(0, rows, 8):
        mid, beside = around(vB, base + lo, 8)
        at = slice(base + lo, base + lo + 8)
        left = gE[at, :] - ((4.0 * mid - beside) + sE[at, :] * mid)
        out_ref[0, lo : lo + 8, :] = mid[:, 0:cols]
        out_ref[1, lo : lo + 8, :] = left[:, 0:cols]

    coarse_wait(0)


def solution(mesh):
    gx_count, gy_count = mesh.shape["gx"], mesh.shape["gy"]
    total = gx_count * gy_count

    def body(right_side, shift):
        rows, cols = right_side.shape
        assert cols == 256 and rows == 128 and gy_count % 8 == 0
        ext, width = rows + 2 * (HALO + ROWS_PAD), cols + 128
        ext1, width1 = ext // 2 + 2 * ROWS_PAD, 256
        wide1 = rows // 2 + 2 * (ROW_HALO + ROWS_PAD)
        window = rows // 16 + 8
        p, q = rows // 16 * gx_count, cols // 16 * gy_count
        V = pltpu.VMEM
        dma = pltpu.SemaphoreType.DMA
        big = [V((ext, width), F32)] * 5 + [V((width // 128, ext, 128), F32)]
        one = [V((ext1, width1), F32)] * 5
        one += [V((wide1, width1), F32)] * 5 + [V((width1 // 128, wide1, 128), F32)]
        levels = []
        for n in (16, 4, 1):
            levels += [V((n, p, q), F32)] * 3 + [V((n, p + 16, q), F32)] * (2 if n > 1 else 1)
        scratch = (
            [V((rows, cols), F32)] * 2 + [dma((2,))]
            + big + one
            + [V((rows, 128), F32)] * 2 + [V((ext, 128), F32)] * 2
            + [V((width, width1), BF16), V((width1, width), BF16), V((width1, 128), BF16), V((4 * q, width1), BF16)]
            + [V((width1, 128), BF16), V((128, width1), BF16)]
            + [V((2, total, 16, 128), F32), V((total, 8, 128), F32)]
            + levels
            + [V((4, 24, width1), F32)]
            + [V((4, window, 128), F32)] * 2 + [V((2, window, 128), F32)] * 2
            + [V((5, p, q), F32), V((2, p, q), F32), V((20, p + 16, q), F32)]
            + [dma((10,)), dma((10,)), dma((4,)), dma((4,)), dma((2, total)), dma((2, total)), dma((2,))]
            + [pltpu.SemaphoreType.REGULAR]
        )
        out = pltpu.VMEM((2,) + right_side.shape, F32)
        both = pl.pallas_call(
            functools.partial(kernel, gx_count, gy_count),
            out_shape=out,
            in_specs=[pl.BlockSpec(memory_space=pltpu.HBM)] * 2,
            out_specs=pl.BlockSpec(memory_space=pltpu.VMEM),
            scratch_shapes=scratch,
            compiler_params=pltpu.CompilerParams(
                collective_id=0, has_side_effects=True, vmem_limit_bytes=60*1024*1024
            ),
        )(right_side, shift)
        return both[0], both[1]

    spec = P("gx", "gy")
    return jax.shard_map(body, mesh=mesh, in_specs=(spec, spec), out_specs=(spec, spec), check_vma=False)
```

```python
import functools

import jax
import jax.numpy as jnp
from jax import lax
from jax.experimental import pallas as pl
from jax.experimental.pallas import tpu as pltpu
from jax.sharding import PartitionSpec as P

DAMPING = 0.8
MESH = pl.DeviceIdType.MESH
F32 = jnp.float32
BF16 = jnp.bfloat16

ROWS_PAD = 8
HALO = 8
ROW_HALO = 32


def iota(shape, dim):
    return lax.broadcasted_iota(jnp.int32, shape, dim)


def put_strips(ref, at, values):
    for k in range(ref.shape[0]):
        ref[k, at, :] = values[:, k * 128 : (k + 1) * 128]


def get_strips(ref, at, count=None):
    return jnp.concatenate([ref[k, at, :] for k in range(count or ref.shape[0])], 1)


def exact_dot(values, selector):
    first = values.astype(BF16)
    rest = values - first.astype(F32)
    second = rest.astype(BF16)
    third = (rest - second.astype(F32)).astype(BF16)
    dot = functools.partial(jnp.dot, preferred_element_type=F32)
    return dot(first, selector) + (dot(second, selector) + dot(third, selector))


def kernel(
    gx_count, gy_count, g_hbm, s_hbm, out_ref,
    g_ref, s_ref, load_sem,
    gE, sE, wE, vA, vB, fine_add,
    gP, sP, wP, aP, bP,
    g1, s1, w1, a1, b1, r1,
    send_l, send_r, recv_l, recv_r,
    down0, up0, down1, spread, down_w, up_w,
    rbuf, cbuf, s2, w2, g2, a2, b2, s3, w3, g3, a3, b3, s4, w4, g4, a4, picked,
    s2w, w2w, s3w, w3w, hw4, phi, beside4,
    halo_send, halo_recv, row_send, row_recv, all_send, all_recv, coarse_sems, told,
):
    gx, gy = lax.axis_index("gx"), lax.axis_index("gy")
    total = gx_count * gy_count
    me = gx * gy_count + gy
    rows, cols = g_hbm.shape
    base = ROWS_PAD + HALO
    base1 = ROWS_PAD + (ROWS_PAD + HALO) // 2
    ext, width = gE.shape
    ext1, width1 = ext // 2, g1.shape[1]
    half_rows = rows // 2
    base_w = ROWS_PAD + ROW_HALO
    near1 = slice(ROWS_PAD, ROWS_PAD + ext1)
    wide1 = slice(ROWS_PAD, base_w + half_rows + ROW_HALO)
    lanes = 128

    load_g = pltpu.make_async_copy(g_hbm, g_ref, load_sem.at[0])
    load_s = pltpu.make_async_copy(s_hbm, s_ref, load_sem.at[1])
    load_g.start()
    load_s.start()
    zero_halo = jnp.zeros((base, width), F32)
    for ref in (gE, sE):
        ref[0:base, :] = zero_halo
        ref[base + rows : ext, :] = zero_halo
    for ref in (recv_l, recv_r):
        ref[...] = jnp.zeros(ref.shape, F32)
    for ref in (g1, s1):
        ref[0:base_w, :] = jnp.zeros((base_w, width1), F32)
        ref[base_w + half_rows :, :] = jnp.zeros((base_w, width1), F32)
    def inside(dx, dy):
        ok = None
        for step, at, count in ((dx, gx, gx_count), (dy, gy, gy_count)):
            if step:
                here = (at > 0) if step < 0 else (at < count - 1)
                ok = here if ok is None else ok & here
        return ok

    def wrap(at, step, count):
        return lax.rem(at + count + step, count)

    def each(count, body):
        if count <= 64:
            for j in range(1, count):
                body(j)
        else:
            pl.loop(1, count)(body)

    barrier = pltpu.get_barrier_semaphore()
    corners = [(dx, dy) for dx in (-1, 1) for dy in (-1, 1)]

    def greet(x, y):
        pl.semaphore_signal(barrier, inc=1, device_id=(x, y), device_id_type=MESH)

    each(gx_count, lambda k: greet(wrap(gx, k, gx_count), gy))
    for dx, dy in corners:
        @pl.when(inside(dx, dy))
        def _():
            greet(gx + dx, gy + dy)

    bits = [1 << b for b in range(1, gy_count.bit_length() - 1)] + [1]

    def flip(bit):
        return gy + bit * (1 - 2 * lax.rem(gy // bit, 2))

    for bit in bits[:-1]:
        greet(gx, flip(bit))
    for dy in (-1, 1):
        @pl.when(inside(0, dy))
        def _():
            greet(gx, gy + dy)


    lane = iota((rows, lanes), 1)
    half = lanes // 2
    l0 = iota((width, width1), 0)
    col0 = jnp.where(l0 < cols + half, l0, l0 - width)
    down0[...] = jnp.where(
        ((col0 + 2 * width1) // 2) % width1 == iota((width, width1), 1), 1.0, 0.0
    ).astype(BF16)
    l0 = iota((width1, width), 1)
    col0 = jnp.where(l0 < cols + half, l0, l0 - width)
    up0[...] = jnp.where(
        ((col0 + 2 * width1) // 2) % width1 == iota((width1, width), 0), 1.0, 0.0
    ).astype(BF16)
    l1 = iota((width1, lanes), 0)
    j2 = l1 // 2
    place = ((j2 + gy) % 4) * 16 + j2 // 4
    down1[...] = jnp.where(
        (l1 < lanes) & (iota((width1, lanes), 1) % half == place), 1.0, 0.0
    ).astype(BF16)
    q_count = s2.shape[2]
    p_count = s2.shape[1]
    m1 = iota((q_count, width1), 1)
    col1 = jnp.where(m1 < lanes + half // 2, m1, m1 - width1)
    wide = gy * half + (col1 + 512) // 2 - 256
    for r in range(4):
        spread[r * q_count : (r + 1) * q_count, :] = jnp.where(
            wide == 4 * iota((q_count, width1), 0) + r, 1.0, 0.0
        ).astype(BF16)

    load_g.wait()
    load_s.wait()
    send_l[...] = jnp.where(lane < half, g_ref[:, 0:lanes], pltpu.roll(s_ref[:, 0:lanes], half, 1))
    send_r[...] = jnp.where(
        lane < half, pltpu.roll(s_ref[:, cols - lanes : cols], half, 1), g_ref[:, cols - lanes : cols]
    )

    l1 = iota((width1, lanes), 0)
    at2 = (jnp.where(l1 < lanes + half // 2, l1, l1 - width1) + 2 * lanes) // 2
    at4 = at2 // 4 - 24
    down_w[...] = jnp.where(
        (at4 >= 0) & (at4 < 32) & (iota((width1, lanes), 1) == (at2 % 4) * 32 + at4), 1.0, 0.0
    ).astype(BF16)
    l1 = iota((lanes, width1), 1)
    at2 = (jnp.where(l1 < lanes + half // 2, l1, l1 - width1) + 2 * lanes) // 2
    at4 = at2 // 4 - 24
    up_w[...] = jnp.where(
        (at4 >= 0) & (at4 < 32) & (iota((lanes, width1), 0) == (at2 % 4) * 32 + at4), 1.0, 0.0
    ).astype(BF16)

    def pack_level2(source):
        parts = []
        for t in range(4):
            start = base1 + 2 * t
            parts.append(
                get_strips(source, pl.ds(start, 8, 8)) + get_strips(source, pl.ds(start + 1, 8, 8))
            )
        means = 0.25 * exact_dot(jnp.concatenate(parts, 0), down1[...])
        low = (iota((16, lanes), 1) // 16 + 8 - lax.rem(gy, 8)) % 8 < 4
        return jnp.where(low, means[0:16], means[16:32])

    def beside_count(at, count):
        return (at + count - 1) // count + 1 - (at + 1) // count

    pl.semaphore_wait(
        barrier,
        gx_count + len(bits) - 2 + beside_count(gy, gy_count) * (1 + beside_count(gx, gx_count)),
    )

    def tell(n):
        pl.semaphore_signal(told.at[n], inc=1, device_id=(gx, flip(bits[n])), device_id_type=MESH)

    tell(0)

    top, bottom = slice(0, HALO), slice(rows - HALO, rows)
    above, below = slice(ROWS_PAD, base), slice(base + rows, base + rows + HALO)
    middle = slice(base, base + rows)
    sends = (
        (-1, -1, send_l.at[top, :], recv_r.at[below, :]),
        (1, -1, send_l.at[bottom, :], recv_r.at[above, :]),
        (-1, 1, send_r.at[top, :], recv_l.at[below, :]),
        (1, 1, send_r.at[bottom, :], recv_l.at[above, :]),
        (-1, 0, g_ref.at[top, :], gE.at[below, 0:cols]),
        (-1, 0, s_ref.at[top, :], sE.at[below, 0:cols]),
        (1, 0, g_ref.at[bottom, :], gE.at[above, 0:cols]),
        (1, 0, s_ref.at[bottom, :], sE.at[above, 0:cols]),
        (0, -1, send_l, recv_r.at[middle, :]),
        (0, 1, send_r, recv_l.at[middle, :]),
    )

    def halo_copy(n, dx, dy, source, target):
        return pltpu.make_async_remote_copy(
            src_ref=source, dst_ref=target, send_sem=halo_send.at[n], recv_sem=halo_recv.at[n],
            device_id=(gx + dx, gy + dy), device_id_type=MESH,
        )

    for n, (dx, dy, source, target) in enumerate(sends):
        @pl.when(inside(dx, dy))
        def _():
            halo_copy(n, dx, dy, source, target).start()

    core = lax.rem(gy, 2)
    per_row = gy_count // 2
    chips = total // 2
    partner = (gx, gy + 1 - 2 * core)

    def zigzag(j, count):
        odd = j % 2
        return odd * ((j + 1) // 2) + (1 - odd) * (count - j // 2)

    def block_copy(turn, n, slot, peer):
        return pltpu.make_async_remote_copy(
            src_ref=rbuf.at[turn, slot], dst_ref=rbuf.at[turn, slot],
            send_sem=all_send.at[turn, n], recv_sem=all_recv.at[turn, slot],
            device_id=peer, device_id_type=MESH,
        )

    def direct(turn, j):
        n = zigzag(j, chips)
        peer = (wrap(gx, n // per_row, gx_count), wrap(gy, 2 * (n % per_row), gy_count))
        return block_copy(turn, j, me, peer)

    def sender(j):
        n = zigzag(j, chips)
        return wrap(gx, -(n // per_row), gx_count) * gy_count + wrap(gy, -2 * (n % per_row), gy_count)

    def onward(turn, j):
        return block_copy(turn, chips + j, sender(j), partner)

    def gather_start(turn):
        block_copy(turn, 0, me, partner).start()
        each(chips, lambda j: direct(turn, chips - j).start())

    def gather_wait(turn):
        def pass_block(j):
            copy = onward(turn, j)
            copy.wait_recv()
            copy.start()

        each(chips, pass_block)
        block_copy(turn, 0, me + 1 - 2 * core, partner).wait_recv()
        each(chips, lambda j: block_copy(turn, chips + j, sender(j) + 1 - 2 * core, partner).wait_recv())

    def gather_sent(turn):
        def sent(j):
            direct(turn, j).wait_send()
            onward(turn, j).wait_send()

        block_copy(turn, 0, me, partner).wait_send()
        each(chips, sent)

    def slot_of(d, j):
        return wrap(gx, -d, gx_count) * gy_count + wrap(gy, -2 * j, gy_count)

    def each_block(first_d, first_j, body):
        if total <= 64:
            for d in range(first_d, gx_count):
                for j in range(first_j, per_row):
                    body(d, j)
        else:
            pl.loop(first_d, gx_count)(lambda d: pl.loop(first_j, per_row)(lambda j: body(d, j)))

    def along_line(turn, d):
        return block_copy(turn, d, me, (wrap(gx, d, gx_count), gy))

    def across(turn, d, j):
        n = gx_count + d * (per_row - 1) + j - 1
        return block_copy(turn, n, slot_of(d, 0), (gx, wrap(gy, 2 * j, gy_count)))

    def to_partner(turn, d, j):
        return block_copy(turn, chips + d * per_row + j, slot_of(d, j), partner)

    def from_partner(turn, d, j):
        return block_copy(turn, 0, slot_of(d, j) + 1 - 2 * core, partner)

    def line_start(turn):
        block_copy(turn, 0, me, partner).start()
        each(gx_count, lambda d: along_line(turn, gx_count - d).start())

    def line_pass(turn):
        def pass_line(d):
            block_copy(turn, 0, slot_of(d, 0), partner).wait_recv()
            each(per_row, lambda j: across(turn, d, per_row - j).start())
            to_partner(turn, d, 0).start()

        each(gx_count, pass_line)

    def line_wait(turn):
        def pass_block(d, j):
            copy = to_partner(turn, d, j)
            copy.wait_recv()
            copy.start()

        each_block(0, 1, pass_block)
        each_block(0, 0, lambda d, j: from_partner(turn, d, j).wait_recv())

    def line_sent(turn):
        block_copy(turn, 0, me, partner).wait_send()
        each(gx_count, lambda d: along_line(turn, d).wait_send())
        each_block(0, 1, lambda d, j: across(turn, d, j).wait_send())
        each_block(1, 0, lambda d, j: to_partner(turn, d, j).wait_send())
        each(per_row, lambda j: to_partner(turn, 0, j).wait_send())

    gE[base : base + rows, 0:cols] = g_ref[...]
    sE[base : base + rows, 0:cols] = s_ref[...]

    own_strips = cols // lanes
    for k in range(own_strips):
        fine_add[k, base : base + rows, :] = s_ref[:, k * lanes : (k + 1) * lanes]
    own = get_strips(fine_add, pl.ds(base, half_rows, 2), own_strips)
    own = own + get_strips(fine_add, pl.ds(base + 1, half_rows, 2), own_strips)
    put_strips(r1, slice(base1, base1 + half_rows), 0.25 * exact_dot(own, down0[0:cols, :]))
    rbuf[0, me] = pack_level2(r1)
    line_start(0)
    for n in range(len(bits)):
        pl.semaphore_wait(told.at[n], 1)
        if n < len(bits) - 1:
            tell(n + 1)
    each(per_row, lambda j: across(0, 0, per_row - j).start())
    zero_tile = jnp.zeros((ROWS_PAD, width), F32)
    for ref in (vA, vB):
        ref[0:ROWS_PAD, :] = zero_tile
        ref[ext - ROWS_PAD : ext, :] = zero_tile
    for ref in (aP, bP, a1, b1):
        ref[0:ROWS_PAD, :] = jnp.zeros((ROWS_PAD, width1), F32)
        ref[ref.shape[0] - ROWS_PAD :, :] = jnp.zeros((ROWS_PAD, width1), F32)
    for ref in (a2, b2, a3, b3, a4):
        for i in range(ref.shape[0]):
            ref[i, 0:8, :] = jnp.zeros((8, q_count), F32)
            ref[i, 8 + p_count : 16 + p_count, :] = jnp.zeros((8, q_count), F32)

    for n, (dx, dy, source, target) in enumerate(sends):
        @pl.when(inside(-dx, -dy))
        def _():
            halo_copy(n, -dx, -dy, source, target).wait_recv()

    lane_e = iota((ext, lanes), 1)
    gE[:, cols:width] = jnp.where(lane_e < half, recv_r[...], recv_l[...])
    sE[:, cols:width] = pltpu.roll(jnp.where(lane_e < half, recv_l[...], recv_r[...]), half, 1)

    def weight(shifts, first_row, own_rows, own_cols, split, level):
        shape = shifts.shape
        at_row = gx * own_rows + iota(shape, 0) + first_row
        lane_at = iota(shape, 1)
        at_col = gy * own_cols + jnp.where(lane_at < own_cols + split, lane_at, lane_at - shape[1])
        good = (at_row >= 0) & (at_row < gx_count * own_rows)
        good = good & (at_col >= 0) & (at_col < gy_count * own_cols)
        return jnp.where(good, DAMPING / (4.0 ** (1 - level) + shifts), 0.0)

    def around(v, lo, size):
        span = v.shape[1]
        mid = v[lo : lo + size, :]
        beside = pltpu.roll(mid, 1, 1) + pltpu.roll(mid, span - 1, 1)
        return mid, beside + (v[lo - 1 : lo - 1 + size, :] + v[lo + 1 : lo + 1 + size, :])

    def sweep_block(v, out, g, w, level, span=None):
        scale = 4.0 ** (-level)
        for lo in range(*(span or (ROWS_PAD, v.shape[0] - ROWS_PAD)), 8):
            mid, beside = around(v, lo, 8)
            at = slice(lo, lo + 8)
            out[at, :] = (1.0 - DAMPING) * mid + w[at, :] * (g[at, :] + scale * beside)

    def residual_block(v, out, g, s, level, span=None):
        scale = 4.0 ** (-level)
        for lo in range(*(span or (ROWS_PAD, v.shape[0] - ROWS_PAD)), 8):
            mid, beside = around(v, lo, 8)
            at = slice(lo, lo + 8)
            put_strips(out, at, g[at, :] - (scale * (4.0 * mid - beside) + s[at, :] * mid))

    row_moves = (
        (-1, sP.at[base1 : base1 + ROW_HALO, :], s1.at[base_w + half_rows : base_w + half_rows + ROW_HALO, :]),
        (1, sP.at[base1 + half_rows - ROW_HALO : base1 + half_rows, :], s1.at[ROWS_PAD:base_w, :]),
        (-1, gP.at[base1 : base1 + ROW_HALO, :], g1.at[base_w + half_rows : base_w + half_rows + ROW_HALO, :]),
        (1, gP.at[base1 + half_rows - ROW_HALO : base1 + half_rows, :], g1.at[ROWS_PAD:base_w, :]),
    )

    def row_copy(n, dx):
        _, source, target = row_moves[n]
        return pltpu.make_async_remote_copy(
            src_ref=source, dst_ref=target, send_sem=row_send.at[n], recv_sem=row_recv.at[n],
            device_id=(gx + dx, gy), device_id_type=MESH,
        )

    def rows_start(which):
        for n in which:
            dx = row_moves[n][0]
            @pl.when(inside(dx, 0))
            def _():
                row_copy(n, dx).start()

    def halved():
        pairs = get_strips(fine_add, pl.ds(0, ext1, 2)) + get_strips(fine_add, pl.ds(1, ext1, 2))
        return 0.25 * exact_dot(pairs, down0[...])

    put_strips(fine_add, slice(0, ext), sE[...])
    sP[near1, :] = halved()
    rows_start((0, 1))
    chunk = 16
    for lo in range(0, ext, chunk):
        at = slice(lo, lo + chunk)
        wE[at, :] = weight(sE[at, :], lo - base, rows, cols, half, 0)
    for lo in range(ROWS_PAD, ext - ROWS_PAD, 8):
        at = slice(lo, lo + 8)
        vA[at, :] = wE[at, :] * gE[at, :]
    sweep_block(vA, vB, gE, wE, 0)
    put_strips(fine_add, slice(0, ROWS_PAD), zero_tile)
    put_strips(fine_add, slice(ext - ROWS_PAD, ext), zero_tile)
    residual_block(vB, fine_add, gE, sE, 0)
    gP[near1, :] = halved()
    wP[near1, :] = weight(sP[near1, :], ROWS_PAD - base1, half_rows, cols // 2, half // 2, 1)
    aP[near1, :] = wP[near1, :] * gP[near1, :]
    sweep_block(aP, bP, gP, wP, 1)
    residual_block(bP, r1, gP, sP, 1, (base1, base1 + half_rows))
    rbuf[1, me] = pack_level2(r1)
    gather_start(1)
    line_pass(0)

    block = (lane_e[0:8] // 16)

    def unpack(turn, target):
        for x in range(gx_count):
            for u in range(gy_count // 8):
                for tl in range(2):
                    tiles = [rbuf[turn, x * gy_count + u * 8 + g, tl * 8 : tl * 8 + 8, :] for g in range(8)]
                    tiles = [tiles[-b % 8] for b in range(8)]
                    for bit in (1, 2, 4):
                        keep = (block & bit) == 0
                        tiles = [jnp.where(keep, tiles[b], tiles[(b - bit) % 8]) for b in range(8)]
                    for b in range(8):
                        t, r = (b // 4) * 2 + tl, b % 4
                        target[t * 4 + r, 8 * x : 8 * x + 8, u * lanes : (u + 1) * lanes] = pltpu.roll(
                            tiles[b], (lanes - 16 * b) % lanes, 1
                        )

    lane_q = iota((p_count, q_count), 1)
    rows_q = slice(8, 8 + p_count)

    def sides(v, n, t, r):
        mid = v[t * n + r, rows_q, :]
        if t > 0:
            north = v[(t - 1) * n + r, rows_q, :]
        else:
            north = v[(n - 1) * n + r, 7 : 7 + p_count, :]
        if t < n - 1:
            south = v[(t + 1) * n + r, rows_q, :]
        else:
            south = v[r, 9 : 9 + p_count, :]
        if r > 0:
            west = v[t * n + r - 1, rows_q, :]
        else:
            west = jnp.where(lane_q == 0, 0.0, pltpu.roll(v[t * n + n - 1, rows_q, :], 1, 1))
        if r < n - 1:
            east = v[t * n + r + 1, rows_q, :]
        else:
            east = jnp.where(
                lane_q == q_count - 1, 0.0, pltpu.roll(v[t * n, rows_q, :], q_count - 1, 1)
            )
        return mid, (north + south) + (west + east)

    level_refs = {2: (s2, w2, g2, a2, b2, 4), 3: (s3, w3, g3, a3, b3, 2), 4: (s4, w4, g4, a4, None, 1)}

    def sweep(level, v, out):
        s, w, g, _, _, n = level_refs[level]
        for t in range(n):
            for r in range(n):
                i = t * n + r
                mid, beside = sides(v, n, t, r)
                out[i, rows_q, :] = (1.0 - DAMPING) * mid + w[i] * (g[i] + 4.0 ** (-level) * beside)

    def first_sweep(level, out):
        s, w, g, _, _, n = level_refs[level]
        for i in range(n * n):
            out[i, rows_q, :] = w[i] * g[i]

    def restricted(level, v):
        s, w, g, _, _, n = level_refs[level]
        coarse_g = level_refs[level + 1][2]
        for t in range(n // 2):
            for r in range(n // 2):
                sums = None
                for dt in range(2):
                    for dr in range(2):
                        i = (2 * t + dt) * n + 2 * r + dr
                        mid, beside = sides(v, n, 2 * t + dt, 2 * r + dr)
                        left = g[i] - (4.0 ** (-level) * (4.0 * mid - beside) + s[i] * mid)
                        sums = left if sums is None else sums + left
                coarse_g[t * (n // 2) + r] = 0.25 * sums

    def correct(level, v, e):
        n = level_refs[level][5]
        for t in range(n):
            for r in range(n):
                i = t * n + r
                v[i, rows_q, :] = v[i, rows_q, :] + e[(t // 2) * (n // 2) + r // 2, rows_q, :]

    def prepare(level):
        s, w, _, _, _, n = level_refs[level]
        for i in range(n * n):
            w[i] = DAMPING / (4.0 ** (1 - level) + s[i])
        if level < 4:
            coarse_s = level_refs[level + 1][0]
            m = n // 2
            for t in range(m):
                for r in range(m):
                    i = 2 * t * n + 2 * r
                    coarse_s[t * m + r] = 0.25 * ((s[i] + s[i + n]) + (s[i + 1] + s[i + n + 1]))

    def total_of(x):
        return jnp.sum(jnp.sum(x, axis=0, keepdims=True), axis=1, keepdims=True)

    window = picked.shape[1] - 8
    lane_w, row_w = iota((window, lanes), 1), iota((window, lanes), 0)

    def in_domain(period):
        at_p, at_q = gx * 8 - 4 + row_w, gy * 16 - 8 + lane_w % period
        good = (at_p >= 0) & (at_p < p_count) & (at_q >= 0) & (at_q < q_count)
        return good & (lane_w % period < 32)

    def put_window(t, values):
        for a in range(2):
            put_strips(r1, pl.ds(ROWS_PAD + 2 * t + a, window, 8), values)

    def add_level2(e, v):
        for t in range(4):
            tiles = [e[t * 4 + r, pl.ds(pl.multiple_of(gx * 8, 8), 24), :] for r in range(4)]
            picked[t] = exact_dot(jnp.concatenate(tiles, 1), spread[...])
        for t in range(4):
            put_window(t, picked[t, 4 : 4 + window, :])
        v[wide1, :] = v[wide1, :] + get_strips(r1, wide1)

    def pack_window(source):
        parts = []
        for t in range(4):
            start = ROWS_PAD + 2 * t
            parts.append(
                get_strips(source, pl.ds(start, window, 8)) + get_strips(source, pl.ds(start + 1, window, 8))
            )
        means = 0.25 * exact_dot(jnp.concatenate(parts, 0), down_w[...])
        return [means[t * window : (t + 1) * window] for t in range(4)]

    def joined(x, unit):
        return x + pltpu.roll(x, lanes - unit, 1)

    def halved_window(tiles, unit):
        return [0.25 * joined(tiles[2 * t] + tiles[2 * t + 1], unit) for t in range(len(tiles) // 2)]

    def beside_window(v, unit):
        n = len(v)
        out = []
        for t in range(n):
            north = v[t - 1] if t > 0 else pltpu.roll(v[n - 1], 1, 0)
            south = v[t + 1] if t < n - 1 else pltpu.roll(v[0], window - 1, 0)
            west = jnp.where(lane_w < unit, pltpu.roll(v[t], unit + 1, 1), pltpu.roll(v[t], unit, 1))
            east = jnp.where(
                lane_w >= lanes - unit,
                pltpu.roll(v[t], lanes - unit - 1, 1), pltpu.roll(v[t], lanes - unit, 1),
            )
            out.append((north + south) + (west + east))
        return out

    window_refs = {2: (s2w, w2w, 32), 3: (s3w, w3w, 64)}

    def sweep_window(level, v, g):
        _, w, unit = window_refs[level]
        beside = beside_window(v, unit)
        return [
            (1.0 - DAMPING) * v[t] + w[t] * (g[t] + 4.0 ** (-level) * beside[t]) for t in range(len(v))
        ]

    def residual_window(level, v, g):
        s, _, unit = window_refs[level]
        beside = beside_window(v, unit)
        return [
            g[t] - (4.0 ** (-level) * (4.0 * v[t] - beside[t]) + s[t] * v[t]) for t in range(len(v))
        ]

    def rows_wait(which):
        for n in which:
            dx = row_moves[n][0]
            @pl.when(inside(-dx, 0))
            def _():
                row_copy(n, -dx).wait_recv()

    own1, own_w = slice(base1, base1 + half_rows), slice(base_w, base_w + half_rows)
    rows_wait((0, 1))
    s1[own_w, :] = sP[own1, :]
    w1[wide1, :] = weight(s1[wide1, :], ROWS_PAD - base_w, half_rows, cols // 2, half // 2, 1)
    put_strips(r1, wide1, s1[wide1, :])
    tiles = pack_window(r1)
    for t in range(4):
        s2w[t] = tiles[t]
        w2w[t] = jnp.where(in_domain(32), DAMPING / (4.0 ** (-1) + tiles[t]), 0.0)
    tiles = halved_window(tiles, 32)
    for t in range(2):
        s3w[t] = tiles[t]
        w3w[t] = jnp.where(in_domain(64), DAMPING / (4.0 ** (-2) + tiles[t]), 0.0)

    line_wait(0)
    unpack(0, s2)
    for level in (2, 3, 4):
        prepare(level)
    row_q = iota((p_count, q_count), 0)
    edges = jnp.where(row_q == 0, 1.0, 0.0) + jnp.where(row_q == p_count - 1, 1.0, 0.0)
    edges = edges + jnp.where(lane_q == 0, 1.0, 0.0) + jnp.where(lane_q == q_count - 1, 1.0, 0.0)
    unit4 = 4.0 ** (-4) * edges + s4[0]
    per_unit = 1.0 / total_of(unit4)

    def shifted(x, reach):
        out = {0: x}
        for k in range(1, reach + 1):
            out[k] = jnp.where(lane_q < q_count - k, pltpu.roll(x, q_count - k, 1), 0.0)
            out[-k] = jnp.where(lane_q >= k, pltpu.roll(x, k, 1), 0.0)
        return out

    reach4 = 2
    for k, values in shifted(4.0 ** (-4) * w4[0], reach4).items():
        hw4[k + reach4] = values
    for i in range(beside4.shape[0]):
        beside4[i, 0:8, :] = jnp.zeros((8, q_count), F32)
        beside4[i, 8 + p_count : 16 + p_count, :] = jnp.zeros((8, q_count), F32)

    def fused_sweeps(v, source, count, first_slot=0):
        for turn in range(count):
            reach = count - 1 - turn
            new = {}
            for k in range(-reach, reach + 1):
                slot = first_slot + (turn % 2) * 5 + k + reach4
                beside4[slot, rows_q, :] = v[k]
                along = beside4[slot, 7 : 7 + p_count, :] + beside4[slot, 9 : 9 + p_count, :]
                value = (1.0 - DAMPING) * v[k] + hw4[k + reach4] * ((v[k - 1] + v[k + 1]) + along)
                new[k] = value if source is None else value + source[k]
            v = new
        return v[0]

    def six_sweeps(v, source, first_slot=0):
        v = fused_sweeps(shifted(v, 3), source, 3, first_slot)
        return fused_sweeps(shifted(v, 3), source, 3, first_slot)

    def coarse(twice=False):
        source = shifted(w4[0] * g4[0], 3)
        v = fused_sweeps(source, source, 3)
        v = fused_sweeps(shifted(v, 2), source, 2)
        add = total_of(g4[0]) * per_unit
        if twice:
            phi[0] = six_sweeps(jnp.ones((p_count, q_count), F32), None, 10)
            phi[1] = six_sweeps(phi[0], None, 10)
            kept = 1.0 - per_unit * total_of(unit4 * phi[0])
            again = add * kept - total_of(unit4 * v) * per_unit
            v = six_sweeps(v, source) + add * phi[1] + again * phi[0]
        else:
            v = v + add * phi[0]
        a4[0, rows_q, :] = v
        return a4

    def vcycle(level, v):
        if level == 4:
            return coarse()
        _, _, _, a, b, n = level_refs[level]
        if v is None:
            first_sweep(level, a)
            sweep(level, a, b)
            now, later = b, a
        else:
            later = b if v is a else a
            sweep(level, v, later)
            sweep(level, later, v)
            now = v
        restricted(level, now)
        correct(level, now, vcycle(level + 1, None))
        sweep(level, now, later)
        sweep(level, later, now)
        return now

    def fcycle(level):
        _, _, _, a, b, n = level_refs[level]
        first_sweep(level, a)
        sweep(level, a, b)
        restricted(level, b)
        if level == 3:
            e = coarse(True)
        else:
            e = vcycle(level + 1, fcycle(level + 1))
        correct(level, b, e)
        sweep(level, b, a)
        sweep(level, a, b)
        return b

    def coarse_send(k):
        n = zigzag(total - k, total)
        pltpu.make_async_remote_copy(
            src_ref=cbuf.at[me], dst_ref=cbuf.at[me], send_sem=coarse_sems.at[0], recv_sem=coarse_sems.at[1],
            device_id=(wrap(gx, n // gy_count, gx_count), wrap(gy, n % gy_count, gy_count)), device_id_type=MESH,
        ).start()

    def coarse_wait(n):
        others = cbuf.at[pl.ds(0, total - 1)]
        pltpu.make_async_copy(others, others, coarse_sems.at[n]).wait()

    gather_wait(1)
    rows_start((2, 3))
    unpack(1, g2)
    e = fcycle(2)
    e = vcycle(2, e)
    rows_wait((2, 3))
    g1[own_w, :] = gP[own1, :]
    a1[wide1, :] = w1[wide1, :] * g1[wide1, :]
    sweep_block(a1, b1, g1, w1, 1)
    add_level2(e, b1)
    sweep_block(b1, a1, g1, w1, 1)
    sweep_block(a1, b1, g1, w1, 1)
    sweep_block(b1, a1, g1, w1, 1)
    sweep_block(a1, b1, g1, w1, 1)
    residual_block(b1, r1, g1, s1, 1)
    source2 = pack_window(r1)
    v2 = sweep_window(2, [w2w[t] * source2[t] for t in range(4)], source2)
    source3 = halved_window(residual_window(2, v2, source2), 32)
    v3 = sweep_window(3, [w3w[t] * source3[t] for t in range(2)], source3)
    left3 = residual_window(3, v3, source3)
    left3 = 0.25 * (left3[0] + left3[1])
    place = lax.rem(gy, 8) * 16
    turns = lax.rem(place + lanes - 8, lanes), lax.rem(place + lanes + half - 8, lanes)
    lane_c = iota((4, lanes), 1)
    upper, lower = (
        pltpu.roll(left3[at : at + 4], turns[0], 1) + pltpu.roll(left3[at : at + 4], turns[1], 1) for at in (4, 8)
    )
    after = (lane_c + lanes - place) % lanes
    cbuf[me] = jnp.where(after < 16, upper, jnp.where((after >= half) & (after < half + 16), lower, 0.0))
    each(total, coarse_send)
    line_sent(0)
    gather_sent(1)
    for n, (dx, dy, source, target) in enumerate(sends):
        @pl.when(inside(dx, dy))
        def _():
            halo_copy(n, dx, dy, source, target).wait_send()
    for n, (dx, _, _) in enumerate(row_moves):
        @pl.when(inside(dx, 0))
        def _():
            row_copy(n, dx).wait_send()
    coarse_wait(1)
    for x in range(gx_count):
        for u in range(gy_count // 8):
            first = x * gy_count + u * 8
            left, right = (
                (cbuf[k] + cbuf[k + 1]) + (cbuf[k + 2] + cbuf[k + 3]) for k in (first, first + 4)
            )
            at = slice(u * lanes, (u + 1) * lanes)
            g4[0, x * 8 : x * 8 + 4, at] = jnp.where(lane_c < half, left, right)
            g4[0, x * 8 + 4 : x * 8 + 8, at] = pltpu.roll(jnp.where(lane_c < half, right, left), half, 1)
    e = coarse()
    e = e[0, pl.ds(pl.multiple_of(gx * 8, 8), 24), :][4 : 4 + window]
    near_e, far_e = (
        pltpu.roll(e, lax.rem(2 * q_count + 8 + k - gy * 16, q_count), 1)[:, 0:lanes] for k in (0, half)
    )
    e = jnp.where(in_domain(half), jnp.where(lane_w < half, near_e, far_e), 0.0)
    v3 = [v3[t] + e for t in range(2)]
    v3 = sweep_window(3, sweep_window(3, v3, source3), source3)
    e = [v3[t] + pltpu.roll(v3[t], 32, 1) for t in range(2)]
    v2 = [v2[t] + e[t // 2] for t in range(4)]
    v2 = sweep_window(2, sweep_window(2, v2, source2), source2)
    raised = exact_dot(jnp.concatenate(v2, 0), up_w[...])
    for t in range(4):
        put_window(t, raised[t * window : (t + 1) * window])
    b1[wide1, :] = b1[wide1, :] + get_strips(r1, wide1)
    near_w = (base_w - 8, base_w + half_rows + 8)
    sweep_block(b1, a1, g1, w1, 1, near_w)
    sweep_block(a1, b1, g1, w1, 1, near_w)
    raised = exact_dot(b1[slice(*near_w), :], up0[...])
    put_strips(fine_add, pl.ds(0, ext1, 2), raised)
    put_strips(fine_add, pl.ds(1, ext1, 2), raised)
    for lo in range(ROWS_PAD, ext - ROWS_PAD, 8):
        at = slice(lo, lo + 8)
        vB[at, :] = vB[at, :] + get_strips(fine_add, at)
    sweep_block(vB, vA, gE, wE, 0)
    sweep_block(vA, vB, gE, wE, 0)
    for lo in range(0, rows, 8):
        mid, beside = around(vB, base + lo, 8)
        at = slice(base + lo, base + lo + 8)
        left = gE[at, :] - ((4.0 * mid - beside) + sE[at, :] * mid)
        out_ref[0, lo : lo + 8, :] = mid[:, 0:cols]
        out_ref[1, lo : lo + 8, :] = left[:, 0:cols]

    coarse_wait(0)


def solution(mesh):
    gx_count, gy_count = mesh.shape["gx"], mesh.shape["gy"]
    total = gx_count * gy_count

    def body(right_side, shift):
        rows, cols = right_side.shape
        assert cols == 256 and rows == 128 and gy_count % 8 == 0 and gy_count & (gy_count - 1) == 0
        ext, width = rows + 2 * (HALO + ROWS_PAD), cols + 128
        ext1, width1 = ext // 2 + 2 * ROWS_PAD, 256
        wide1 = rows // 2 + 2 * (ROW_HALO + ROWS_PAD)
        window = rows // 16 + 8
        p, q = rows // 16 * gx_count, cols // 16 * gy_count
        V = pltpu.VMEM
        dma = pltpu.SemaphoreType.DMA
        big = [V((ext, width), F32)] * 5 + [V((width // 128, ext, 128), F32)]
        one = [V((ext1, width1), F32)] * 5
        one += [V((wide1, width1), F32)] * 5 + [V((width1 // 128, wide1, 128), F32)]
        levels = []
        for n in (16, 4, 1):
            levels += [V((n, p, q), F32)] * 3 + [V((n, p + 16, q), F32)] * (2 if n > 1 else 1)
        scratch = (
            [V((rows, cols), F32)] * 2 + [dma((2,))]
            + big + one
            + [V((rows, 128), F32)] * 2 + [V((ext, 128), F32)] * 2
            + [V((width, width1), BF16), V((width1, width), BF16), V((width1, 128), BF16), V((4 * q, width1), BF16)]
            + [V((width1, 128), BF16), V((128, width1), BF16)]
            + [V((2, total, 16, 128), F32), V((total, 4, 128), F32)]
            + levels
            + [V((4, 24, width1), F32)]
            + [V((4, window, 128), F32)] * 2 + [V((2, window, 128), F32)] * 2
            + [V((5, p, q), F32), V((2, p, q), F32), V((20, p + 16, q), F32)]
            + [dma((10,)), dma((10,)), dma((4,)), dma((4,)), dma((2, total)), dma((2, total)), dma((2,))]
            + [pltpu.SemaphoreType.REGULAR((gy_count.bit_length() - 1,))]
        )
        out = pltpu.VMEM((2,) + right_side.shape, F32)
        both = pl.pallas_call(
            functools.partial(kernel, gx_count, gy_count),
            out_shape=out,
            in_specs=[pl.BlockSpec(memory_space=pltpu.HBM)] * 2,
            out_specs=pl.BlockSpec(memory_space=pltpu.VMEM),
            scratch_shapes=scratch,
            compiler_params=pltpu.CompilerParams(
                collective_id=0, has_side_effects=True, vmem_limit_bytes=60*1024*1024
            ),
        )(right_side, shift)
        return both[0], both[1]

    spec = P("gx", "gy")
    return jax.shard_map(body, mesh=mesh, in_specs=(spec, spec), out_specs=(spec, spec), check_vma=False)
```

```python
import functools

import jax
import jax.numpy as jnp
from jax import lax
from jax.experimental import pallas as pl
from jax.experimental.pallas import tpu as pltpu
from jax.sharding import PartitionSpec as P

DAMPING = 0.8
MESH = pl.DeviceIdType.MESH
F32 = jnp.float32
BF16 = jnp.bfloat16

ROWS_PAD = 8
HALO = 8
ROW_HALO = 32


def iota(shape, dim):
    return lax.broadcasted_iota(jnp.int32, shape, dim)


def put_strips(ref, at, values):
    for k in range(ref.shape[0]):
        ref[k, at, :] = values[:, k * 128 : (k + 1) * 128]


def get_strips(ref, at, count=None):
    return jnp.concatenate([ref[k, at, :] for k in range(count or ref.shape[0])], 1)


def exact_dot(values, selector):
    first = values.astype(BF16)
    rest = values - first.astype(F32)
    second = rest.astype(BF16)
    third = (rest - second.astype(F32)).astype(BF16)
    dot = functools.partial(jnp.dot, preferred_element_type=F32)
    return dot(first, selector) + (dot(second, selector) + dot(third, selector))


def kernel(
    gx_count, gy_count, g_hbm, s_hbm, out_ref,
    g_ref, s_ref, load_sem,
    gE, sE, wE, vA, vB, fine_add,
    gP, sP, wP, aP, bP,
    g1, s1, w1, a1, b1, r1,
    send_l, send_r, recv_l, recv_r,
    down0, up0, down1, spread, down_w, up_w,
    rbuf, cbuf, s2, w2, g2, a2, b2, s3, w3, g3, a3, b3, s4, w4, g4, a4, picked,
    s2w, w2w, s3w, w3w, hw4, phi, beside4,
    halo_send, halo_recv, row_send, row_recv, all_send, all_recv, coarse_sems, told,
):
    gx, gy = lax.axis_index("gx"), lax.axis_index("gy")
    total = gx_count * gy_count
    me = gx * gy_count + gy
    rows, cols = g_hbm.shape
    base = ROWS_PAD + HALO
    base1 = ROWS_PAD + (ROWS_PAD + HALO) // 2
    ext, width = gE.shape
    ext1, width1 = ext // 2, g1.shape[1]
    half_rows = rows // 2
    base_w = ROWS_PAD + ROW_HALO
    near1 = slice(ROWS_PAD, ROWS_PAD + ext1)
    wide1 = slice(ROWS_PAD, base_w + half_rows + ROW_HALO)
    lanes = 128

    load_g = pltpu.make_async_copy(g_hbm, g_ref, load_sem.at[0])
    load_s = pltpu.make_async_copy(s_hbm, s_ref, load_sem.at[1])
    load_g.start()
    load_s.start()
    zero_halo = jnp.zeros((base, width), F32)
    for ref in (gE, sE):
        ref[0:base, :] = zero_halo
        ref[base + rows : ext, :] = zero_halo
    for ref in (recv_l, recv_r):
        ref[...] = jnp.zeros(ref.shape, F32)
    for ref in (g1, s1):
        ref[0:base_w, :] = jnp.zeros((base_w, width1), F32)
        ref[base_w + half_rows :, :] = jnp.zeros((base_w, width1), F32)
    def inside(dx, dy):
        ok = None
        for step, at, count in ((dx, gx, gx_count), (dy, gy, gy_count)):
            if step:
                here = (at > 0) if step < 0 else (at < count - 1)
                ok = here if ok is None else ok & here
        return ok

    def wrap(at, step, count):
        return lax.rem(at + count + step, count)

    def each(count, body):
        if count <= 64:
            for j in range(1, count):
                body(j)
        else:
            pl.loop(1, count)(body)

    barrier = pltpu.get_barrier_semaphore()
    corners = [(dx, dy) for dx in (-1, 1) for dy in (-1, 1)]

    def greet(x, y):
        pl.semaphore_signal(barrier, inc=1, device_id=(x, y), device_id_type=MESH)

    each(gx_count, lambda k: greet(wrap(gx, k, gx_count), gy))
    for dx, dy in corners:
        @pl.when(inside(dx, dy))
        def _():
            greet(gx + dx, gy + dy)

    bits = [1 << b for b in range(1, gy_count.bit_length() - 1)] + [1]

    def flip(bit):
        return gy + bit * (1 - 2 * lax.rem(gy // bit, 2))

    for bit in bits[:-1]:
        greet(gx, flip(bit))
    for dy in (-1, 1):
        @pl.when(inside(0, dy))
        def _():
            greet(gx, gy + dy)


    lane = iota((rows, lanes), 1)
    half = lanes // 2
    l0 = iota((width, width1), 0)
    col0 = jnp.where(l0 < cols + half, l0, l0 - width)
    down0[...] = jnp.where(
        ((col0 + 2 * width1) // 2) % width1 == iota((width, width1), 1), 1.0, 0.0
    ).astype(BF16)
    l0 = iota((width1, width), 1)
    col0 = jnp.where(l0 < cols + half, l0, l0 - width)
    up0[...] = jnp.where(
        ((col0 + 2 * width1) // 2) % width1 == iota((width1, width), 0), 1.0, 0.0
    ).astype(BF16)
    l1 = iota((width1, lanes), 0)
    j2 = l1 // 2
    place = ((j2 + gy) % 4) * 16 + j2 // 4
    down1[...] = jnp.where(
        (l1 < lanes) & (iota((width1, lanes), 1) % half == place), 1.0, 0.0
    ).astype(BF16)
    q_count = s2.shape[2]
    p_count = s2.shape[1]
    m1 = iota((q_count, width1), 1)
    col1 = jnp.where(m1 < lanes + half // 2, m1, m1 - width1)
    wide = gy * half + (col1 + 512) // 2 - 256
    for r in range(4):
        spread[r * q_count : (r + 1) * q_count, :] = jnp.where(
            wide == 4 * iota((q_count, width1), 0) + r, 1.0, 0.0
        ).astype(BF16)

    load_g.wait()
    load_s.wait()
    send_l[...] = jnp.where(lane < half, g_ref[:, 0:lanes], pltpu.roll(s_ref[:, 0:lanes], half, 1))
    send_r[...] = jnp.where(
        lane < half, pltpu.roll(s_ref[:, cols - lanes : cols], half, 1), g_ref[:, cols - lanes : cols]
    )

    l1 = iota((width1, lanes), 0)
    at2 = (jnp.where(l1 < lanes + half // 2, l1, l1 - width1) + 2 * lanes) // 2
    at4 = at2 // 4 - 24
    down_w[...] = jnp.where(
        (at4 >= 0) & (at4 < 32) & (iota((width1, lanes), 1) == (at2 % 4) * 32 + at4), 1.0, 0.0
    ).astype(BF16)
    l1 = iota((lanes, width1), 1)
    at2 = (jnp.where(l1 < lanes + half // 2, l1, l1 - width1) + 2 * lanes) // 2
    at4 = at2 // 4 - 24
    up_w[...] = jnp.where(
        (at4 >= 0) & (at4 < 32) & (iota((lanes, width1), 0) == (at2 % 4) * 32 + at4), 1.0, 0.0
    ).astype(BF16)

    def pack_level2(source):
        parts = []
        for t in range(4):
            start = base1 + 2 * t
            parts.append(
                get_strips(source, pl.ds(start, 8, 8)) + get_strips(source, pl.ds(start + 1, 8, 8))
            )
        means = 0.25 * exact_dot(jnp.concatenate(parts, 0), down1[...])
        low = (iota((16, lanes), 1) // 16 + 8 - lax.rem(gy, 8)) % 8 < 4
        return jnp.where(low, means[0:16], means[16:32])

    def beside_count(at, count):
        return (at + count - 1) // count + 1 - (at + 1) // count

    pl.semaphore_wait(
        barrier,
        gx_count + len(bits) - 2 + beside_count(gy, gy_count) * (1 + beside_count(gx, gx_count)),
    )

    def tell(n):
        pl.semaphore_signal(told.at[n], inc=1, device_id=(gx, flip(bits[n])), device_id_type=MESH)

    tell(0)

    top, bottom = slice(0, HALO), slice(rows - HALO, rows)
    above, below = slice(ROWS_PAD, base), slice(base + rows, base + rows + HALO)
    middle = slice(base, base + rows)
    sends = (
        (-1, -1, send_l.at[top, :], recv_r.at[below, :]),
        (1, -1, send_l.at[bottom, :], recv_r.at[above, :]),
        (-1, 1, send_r.at[top, :], recv_l.at[below, :]),
        (1, 1, send_r.at[bottom, :], recv_l.at[above, :]),
        (-1, 0, g_ref.at[top, :], gE.at[below, 0:cols]),
        (-1, 0, s_ref.at[top, :], sE.at[below, 0:cols]),
        (1, 0, g_ref.at[bottom, :], gE.at[above, 0:cols]),
        (1, 0, s_ref.at[bottom, :], sE.at[above, 0:cols]),
        (0, -1, send_l, recv_r.at[middle, :]),
        (0, 1, send_r, recv_l.at[middle, :]),
    )

    def halo_copy(n, dx, dy, source, target):
        return pltpu.make_async_remote_copy(
            src_ref=source, dst_ref=target, send_sem=halo_send.at[n], recv_sem=halo_recv.at[n],
            device_id=(gx + dx, gy + dy), device_id_type=MESH,
        )

    for n, (dx, dy, source, target) in enumerate(sends):
        @pl.when(inside(dx, dy))
        def _():
            halo_copy(n, dx, dy, source, target).start()

    core = lax.rem(gy, 2)
    per_row = gy_count // 2
    chips = total // 2
    partner = (gx, gy + 1 - 2 * core)

    def zigzag(j, count):
        if total <= 64:
            width_of = count // gx_count
            lines = [0] + sorted(range(1, gx_count), key=lambda d: -abs(2 * d - gx_count))
            return lines[j // width_of] * width_of + j % width_of
        odd = j % 2
        return odd * ((j + 1) // 2) + (1 - odd) * (count - j // 2)

    def block_copy(turn, n, slot, peer):
        return pltpu.make_async_remote_copy(
            src_ref=rbuf.at[turn, slot], dst_ref=rbuf.at[turn, slot],
            send_sem=all_send.at[turn, n], recv_sem=all_recv.at[turn, slot],
            device_id=peer, device_id_type=MESH,
        )

    def direct(turn, j):
        n = zigzag(j, chips)
        peer = (wrap(gx, n // per_row, gx_count), wrap(gy, 2 * (n % per_row), gy_count))
        return block_copy(turn, j, me, peer)

    def sender(j):
        n = zigzag(j, chips)
        return wrap(gx, -(n // per_row), gx_count) * gy_count + wrap(gy, -2 * (n % per_row), gy_count)

    def onward(turn, j):
        return block_copy(turn, chips + j, sender(j), partner)

    def gather_start(turn):
        block_copy(turn, 0, me, partner).start()
        each(chips, lambda j: direct(turn, chips - j).start())

    def gather_wait(turn):
        def pass_block(j):
            copy = onward(turn, j)
            copy.wait_recv()
            copy.start()

        each(chips, pass_block)
        block_copy(turn, 0, me + 1 - 2 * core, partner).wait_recv()
        each(chips, lambda j: block_copy(turn, chips + j, sender(j) + 1 - 2 * core, partner).wait_recv())

    def gather_sent(turn):
        def sent(j):
            direct(turn, j).wait_send()
            onward(turn, j).wait_send()

        block_copy(turn, 0, me, partner).wait_send()
        each(chips, sent)

    def slot_of(d, j):
        return wrap(gx, -d, gx_count) * gy_count + wrap(gy, -2 * j, gy_count)

    def each_block(first_d, first_j, body):
        if total <= 64:
            for d in range(first_d, gx_count):
                for j in range(first_j, per_row):
                    body(d, j)
        else:
            pl.loop(first_d, gx_count)(lambda d: pl.loop(first_j, per_row)(lambda j: body(d, j)))

    def along_line(turn, d):
        return block_copy(turn, d, me, (wrap(gx, d, gx_count), gy))

    def across(turn, d, j):
        n = gx_count + d * (per_row - 1) + j - 1
        return block_copy(turn, n, slot_of(d, 0), (gx, wrap(gy, 2 * j, gy_count)))

    def to_partner(turn, d, j):
        return block_copy(turn, chips + d * per_row + j, slot_of(d, j), partner)

    def from_partner(turn, d, j):
        return block_copy(turn, 0, slot_of(d, j) + 1 - 2 * core, partner)

    def line_start(turn):
        block_copy(turn, 0, me, partner).start()
        each(gx_count, lambda d: along_line(turn, gx_count - d).start())

    def line_pass(turn):
        def pass_line(d):
            block_copy(turn, 0, slot_of(d, 0), partner).wait_recv()
            each(per_row, lambda j: across(turn, d, per_row - j).start())
            to_partner(turn, d, 0).start()

        each(gx_count, pass_line)

    def line_wait(turn):
        def pass_block(d, j):
            copy = to_partner(turn, d, j)
            copy.wait_recv()
            copy.start()

        each_block(0, 1, pass_block)
        each_block(0, 0, lambda d, j: from_partner(turn, d, j).wait_recv())

    def line_sent(turn):
        block_copy(turn, 0, me, partner).wait_send()
        each(gx_count, lambda d: along_line(turn, d).wait_send())
        each_block(0, 1, lambda d, j: across(turn, d, j).wait_send())
        each_block(1, 0, lambda d, j: to_partner(turn, d, j).wait_send())
        each(per_row, lambda j: to_partner(turn, 0, j).wait_send())

    gE[base : base + rows, 0:cols] = g_ref[...]
    sE[base : base + rows, 0:cols] = s_ref[...]

    own_strips = cols // lanes
    for k in range(own_strips):
        fine_add[k, base : base + rows, :] = s_ref[:, k * lanes : (k + 1) * lanes]
    own = get_strips(fine_add, pl.ds(base, half_rows, 2), own_strips)
    own = own + get_strips(fine_add, pl.ds(base + 1, half_rows, 2), own_strips)
    put_strips(r1, slice(base1, base1 + half_rows), 0.25 * exact_dot(own, down0[0:cols, :]))
    rbuf[0, me] = pack_level2(r1)
    line_start(0)
    for n in range(len(bits)):
        pl.semaphore_wait(told.at[n], 1)
        if n < len(bits) - 1:
            tell(n + 1)
    each(per_row, lambda j: across(0, 0, per_row - j).start())
    zero_tile = jnp.zeros((ROWS_PAD, width), F32)
    for ref in (vA, vB):
        ref[0:ROWS_PAD, :] = zero_tile
        ref[ext - ROWS_PAD : ext, :] = zero_tile
    for ref in (aP, bP, a1, b1):
        ref[0:ROWS_PAD, :] = jnp.zeros((ROWS_PAD, width1), F32)
        ref[ref.shape[0] - ROWS_PAD :, :] = jnp.zeros((ROWS_PAD, width1), F32)
    for ref in (a2, b2, a3, b3, a4):
        for i in range(ref.shape[0]):
            ref[i, 0:8, :] = jnp.zeros((8, q_count), F32)
            ref[i, 8 + p_count : 16 + p_count, :] = jnp.zeros((8, q_count), F32)

    for n, (dx, dy, source, target) in enumerate(sends):
        @pl.when(inside(-dx, -dy))
        def _():
            halo_copy(n, -dx, -dy, source, target).wait_recv()

    lane_e = iota((ext, lanes), 1)
    gE[:, cols:width] = jnp.where(lane_e < half, recv_r[...], recv_l[...])
    sE[:, cols:width] = pltpu.roll(jnp.where(lane_e < half, recv_l[...], recv_r[...]), half, 1)

    def weight(shifts, first_row, own_rows, own_cols, split, level):
        shape = shifts.shape
        at_row = gx * own_rows + iota(shape, 0) + first_row
        lane_at = iota(shape, 1)
        at_col = gy * own_cols + jnp.where(lane_at < own_cols + split, lane_at, lane_at - shape[1])
        good = (at_row >= 0) & (at_row < gx_count * own_rows)
        good = good & (at_col >= 0) & (at_col < gy_count * own_cols)
        return jnp.where(good, DAMPING / (4.0 ** (1 - level) + shifts), 0.0)

    def around(v, lo, size):
        span = v.shape[1]
        mid = v[lo : lo + size, :]
        beside = pltpu.roll(mid, 1, 1) + pltpu.roll(mid, span - 1, 1)
        return mid, beside + (v[lo - 1 : lo - 1 + size, :] + v[lo + 1 : lo + 1 + size, :])

    def sweep_block(v, out, g, w, level, span=None):
        scale = 4.0 ** (-level)
        for lo in range(*(span or (ROWS_PAD, v.shape[0] - ROWS_PAD)), 8):
            mid, beside = around(v, lo, 8)
            at = slice(lo, lo + 8)
            out[at, :] = (1.0 - DAMPING) * mid + w[at, :] * (g[at, :] + scale * beside)

    def residual_block(v, out, g, s, level, span=None):
        scale = 4.0 ** (-level)
        for lo in range(*(span or (ROWS_PAD, v.shape[0] - ROWS_PAD)), 8):
            mid, beside = around(v, lo, 8)
            at = slice(lo, lo + 8)
            put_strips(out, at, g[at, :] - (scale * (4.0 * mid - beside) + s[at, :] * mid))

    row_moves = (
        (-1, sP.at[base1 : base1 + ROW_HALO, :], s1.at[base_w + half_rows : base_w + half_rows + ROW_HALO, :]),
        (1, sP.at[base1 + half_rows - ROW_HALO : base1 + half_rows, :], s1.at[ROWS_PAD:base_w, :]),
        (-1, gP.at[base1 : base1 + ROW_HALO, :], g1.at[base_w + half_rows : base_w + half_rows + ROW_HALO, :]),
        (1, gP.at[base1 + half_rows - ROW_HALO : base1 + half_rows, :], g1.at[ROWS_PAD:base_w, :]),
    )

    def row_copy(n, dx):
        _, source, target = row_moves[n]
        return pltpu.make_async_remote_copy(
            src_ref=source, dst_ref=target, send_sem=row_send.at[n], recv_sem=row_recv.at[n],
            device_id=(gx + dx, gy), device_id_type=MESH,
        )

    def rows_start(which):
        for n in which:
            dx = row_moves[n][0]
            @pl.when(inside(dx, 0))
            def _():
                row_copy(n, dx).start()

    def halved():
        pairs = get_strips(fine_add, pl.ds(0, ext1, 2)) + get_strips(fine_add, pl.ds(1, ext1, 2))
        return 0.25 * exact_dot(pairs, down0[...])

    put_strips(fine_add, slice(0, ext), sE[...])
    sP[near1, :] = halved()
    rows_start((0, 1))
    chunk = 16
    for lo in range(0, ext, chunk):
        at = slice(lo, lo + chunk)
        wE[at, :] = weight(sE[at, :], lo - base, rows, cols, half, 0)
    for lo in range(ROWS_PAD, ext - ROWS_PAD, 8):
        at = slice(lo, lo + 8)
        vA[at, :] = wE[at, :] * gE[at, :]
    sweep_block(vA, vB, gE, wE, 0)
    put_strips(fine_add, slice(0, ROWS_PAD), zero_tile)
    put_strips(fine_add, slice(ext - ROWS_PAD, ext), zero_tile)
    residual_block(vB, fine_add, gE, sE, 0)
    gP[near1, :] = halved()
    wP[near1, :] = weight(sP[near1, :], ROWS_PAD - base1, half_rows, cols // 2, half // 2, 1)
    aP[near1, :] = wP[near1, :] * gP[near1, :]
    sweep_block(aP, bP, gP, wP, 1)
    residual_block(bP, r1, gP, sP, 1, (base1, base1 + half_rows))
    rbuf[1, me] = pack_level2(r1)
    gather_start(1)
    line_pass(0)

    block = (lane_e[0:8] // 16)

    def unpack(turn, target):
        for x in range(gx_count):
            for u in range(gy_count // 8):
                for tl in range(2):
                    tiles = [rbuf[turn, x * gy_count + u * 8 + g, tl * 8 : tl * 8 + 8, :] for g in range(8)]
                    tiles = [tiles[-b % 8] for b in range(8)]
                    for bit in (1, 2, 4):
                        keep = (block & bit) == 0
                        tiles = [jnp.where(keep, tiles[b], tiles[(b - bit) % 8]) for b in range(8)]
                    for b in range(8):
                        t, r = (b // 4) * 2 + tl, b % 4
                        target[t * 4 + r, 8 * x : 8 * x + 8, u * lanes : (u + 1) * lanes] = pltpu.roll(
                            tiles[b], (lanes - 16 * b) % lanes, 1
                        )

    lane_q = iota((p_count, q_count), 1)
    rows_q = slice(8, 8 + p_count)

    def sides(v, n, t, r):
        mid = v[t * n + r, rows_q, :]
        if t > 0:
            north = v[(t - 1) * n + r, rows_q, :]
        else:
            north = v[(n - 1) * n + r, 7 : 7 + p_count, :]
        if t < n - 1:
            south = v[(t + 1) * n + r, rows_q, :]
        else:
            south = v[r, 9 : 9 + p_count, :]
        if r > 0:
            west = v[t * n + r - 1, rows_q, :]
        else:
            west = jnp.where(lane_q == 0, 0.0, pltpu.roll(v[t * n + n - 1, rows_q, :], 1, 1))
        if r < n - 1:
            east = v[t * n + r + 1, rows_q, :]
        else:
            east = jnp.where(
                lane_q == q_count - 1, 0.0, pltpu.roll(v[t * n, rows_q, :], q_count - 1, 1)
            )
        return mid, (north + south) + (west + east)

    level_refs = {2: (s2, w2, g2, a2, b2, 4), 3: (s3, w3, g3, a3, b3, 2), 4: (s4, w4, g4, a4, None, 1)}

    def sweep(level, v, out):
        s, w, g, _, _, n = level_refs[level]
        for t in range(n):
            for r in range(n):
                i = t * n + r
                mid, beside = sides(v, n, t, r)
                out[i, rows_q, :] = (1.0 - DAMPING) * mid + w[i] * (g[i] + 4.0 ** (-level) * beside)

    def first_sweep(level, out):
        s, w, g, _, _, n = level_refs[level]
        for i in range(n * n):
            out[i, rows_q, :] = w[i] * g[i]

    def restricted(level, v):
        s, w, g, _, _, n = level_refs[level]
        coarse_g = level_refs[level + 1][2]
        for t in range(n // 2):
            for r in range(n // 2):
                sums = None
                for dt in range(2):
                    for dr in range(2):
                        i = (2 * t + dt) * n + 2 * r + dr
                        mid, beside = sides(v, n, 2 * t + dt, 2 * r + dr)
                        left = g[i] - (4.0 ** (-level) * (4.0 * mid - beside) + s[i] * mid)
                        sums = left if sums is None else sums + left
                coarse_g[t * (n // 2) + r] = 0.25 * sums

    def correct(level, v, e):
        n = level_refs[level][5]
        for t in range(n):
            for r in range(n):
                i = t * n + r
                v[i, rows_q, :] = v[i, rows_q, :] + e[(t // 2) * (n // 2) + r // 2, rows_q, :]

    def prepare(level):
        s, w, _, _, _, n = level_refs[level]
        for i in range(n * n):
            w[i] = DAMPING / (4.0 ** (1 - level) + s[i])
        if level < 4:
            coarse_s = level_refs[level + 1][0]
            m = n // 2
            for t in range(m):
                for r in range(m):
                    i = 2 * t * n + 2 * r
                    coarse_s[t * m + r] = 0.25 * ((s[i] + s[i + n]) + (s[i + 1] + s[i + n + 1]))

    def total_of(x):
        return jnp.sum(jnp.sum(x, axis=0, keepdims=True), axis=1, keepdims=True)

    window = picked.shape[1] - 8
    lane_w, row_w = iota((window, lanes), 1), iota((window, lanes), 0)

    def in_domain(period):
        at_p, at_q = gx * 8 - 4 + row_w, gy * 16 - 8 + lane_w % period
        good = (at_p >= 0) & (at_p < p_count) & (at_q >= 0) & (at_q < q_count)
        return good & (lane_w % period < 32)

    def put_window(t, values):
        for a in range(2):
            put_strips(r1, pl.ds(ROWS_PAD + 2 * t + a, window, 8), values)

    def add_level2(e, v):
        for t in range(4):
            tiles = [e[t * 4 + r, pl.ds(pl.multiple_of(gx * 8, 8), 24), :] for r in range(4)]
            picked[t] = exact_dot(jnp.concatenate(tiles, 1), spread[...])
        for t in range(4):
            put_window(t, picked[t, 4 : 4 + window, :])
        v[wide1, :] = v[wide1, :] + get_strips(r1, wide1)

    def pack_window(source):
        parts = []
        for t in range(4):
            start = ROWS_PAD + 2 * t
            parts.append(
                get_strips(source, pl.ds(start, window, 8)) + get_strips(source, pl.ds(start + 1, window, 8))
            )
        means = 0.25 * exact_dot(jnp.concatenate(parts, 0), down_w[...])
        return [means[t * window : (t + 1) * window] for t in range(4)]

    def joined(x, unit):
        return x + pltpu.roll(x, lanes - unit, 1)

    def halved_window(tiles, unit):
        return [0.25 * joined(tiles[2 * t] + tiles[2 * t + 1], unit) for t in range(len(tiles) // 2)]

    def beside_window(v, unit):
        n = len(v)
        out = []
        for t in range(n):
            north = v[t - 1] if t > 0 else pltpu.roll(v[n - 1], 1, 0)
            south = v[t + 1] if t < n - 1 else pltpu.roll(v[0], window - 1, 0)
            west = jnp.where(lane_w < unit, pltpu.roll(v[t], unit + 1, 1), pltpu.roll(v[t], unit, 1))
            east = jnp.where(
                lane_w >= lanes - unit,
                pltpu.roll(v[t], lanes - unit - 1, 1), pltpu.roll(v[t], lanes - unit, 1),
            )
            out.append((north + south) + (west + east))
        return out

    window_refs = {2: (s2w, w2w, 32), 3: (s3w, w3w, 64)}

    def sweep_window(level, v, g):
        _, w, unit = window_refs[level]
        beside = beside_window(v, unit)
        return [
            (1.0 - DAMPING) * v[t] + w[t] * (g[t] + 4.0 ** (-level) * beside[t]) for t in range(len(v))
        ]

    def residual_window(level, v, g):
        s, _, unit = window_refs[level]
        beside = beside_window(v, unit)
        return [
            g[t] - (4.0 ** (-level) * (4.0 * v[t] - beside[t]) + s[t] * v[t]) for t in range(len(v))
        ]

    def rows_wait(which):
        for n in which:
            dx = row_moves[n][0]
            @pl.when(inside(-dx, 0))
            def _():
                row_copy(n, -dx).wait_recv()

    own1, own_w = slice(base1, base1 + half_rows), slice(base_w, base_w + half_rows)
    rows_wait((0, 1))
    s1[own_w, :] = sP[own1, :]
    w1[wide1, :] = weight(s1[wide1, :], ROWS_PAD - base_w, half_rows, cols // 2, half // 2, 1)
    put_strips(r1, wide1, s1[wide1, :])
    tiles = pack_window(r1)
    for t in range(4):
        s2w[t] = tiles[t]
        w2w[t] = jnp.where(in_domain(32), DAMPING / (4.0 ** (-1) + tiles[t]), 0.0)
    tiles = halved_window(tiles, 32)
    for t in range(2):
        s3w[t] = tiles[t]
        w3w[t] = jnp.where(in_domain(64), DAMPING / (4.0 ** (-2) + tiles[t]), 0.0)

    line_wait(0)
    unpack(0, s2)
    for level in (2, 3, 4):
        prepare(level)
    row_q = iota((p_count, q_count), 0)
    edges = jnp.where(row_q == 0, 1.0, 0.0) + jnp.where(row_q == p_count - 1, 1.0, 0.0)
    edges = edges + jnp.where(lane_q == 0, 1.0, 0.0) + jnp.where(lane_q == q_count - 1, 1.0, 0.0)
    unit4 = 4.0 ** (-4) * edges + s4[0]
    per_unit = 1.0 / total_of(unit4)

    def shifted(x, reach):
        out = {0: x}
        for k in range(1, reach + 1):
            out[k] = jnp.where(lane_q < q_count - k, pltpu.roll(x, q_count - k, 1), 0.0)
            out[-k] = jnp.where(lane_q >= k, pltpu.roll(x, k, 1), 0.0)
        return out

    reach4 = 2
    for k, values in shifted(4.0 ** (-4) * w4[0], reach4).items():
        hw4[k + reach4] = values
    for i in range(beside4.shape[0]):
        beside4[i, 0:8, :] = jnp.zeros((8, q_count), F32)
        beside4[i, 8 + p_count : 16 + p_count, :] = jnp.zeros((8, q_count), F32)

    def fused_sweeps(v, source, count, first_slot=0):
        for turn in range(count):
            reach = count - 1 - turn
            new = {}
            for k in range(-reach, reach + 1):
                slot = first_slot + (turn % 2) * 5 + k + reach4
                beside4[slot, rows_q, :] = v[k]
                along = beside4[slot, 7 : 7 + p_count, :] + beside4[slot, 9 : 9 + p_count, :]
                value = (1.0 - DAMPING) * v[k] + hw4[k + reach4] * ((v[k - 1] + v[k + 1]) + along)
                new[k] = value if source is None else value + source[k]
            v = new
        return v[0]

    def six_sweeps(v, source, first_slot=0):
        v = fused_sweeps(shifted(v, 3), source, 3, first_slot)
        return fused_sweeps(shifted(v, 3), source, 3, first_slot)

    def coarse(twice=False):
        source = shifted(w4[0] * g4[0], 3)
        v = fused_sweeps(source, source, 3)
        v = fused_sweeps(shifted(v, 2), source, 2)
        add = total_of(g4[0]) * per_unit
        if twice:
            phi[0] = six_sweeps(jnp.ones((p_count, q_count), F32), None, 10)
            phi[1] = six_sweeps(phi[0], None, 10)
            kept = 1.0 - per_unit * total_of(unit4 * phi[0])
            again = add * kept - total_of(unit4 * v) * per_unit
            v = six_sweeps(v, source) + add * phi[1] + again * phi[0]
        else:
            v = v + add * phi[0]
        a4[0, rows_q, :] = v
        return a4

    def vcycle(level, v):
        if level == 4:
            return coarse()
        _, _, _, a, b, n = level_refs[level]
        if v is None:
            first_sweep(level, a)
            sweep(level, a, b)
            now, later = b, a
        else:
            later = b if v is a else a
            sweep(level, v, later)
            sweep(level, later, v)
            now = v
        restricted(level, now)
        correct(level, now, vcycle(level + 1, None))
        sweep(level, now, later)
        sweep(level, later, now)
        return now

    def fcycle(level):
        _, _, _, a, b, n = level_refs[level]
        first_sweep(level, a)
        sweep(level, a, b)
        restricted(level, b)
        if level == 3:
            e = coarse(True)
        else:
            e = vcycle(level + 1, fcycle(level + 1))
        correct(level, b, e)
        sweep(level, b, a)
        sweep(level, a, b)
        return b

    def coarse_send(k):
        n = zigzag(total - k, total)
        pltpu.make_async_remote_copy(
            src_ref=cbuf.at[me], dst_ref=cbuf.at[me], send_sem=coarse_sems.at[0], recv_sem=coarse_sems.at[1],
            device_id=(wrap(gx, n // gy_count, gx_count), wrap(gy, n % gy_count, gy_count)), device_id_type=MESH,
        ).start()

    def coarse_wait(n):
        others = cbuf.at[pl.ds(0, total - 1)]
        pltpu.make_async_copy(others, others, coarse_sems.at[n]).wait()

    gather_wait(1)
    rows_start((2, 3))
    unpack(1, g2)
    e = fcycle(2)
    e = vcycle(2, e)
    rows_wait((2, 3))
    g1[own_w, :] = gP[own1, :]
    a1[wide1, :] = w1[wide1, :] * g1[wide1, :]
    sweep_block(a1, b1, g1, w1, 1)
    add_level2(e, b1)
    sweep_block(b1, a1, g1, w1, 1)
    sweep_block(a1, b1, g1, w1, 1)
    sweep_block(b1, a1, g1, w1, 1)
    sweep_block(a1, b1, g1, w1, 1)
    residual_block(b1, r1, g1, s1, 1)
    source2 = pack_window(r1)
    v2 = sweep_window(2, [w2w[t] * source2[t] for t in range(4)], source2)
    source3 = halved_window(residual_window(2, v2, source2), 32)
    v3 = sweep_window(3, [w3w[t] * source3[t] for t in range(2)], source3)
    left3 = residual_window(3, v3, source3)
    left3 = 0.25 * (left3[0] + left3[1])
    place = lax.rem(gy, 8) * 16
    turns = lax.rem(place + lanes - 8, lanes), lax.rem(place + lanes + half - 8, lanes)
    lane_c = iota((4, lanes), 1)
    upper, lower = (
        pltpu.roll(left3[at : at + 4], turns[0], 1) + pltpu.roll(left3[at : at + 4], turns[1], 1) for at in (4, 8)
    )
    after = (lane_c + lanes - place) % lanes
    cbuf[me] = jnp.where(after < 16, upper, jnp.where((after >= half) & (after < half + 16), lower, 0.0))
    each(total, coarse_send)
    line_sent(0)
    gather_sent(1)
    for n, (dx, dy, source, target) in enumerate(sends):
        @pl.when(inside(dx, dy))
        def _():
            halo_copy(n, dx, dy, source, target).wait_send()
    for n, (dx, _, _) in enumerate(row_moves):
        @pl.when(inside(dx, 0))
        def _():
            row_copy(n, dx).wait_send()
    coarse_wait(1)
    for x in range(gx_count):
        for u in range(gy_count // 8):
            first = x * gy_count + u * 8
            left, right = (
                (cbuf[k] + cbuf[k + 1]) + (cbuf[k + 2] + cbuf[k + 3]) for k in (first, first + 4)
            )
            at = slice(u * lanes, (u + 1) * lanes)
            g4[0, x * 8 : x * 8 + 4, at] = jnp.where(lane_c < half, left, right)
            g4[0, x * 8 + 4 : x * 8 + 8, at] = pltpu.roll(jnp.where(lane_c < half, right, left), half, 1)
    e = coarse()
    e = e[0, pl.ds(pl.multiple_of(gx * 8, 8), 24), :][4 : 4 + window]
    near_e, far_e = (
        pltpu.roll(e, lax.rem(2 * q_count + 8 + k - gy * 16, q_count), 1)[:, 0:lanes] for k in (0, half)
    )
    e = jnp.where(in_domain(half), jnp.where(lane_w < half, near_e, far_e), 0.0)
    v3 = [v3[t] + e for t in range(2)]
    v3 = sweep_window(3, sweep_window(3, v3, source3), source3)
    e = [v3[t] + pltpu.roll(v3[t], 32, 1) for t in range(2)]
    v2 = [v2[t] + e[t // 2] for t in range(4)]
    v2 = sweep_window(2, sweep_window(2, v2, source2), source2)
    raised = exact_dot(jnp.concatenate(v2, 0), up_w[...])
    for t in range(4):
        put_window(t, raised[t * window : (t + 1) * window])
    near_w = (base_w - 8, base_w + half_rows + 8)
    around_w = slice(near_w[0] - 8, near_w[1] + 8)
    b1[around_w, :] = b1[around_w, :] + get_strips(r1, around_w)
    sweep_block(b1, a1, g1, w1, 1, near_w)
    sweep_block(a1, b1, g1, w1, 1, near_w)
    raised = exact_dot(b1[slice(*near_w), :], up0[...])
    put_strips(fine_add, pl.ds(0, ext1, 2), raised)
    put_strips(fine_add, pl.ds(1, ext1, 2), raised)
    for lo in range(ROWS_PAD, ext - ROWS_PAD, 8):
        at = slice(lo, lo + 8)
        vB[at, :] = vB[at, :] + get_strips(fine_add, at)
    sweep_block(vB, vA, gE, wE, 0)
    sweep_block(vA, vB, gE, wE, 0)
    for lo in range(0, rows, 8):
        mid, beside = around(vB, base + lo, 8)
        at = slice(base + lo, base + lo + 8)
        left = gE[at, :] - ((4.0 * mid - beside) + sE[at, :] * mid)
        out_ref[0, lo : lo + 8, :] = mid[:, 0:cols]
        out_ref[1, lo : lo + 8, :] = left[:, 0:cols]

    coarse_wait(0)


def solution(mesh):
    gx_count, gy_count = mesh.shape["gx"], mesh.shape["gy"]
    total = gx_count * gy_count

    def body(right_side, shift):
        rows, cols = right_side.shape
        assert cols == 256 and rows == 128 and gy_count % 8 == 0 and gy_count & (gy_count - 1) == 0
        ext, width = rows + 2 * (HALO + ROWS_PAD), cols + 128
        ext1, width1 = ext // 2 + 2 * ROWS_PAD, 256
        wide1 = rows // 2 + 2 * (ROW_HALO + ROWS_PAD)
        window = rows // 16 + 8
        p, q = rows // 16 * gx_count, cols // 16 * gy_count
        V = pltpu.VMEM
        dma = pltpu.SemaphoreType.DMA
        big = [V((ext, width), F32)] * 5 + [V((width // 128, ext, 128), F32)]
        one = [V((ext1, width1), F32)] * 5
        one += [V((wide1, width1), F32)] * 5 + [V((width1 // 128, wide1, 128), F32)]
        levels = []
        for n in (16, 4, 1):
            levels += [V((n, p, q), F32)] * 3 + [V((n, p + 16, q), F32)] * (2 if n > 1 else 1)
        scratch = (
            [V((rows, cols), F32)] * 2 + [dma((2,))]
            + big + one
            + [V((rows, 128), F32)] * 2 + [V((ext, 128), F32)] * 2
            + [V((width, width1), BF16), V((width1, width), BF16), V((width1, 128), BF16), V((4 * q, width1), BF16)]
            + [V((width1, 128), BF16), V((128, width1), BF16)]
            + [V((2, total, 16, 128), F32), V((total, 4, 128), F32)]
            + levels
            + [V((4, 24, width1), F32)]
            + [V((4, window, 128), F32)] * 2 + [V((2, window, 128), F32)] * 2
            + [V((5, p, q), F32), V((2, p, q), F32), V((20, p + 16, q), F32)]
            + [dma((10,)), dma((10,)), dma((4,)), dma((4,)), dma((2, total)), dma((2, total)), dma((2,))]
            + [pltpu.SemaphoreType.REGULAR((gy_count.bit_length() - 1,))]
        )
        out = pltpu.VMEM((2,) + right_side.shape, F32)
        both = pl.pallas_call(
            functools.partial(kernel, gx_count, gy_count),
            out_shape=out,
            in_specs=[pl.BlockSpec(memory_space=pltpu.HBM)] * 2,
            out_specs=pl.BlockSpec(memory_space=pltpu.VMEM),
            scratch_shapes=scratch,
            compiler_params=pltpu.CompilerParams(
                collective_id=0, has_side_effects=True, vmem_limit_bytes=60*1024*1024
            ),
        )(right_side, shift)
        return both[0], both[1]

    spec = P("gx", "gy")
    return jax.shard_map(body, mesh=mesh, in_specs=(spec, spec), out_specs=(spec, spec), check_vma=False)
```

```python
import functools

import jax
import jax.numpy as jnp
from jax import lax
from jax.experimental import pallas as pl
from jax.experimental.pallas import tpu as pltpu
from jax.sharding import PartitionSpec as P

DAMPING = 0.8
MESH = pl.DeviceIdType.MESH
F32 = jnp.float32
BF16 = jnp.bfloat16

ROWS_PAD = 8
HALO = 8
ROW_HALO = 32


def iota(shape, dim):
    return lax.broadcasted_iota(jnp.int32, shape, dim)


def put_strips(ref, at, values):
    for k in range(ref.shape[0]):
        ref[k, at, :] = values[:, k * 128 : (k + 1) * 128]


def get_strips(ref, at, count=None):
    return jnp.concatenate([ref[k, at, :] for k in range(count or ref.shape[0])], 1)


def exact_dot(values, selector):
    first = values.astype(BF16)
    rest = values - first.astype(F32)
    second = rest.astype(BF16)
    third = (rest - second.astype(F32)).astype(BF16)
    dot = functools.partial(jnp.dot, preferred_element_type=F32)
    return dot(first, selector) + (dot(second, selector) + dot(third, selector))


def kernel(
    gx_count, gy_count, g_hbm, s_hbm, out_ref,
    g_ref, s_ref, load_sem,
    gE, sE, wE, vA, vB, fine_add,
    gP, sP, wP, aP, bP,
    g1, s1, w1, a1, b1, r1,
    send_l, send_r, recv_l, recv_r,
    down0, up0, down1, spread, down_w, up_w,
    rbuf, cbuf, s2, w2, g2, a2, b2, s3, w3, g3, a3, b3, s4, w4, g4, a4, picked,
    s2w, w2w, s3w, w3w, hw4, phi, beside4,
    halo_send, halo_recv, row_send, row_recv, all_send, all_recv, coarse_sems, told,
):
    gx, gy = lax.axis_index("gx"), lax.axis_index("gy")
    total = gx_count * gy_count
    me = gx * gy_count + gy
    rows, cols = g_hbm.shape
    base = ROWS_PAD + HALO
    base1 = ROWS_PAD + (ROWS_PAD + HALO) // 2
    ext, width = gE.shape
    ext1, width1 = ext // 2, g1.shape[1]
    half_rows = rows // 2
    base_w = ROWS_PAD + ROW_HALO
    near1 = slice(ROWS_PAD, ROWS_PAD + ext1)
    wide1 = slice(ROWS_PAD, base_w + half_rows + ROW_HALO)
    lanes = 128

    load_g = pltpu.make_async_copy(g_hbm, g_ref, load_sem.at[0])
    load_s = pltpu.make_async_copy(s_hbm, s_ref, load_sem.at[1])
    load_g.start()
    load_s.start()
    zero_halo = jnp.zeros((base, width), F32)
    for ref in (gE, sE):
        ref[0:base, :] = zero_halo
        ref[base + rows : ext, :] = zero_halo
    for ref in (recv_l, recv_r):
        ref[...] = jnp.zeros(ref.shape, F32)
    for ref in (g1, s1):
        ref[0:base_w, :] = jnp.zeros((base_w, width1), F32)
        ref[base_w + half_rows :, :] = jnp.zeros((base_w, width1), F32)
    def inside(dx, dy):
        ok = None
        for step, at, count in ((dx, gx, gx_count), (dy, gy, gy_count)):
            if step:
                here = (at > 0) if step < 0 else (at < count - 1)
                ok = here if ok is None else ok & here
        return ok

    def wrap(at, step, count):
        return lax.rem(at + count + step, count)

    def each(count, body):
        if count <= 64:
            for j in range(1, count):
                body(j)
        else:
            pl.loop(1, count)(body)

    barrier = pltpu.get_barrier_semaphore()
    corners = [(dx, dy) for dx in (-1, 1) for dy in (-1, 1)]

    def greet(x, y):
        pl.semaphore_signal(barrier, inc=1, device_id=(x, y), device_id_type=MESH)

    each(gx_count, lambda k: greet(wrap(gx, k, gx_count), gy))
    for dx, dy in corners:
        @pl.when(inside(dx, dy))
        def _():
            greet(gx + dx, gy + dy)

    bits = [1 << b for b in range(1, gy_count.bit_length() - 1)] + [1]

    def flip(bit):
        return gy + bit * (1 - 2 * lax.rem(gy // bit, 2))

    for bit in bits[:-1]:
        greet(gx, flip(bit))
    for dy in (-1, 1):
        @pl.when(inside(0, dy))
        def _():
            greet(gx, gy + dy)


    lane = iota((rows, lanes), 1)
    half = lanes // 2
    l0 = iota((width, width1), 0)
    col0 = jnp.where(l0 < cols + half, l0, l0 - width)
    down0[...] = jnp.where(
        ((col0 + 2 * width1) // 2) % width1 == iota((width, width1), 1), 1.0, 0.0
    ).astype(BF16)
    l0 = iota((width1, width), 1)
    col0 = jnp.where(l0 < cols + half, l0, l0 - width)
    up0[...] = jnp.where(
        ((col0 + 2 * width1) // 2) % width1 == iota((width1, width), 0), 1.0, 0.0
    ).astype(BF16)
    l1 = iota((width1, lanes), 0)
    j2 = l1 // 2
    place = ((j2 + gy) % 4) * 16 + j2 // 4
    down1[...] = jnp.where(
        (l1 < lanes) & (iota((width1, lanes), 1) % half == place), 1.0, 0.0
    ).astype(BF16)
    q_count = s2.shape[2]
    p_count = s2.shape[1]
    m1 = iota((q_count, width1), 1)
    col1 = jnp.where(m1 < lanes + half // 2, m1, m1 - width1)
    wide = gy * half + (col1 + 512) // 2 - 256
    for r in range(4):
        spread[r * q_count : (r + 1) * q_count, :] = jnp.where(
            wide == 4 * iota((q_count, width1), 0) + r, 1.0, 0.0
        ).astype(BF16)

    load_g.wait()
    load_s.wait()
    send_l[...] = jnp.where(lane < half, g_ref[:, 0:lanes], pltpu.roll(s_ref[:, 0:lanes], half, 1))
    send_r[...] = jnp.where(
        lane < half, pltpu.roll(s_ref[:, cols - lanes : cols], half, 1), g_ref[:, cols - lanes : cols]
    )

    l1 = iota((width1, lanes), 0)
    at2 = (jnp.where(l1 < lanes + half // 2, l1, l1 - width1) + 2 * lanes) // 2
    at4 = at2 // 4 - 24
    down_w[...] = jnp.where(
        (at4 >= 0) & (at4 < 32) & (iota((width1, lanes), 1) == (at2 % 4) * 32 + at4), 1.0, 0.0
    ).astype(BF16)
    l1 = iota((lanes, width1), 1)
    at2 = (jnp.where(l1 < lanes + half // 2, l1, l1 - width1) + 2 * lanes) // 2
    at4 = at2 // 4 - 24
    up_w[...] = jnp.where(
        (at4 >= 0) & (at4 < 32) & (iota((lanes, width1), 0) == (at2 % 4) * 32 + at4), 1.0, 0.0
    ).astype(BF16)

    def pack_level2(source):
        parts = []
        for t in range(4):
            start = base1 + 2 * t
            parts.append(
                get_strips(source, pl.ds(start, 8, 8)) + get_strips(source, pl.ds(start + 1, 8, 8))
            )
        means = 0.25 * exact_dot(jnp.concatenate(parts, 0), down1[...])
        low = (iota((16, lanes), 1) // 16 + 8 - lax.rem(gy, 8)) % 8 < 4
        return jnp.where(low, means[0:16], means[16:32])

    def beside_count(at, count):
        return (at + count - 1) // count + 1 - (at + 1) // count

    pl.semaphore_wait(
        barrier,
        gx_count + len(bits) - 2 + beside_count(gy, gy_count) * (1 + beside_count(gx, gx_count)),
    )

    def tell(n):
        pl.semaphore_signal(told.at[n], inc=1, device_id=(gx, flip(bits[n])), device_id_type=MESH)

    tell(0)

    top, bottom = slice(0, HALO), slice(rows - HALO, rows)
    above, below = slice(ROWS_PAD, base), slice(base + rows, base + rows + HALO)
    middle = slice(base, base + rows)
    sends = (
        (-1, -1, send_l.at[top, :], recv_r.at[below, :]),
        (1, -1, send_l.at[bottom, :], recv_r.at[above, :]),
        (-1, 1, send_r.at[top, :], recv_l.at[below, :]),
        (1, 1, send_r.at[bottom, :], recv_l.at[above, :]),
        (-1, 0, g_ref.at[top, :], gE.at[below, 0:cols]),
        (-1, 0, s_ref.at[top, :], sE.at[below, 0:cols]),
        (1, 0, g_ref.at[bottom, :], gE.at[above, 0:cols]),
        (1, 0, s_ref.at[bottom, :], sE.at[above, 0:cols]),
        (0, -1, send_l, recv_r.at[middle, :]),
        (0, 1, send_r, recv_l.at[middle, :]),
    )

    def halo_copy(n, dx, dy, source, target):
        return pltpu.make_async_remote_copy(
            src_ref=source, dst_ref=target, send_sem=halo_send.at[n], recv_sem=halo_recv.at[n],
            device_id=(gx + dx, gy + dy), device_id_type=MESH,
        )

    for n, (dx, dy, source, target) in enumerate(sends):
        @pl.when(inside(dx, dy))
        def _():
            halo_copy(n, dx, dy, source, target).start()

    core = lax.rem(gy, 2)
    per_row = gy_count // 2
    chips = total // 2
    partner = (gx, gy + 1 - 2 * core)

    def zigzag(j, count):
        if total <= 64:
            width_of = count // gx_count
            lines = [0] + sorted(range(1, gx_count), key=lambda d: -abs(2 * d - gx_count))
            return lines[j // width_of] * width_of + j % width_of
        odd = j % 2
        return odd * ((j + 1) // 2) + (1 - odd) * (count - j // 2)

    def block_copy(turn, n, slot, peer):
        return pltpu.make_async_remote_copy(
            src_ref=rbuf.at[turn, slot], dst_ref=rbuf.at[turn, slot],
            send_sem=all_send.at[turn, n], recv_sem=all_recv.at[turn, slot],
            device_id=peer, device_id_type=MESH,
        )

    def direct(turn, j):
        n = zigzag(j, chips)
        peer = (wrap(gx, n // per_row, gx_count), wrap(gy, 2 * (n % per_row), gy_count))
        return block_copy(turn, j, me, peer)

    def sender(j):
        n = zigzag(j, chips)
        return wrap(gx, -(n // per_row), gx_count) * gy_count + wrap(gy, -2 * (n % per_row), gy_count)

    def onward(turn, j):
        return block_copy(turn, chips + j, sender(j), partner)

    def gather_start(turn):
        block_copy(turn, 0, me, partner).start()
        each(chips, lambda j: direct(turn, chips - j).start())

    def gather_wait(turn):
        def pass_block(j):
            copy = onward(turn, j)
            copy.wait_recv()
            copy.start()

        each(chips, pass_block)
        block_copy(turn, 0, me + 1 - 2 * core, partner).wait_recv()
        each(chips, lambda j: block_copy(turn, chips + j, sender(j) + 1 - 2 * core, partner).wait_recv())

    def gather_sent(turn):
        def sent(j):
            direct(turn, j).wait_send()
            onward(turn, j).wait_send()

        block_copy(turn, 0, me, partner).wait_send()
        each(chips, sent)

    def slot_of(d, j):
        return wrap(gx, -d, gx_count) * gy_count + wrap(gy, -2 * j, gy_count)

    def each_block(first_d, first_j, body):
        if total <= 64:
            for d in range(first_d, gx_count):
                for j in range(first_j, per_row):
                    body(d, j)
        else:
            pl.loop(first_d, gx_count)(lambda d: pl.loop(first_j, per_row)(lambda j: body(d, j)))

    def along_line(turn, d):
        return block_copy(turn, d, me, (wrap(gx, d, gx_count), gy))

    def across(turn, d, j):
        n = gx_count + d * (per_row - 1) + j - 1
        return block_copy(turn, n, slot_of(d, 0), (gx, wrap(gy, 2 * j, gy_count)))

    def to_partner(turn, d, j):
        return block_copy(turn, chips + d * per_row + j, slot_of(d, j), partner)

    def from_partner(turn, d, j):
        return block_copy(turn, 0, slot_of(d, j) + 1 - 2 * core, partner)

    def line_start(turn):
        block_copy(turn, 0, me, partner).start()
        each(gx_count, lambda d: along_line(turn, gx_count - d).start())

    def line_pass(turn):
        def pass_line(d):
            block_copy(turn, 0, slot_of(d, 0), partner).wait_recv()
            each(per_row, lambda j: across(turn, d, per_row - j).start())
            to_partner(turn, d, 0).start()

        each(gx_count, pass_line)

    def line_wait(turn):
        def pass_block(d, j):
            copy = to_partner(turn, d, j)
            copy.wait_recv()
            copy.start()

        each_block(0, 1, pass_block)
        each_block(0, 0, lambda d, j: from_partner(turn, d, j).wait_recv())

    def line_sent(turn):
        block_copy(turn, 0, me, partner).wait_send()
        each(gx_count, lambda d: along_line(turn, d).wait_send())
        each_block(0, 1, lambda d, j: across(turn, d, j).wait_send())
        each_block(1, 0, lambda d, j: to_partner(turn, d, j).wait_send())
        each(per_row, lambda j: to_partner(turn, 0, j).wait_send())

    gE[base : base + rows, 0:cols] = g_ref[...]
    sE[base : base + rows, 0:cols] = s_ref[...]

    own_strips = cols // lanes
    for k in range(own_strips):
        fine_add[k, base : base + rows, :] = s_ref[:, k * lanes : (k + 1) * lanes]
    own = get_strips(fine_add, pl.ds(base, half_rows, 2), own_strips)
    own = own + get_strips(fine_add, pl.ds(base + 1, half_rows, 2), own_strips)
    put_strips(r1, slice(base1, base1 + half_rows), 0.25 * exact_dot(own, down0[0:cols, :]))
    rbuf[0, me] = pack_level2(r1)
    line_start(0)
    for n in range(len(bits)):
        pl.semaphore_wait(told.at[n], 1)
        if n < len(bits) - 1:
            tell(n + 1)
    each(per_row, lambda j: across(0, 0, per_row - j).start())
    zero_tile = jnp.zeros((ROWS_PAD, width), F32)
    for ref in (vA, vB):
        ref[0:ROWS_PAD, :] = zero_tile
        ref[ext - ROWS_PAD : ext, :] = zero_tile
    for ref in (aP, bP, a1, b1):
        ref[0:ROWS_PAD, :] = jnp.zeros((ROWS_PAD, width1), F32)
        ref[ref.shape[0] - ROWS_PAD :, :] = jnp.zeros((ROWS_PAD, width1), F32)
    for ref in (a2, b2, a3, b3, a4):
        for i in range(ref.shape[0]):
            ref[i, 0:8, :] = jnp.zeros((8, q_count), F32)
            ref[i, 8 + p_count : 16 + p_count, :] = jnp.zeros((8, q_count), F32)

    for n, (dx, dy, source, target) in enumerate(sends):
        @pl.when(inside(-dx, -dy))
        def _():
            halo_copy(n, -dx, -dy, source, target).wait_recv()

    lane_e = iota((ext, lanes), 1)
    gE[:, cols:width] = jnp.where(lane_e < half, recv_r[...], recv_l[...])
    sE[:, cols:width] = pltpu.roll(jnp.where(lane_e < half, recv_l[...], recv_r[...]), half, 1)

    def weight(shifts, first_row, own_rows, own_cols, split, level):
        shape = shifts.shape
        at_row = gx * own_rows + iota(shape, 0) + first_row
        lane_at = iota(shape, 1)
        at_col = gy * own_cols + jnp.where(lane_at < own_cols + split, lane_at, lane_at - shape[1])
        good = (at_row >= 0) & (at_row < gx_count * own_rows)
        good = good & (at_col >= 0) & (at_col < gy_count * own_cols)
        return jnp.where(good, DAMPING / (4.0 ** (1 - level) + shifts), 0.0)

    def around(v, lo, size):
        span = v.shape[1]
        mid = v[lo : lo + size, :]
        beside = pltpu.roll(mid, 1, 1) + pltpu.roll(mid, span - 1, 1)
        return mid, beside + (v[lo - 1 : lo - 1 + size, :] + v[lo + 1 : lo + 1 + size, :])

    def sweep_block(v, out, g, w, level, span=None):
        scale = 4.0 ** (-level)
        for lo in range(*(span or (ROWS_PAD, v.shape[0] - ROWS_PAD)), 8):
            mid, beside = around(v, lo, 8)
            at = slice(lo, lo + 8)
            out[at, :] = (1.0 - DAMPING) * mid + w[at, :] * (g[at, :] + scale * beside)

    def residual_block(v, out, g, s, level, span=None):
        scale = 4.0 ** (-level)
        for lo in range(*(span or (ROWS_PAD, v.shape[0] - ROWS_PAD)), 8):
            mid, beside = around(v, lo, 8)
            at = slice(lo, lo + 8)
            put_strips(out, at, g[at, :] - (scale * (4.0 * mid - beside) + s[at, :] * mid))

    row_moves = (
        (-1, sP.at[base1 : base1 + ROW_HALO, :], s1.at[base_w + half_rows : base_w + half_rows + ROW_HALO, :]),
        (1, sP.at[base1 + half_rows - ROW_HALO : base1 + half_rows, :], s1.at[ROWS_PAD:base_w, :]),
        (-1, gP.at[base1 : base1 + ROW_HALO, :], g1.at[base_w + half_rows : base_w + half_rows + ROW_HALO, :]),
        (1, gP.at[base1 + half_rows - ROW_HALO : base1 + half_rows, :], g1.at[ROWS_PAD:base_w, :]),
    )

    def row_copy(n, dx):
        _, source, target = row_moves[n]
        return pltpu.make_async_remote_copy(
            src_ref=source, dst_ref=target, send_sem=row_send.at[n], recv_sem=row_recv.at[n],
            device_id=(gx + dx, gy), device_id_type=MESH,
        )

    def rows_start(which):
        for n in which:
            dx = row_moves[n][0]
            @pl.when(inside(dx, 0))
            def _():
                row_copy(n, dx).start()

    def halved():
        pairs = get_strips(fine_add, pl.ds(0, ext1, 2)) + get_strips(fine_add, pl.ds(1, ext1, 2))
        return 0.25 * exact_dot(pairs, down0[...])

    put_strips(fine_add, slice(0, ext), sE[...])
    sP[near1, :] = halved()
    rows_start((0, 1))
    chunk = 16
    for lo in range(0, ext, chunk):
        at = slice(lo, lo + chunk)
        wE[at, :] = weight(sE[at, :], lo - base, rows, cols, half, 0)
    for lo in range(ROWS_PAD, ext - ROWS_PAD, 8):
        at = slice(lo, lo + 8)
        vA[at, :] = wE[at, :] * gE[at, :]
    sweep_block(vA, vB, gE, wE, 0)
    put_strips(fine_add, slice(0, ROWS_PAD), zero_tile)
    put_strips(fine_add, slice(ext - ROWS_PAD, ext), zero_tile)
    residual_block(vB, fine_add, gE, sE, 0)
    gP[near1, :] = halved()
    wP[near1, :] = weight(sP[near1, :], ROWS_PAD - base1, half_rows, cols // 2, half // 2, 1)
    aP[near1, :] = wP[near1, :] * gP[near1, :]
    sweep_block(aP, bP, gP, wP, 1)
    residual_block(bP, r1, gP, sP, 1, (base1, base1 + half_rows))
    rbuf[1, me] = pack_level2(r1)
    gather_start(1)
    line_pass(0)

    block = (lane_e[0:8] // 16)

    def unpack(turn, target):
        for x in range(gx_count):
            for u in range(gy_count // 8):
                for tl in range(2):
                    tiles = [rbuf[turn, x * gy_count + u * 8 + g, tl * 8 : tl * 8 + 8, :] for g in range(8)]
                    tiles = [tiles[-b % 8] for b in range(8)]
                    for bit in (1, 2, 4):
                        keep = (block & bit) == 0
                        tiles = [jnp.where(keep, tiles[b], tiles[(b - bit) % 8]) for b in range(8)]
                    for b in range(8):
                        t, r = (b // 4) * 2 + tl, b % 4
                        target[t * 4 + r, 8 * x : 8 * x + 8, u * lanes : (u + 1) * lanes] = pltpu.roll(
                            tiles[b], (lanes - 16 * b) % lanes, 1
                        )

    lane_q = iota((p_count, q_count), 1)
    rows_q = slice(8, 8 + p_count)

    def sides(v, n, t, r):
        mid = v[t * n + r, rows_q, :]
        if t > 0:
            north = v[(t - 1) * n + r, rows_q, :]
        else:
            north = v[(n - 1) * n + r, 7 : 7 + p_count, :]
        if t < n - 1:
            south = v[(t + 1) * n + r, rows_q, :]
        else:
            south = v[r, 9 : 9 + p_count, :]
        if r > 0:
            west = v[t * n + r - 1, rows_q, :]
        else:
            west = jnp.where(lane_q == 0, 0.0, pltpu.roll(v[t * n + n - 1, rows_q, :], 1, 1))
        if r < n - 1:
            east = v[t * n + r + 1, rows_q, :]
        else:
            east = jnp.where(
                lane_q == q_count - 1, 0.0, pltpu.roll(v[t * n, rows_q, :], q_count - 1, 1)
            )
        return mid, (north + south) + (west + east)

    level_refs = {2: (s2, w2, g2, a2, b2, 4), 3: (s3, w3, g3, a3, b3, 2), 4: (s4, w4, g4, a4, None, 1)}

    def sweep(level, v, out):
        s, w, g, _, _, n = level_refs[level]
        for t in range(n):
            for r in range(n):
                i = t * n + r
                mid, beside = sides(v, n, t, r)
                out[i, rows_q, :] = (1.0 - DAMPING) * mid + w[i] * (g[i] + 4.0 ** (-level) * beside)

    def first_sweep(level, out):
        s, w, g, _, _, n = level_refs[level]
        for i in range(n * n):
            out[i, rows_q, :] = w[i] * g[i]

    def restricted(level, v):
        s, w, g, _, _, n = level_refs[level]
        coarse_g = level_refs[level + 1][2]
        for t in range(n // 2):
            for r in range(n // 2):
                sums = None
                for dt in range(2):
                    for dr in range(2):
                        i = (2 * t + dt) * n + 2 * r + dr
                        mid, beside = sides(v, n, 2 * t + dt, 2 * r + dr)
                        left = g[i] - (4.0 ** (-level) * (4.0 * mid - beside) + s[i] * mid)
                        sums = left if sums is None else sums + left
                coarse_g[t * (n // 2) + r] = 0.25 * sums

    def correct(level, v, e):
        n = level_refs[level][5]
        for t in range(n):
            for r in range(n):
                i = t * n + r
                v[i, rows_q, :] = v[i, rows_q, :] + e[(t // 2) * (n // 2) + r // 2, rows_q, :]

    def prepare(level):
        s, w, _, _, _, n = level_refs[level]
        for i in range(n * n):
            w[i] = DAMPING / (4.0 ** (1 - level) + s[i])
        if level < 4:
            coarse_s = level_refs[level + 1][0]
            m = n // 2
            for t in range(m):
                for r in range(m):
                    i = 2 * t * n + 2 * r
                    coarse_s[t * m + r] = 0.25 * ((s[i] + s[i + n]) + (s[i + 1] + s[i + n + 1]))

    def total_of(x):
        return jnp.sum(jnp.sum(x, axis=0, keepdims=True), axis=1, keepdims=True)

    window = picked.shape[1] - 8
    lane_w, row_w = iota((window, lanes), 1), iota((window, lanes), 0)

    def in_domain(period):
        at_p, at_q = gx * 8 - 4 + row_w, gy * 16 - 8 + lane_w % period
        good = (at_p >= 0) & (at_p < p_count) & (at_q >= 0) & (at_q < q_count)
        return good & (lane_w % period < 32)

    def put_window(t, values):
        for a in range(2):
            put_strips(r1, pl.ds(ROWS_PAD + 2 * t + a, window, 8), values)

    def add_level2(e, v):
        for t in range(4):
            tiles = [e[t * 4 + r, pl.ds(pl.multiple_of(gx * 8, 8), 24), :] for r in range(4)]
            picked[t] = exact_dot(jnp.concatenate(tiles, 1), spread[...])
        for t in range(4):
            put_window(t, picked[t, 4 : 4 + window, :])
        v[wide1, :] = v[wide1, :] + get_strips(r1, wide1)

    def pack_window(source):
        parts = []
        for t in range(4):
            start = ROWS_PAD + 2 * t
            parts.append(
                get_strips(source, pl.ds(start, window, 8)) + get_strips(source, pl.ds(start + 1, window, 8))
            )
        means = 0.25 * exact_dot(jnp.concatenate(parts, 0), down_w[...])
        return [means[t * window : (t + 1) * window] for t in range(4)]

    def joined(x, unit):
        return x + pltpu.roll(x, lanes - unit, 1)

    def halved_window(tiles, unit):
        return [0.25 * joined(tiles[2 * t] + tiles[2 * t + 1], unit) for t in range(len(tiles) // 2)]

    def beside_window(v, unit):
        n = len(v)
        out = []
        for t in range(n):
            north = v[t - 1] if t > 0 else pltpu.roll(v[n - 1], 1, 0)
            south = v[t + 1] if t < n - 1 else pltpu.roll(v[0], window - 1, 0)
            west = jnp.where(lane_w < unit, pltpu.roll(v[t], unit + 1, 1), pltpu.roll(v[t], unit, 1))
            east = jnp.where(
                lane_w >= lanes - unit,
                pltpu.roll(v[t], lanes - unit - 1, 1), pltpu.roll(v[t], lanes - unit, 1),
            )
            out.append((north + south) + (west + east))
        return out

    window_refs = {2: (s2w, w2w, 32), 3: (s3w, w3w, 64)}

    def sweep_window(level, v, g):
        _, w, unit = window_refs[level]
        beside = beside_window(v, unit)
        return [
            (1.0 - DAMPING) * v[t] + w[t] * (g[t] + 4.0 ** (-level) * beside[t]) for t in range(len(v))
        ]

    def residual_window(level, v, g):
        s, _, unit = window_refs[level]
        beside = beside_window(v, unit)
        return [
            g[t] - (4.0 ** (-level) * (4.0 * v[t] - beside[t]) + s[t] * v[t]) for t in range(len(v))
        ]

    def rows_wait(which):
        for n in which:
            dx = row_moves[n][0]
            @pl.when(inside(-dx, 0))
            def _():
                row_copy(n, -dx).wait_recv()

    own1, own_w = slice(base1, base1 + half_rows), slice(base_w, base_w + half_rows)
    rows_wait((0, 1))
    s1[own_w, :] = sP[own1, :]
    w1[wide1, :] = weight(s1[wide1, :], ROWS_PAD - base_w, half_rows, cols // 2, half // 2, 1)
    put_strips(r1, wide1, s1[wide1, :])
    tiles = pack_window(r1)
    for t in range(4):
        s2w[t] = tiles[t]
        w2w[t] = jnp.where(in_domain(32), DAMPING / (4.0 ** (-1) + tiles[t]), 0.0)
    tiles = halved_window(tiles, 32)
    for t in range(2):
        s3w[t] = tiles[t]
        w3w[t] = jnp.where(in_domain(64), DAMPING / (4.0 ** (-2) + tiles[t]), 0.0)

    line_wait(0)
    unpack(0, s2)
    for level in (2, 3, 4):
        prepare(level)
    row_q = iota((p_count, q_count), 0)
    edges = jnp.where(row_q == 0, 1.0, 0.0) + jnp.where(row_q == p_count - 1, 1.0, 0.0)
    edges = edges + jnp.where(lane_q == 0, 1.0, 0.0) + jnp.where(lane_q == q_count - 1, 1.0, 0.0)
    unit4 = 4.0 ** (-4) * edges + s4[0]
    per_unit = 1.0 / total_of(unit4)

    def shifted(x, reach):
        out = {0: x}
        for k in range(1, reach + 1):
            out[k] = jnp.where(lane_q < q_count - k, pltpu.roll(x, q_count - k, 1), 0.0)
            out[-k] = jnp.where(lane_q >= k, pltpu.roll(x, k, 1), 0.0)
        return out

    reach4 = 2
    for k, values in shifted(4.0 ** (-4) * w4[0], reach4).items():
        hw4[k + reach4] = values
    for i in range(beside4.shape[0]):
        beside4[i, 0:8, :] = jnp.zeros((8, q_count), F32)
        beside4[i, 8 + p_count : 16 + p_count, :] = jnp.zeros((8, q_count), F32)

    def fused_sweeps(v, source, count, first_slot=0):
        for turn in range(count):
            reach = count - 1 - turn
            new = {}
            for k in range(-reach, reach + 1):
                slot = first_slot + (turn % 2) * 5 + k + reach4
                beside4[slot, rows_q, :] = v[k]
                along = beside4[slot, 7 : 7 + p_count, :] + beside4[slot, 9 : 9 + p_count, :]
                value = (1.0 - DAMPING) * v[k] + hw4[k + reach4] * ((v[k - 1] + v[k + 1]) + along)
                new[k] = value if source is None else value + source[k]
            v = new
        return v[0]

    def six_sweeps(v, source, first_slot=0):
        v = fused_sweeps(shifted(v, 3), source, 3, first_slot)
        return fused_sweeps(shifted(v, 3), source, 3, first_slot)

    def coarse(twice=False):
        source = shifted(w4[0] * g4[0], 3)
        v = fused_sweeps(source, source, 3)
        v = fused_sweeps(shifted(v, 2), source, 2)
        add = total_of(g4[0]) * per_unit
        if twice:
            phi[0] = six_sweeps(jnp.ones((p_count, q_count), F32), None, 10)
            phi[1] = six_sweeps(phi[0], None, 10)
            kept = 1.0 - per_unit * total_of(unit4 * phi[0])
            again = add * kept - total_of(unit4 * v) * per_unit
            v = six_sweeps(v, source) + add * phi[1] + again * phi[0]
        else:
            v = v + add * phi[0]
        a4[0, rows_q, :] = v
        return a4

    def vcycle(level, v):
        if level == 4:
            return coarse()
        _, _, _, a, b, n = level_refs[level]
        if v is None:
            first_sweep(level, a)
            sweep(level, a, b)
            now, later = b, a
        else:
            later = b if v is a else a
            sweep(level, v, later)
            sweep(level, later, v)
            now = v
        restricted(level, now)
        correct(level, now, vcycle(level + 1, None))
        sweep(level, now, later)
        sweep(level, later, now)
        return now

    def fcycle(level):
        _, _, _, a, b, n = level_refs[level]
        first_sweep(level, a)
        sweep(level, a, b)
        restricted(level, b)
        if level == 3:
            e = coarse(True)
        else:
            e = vcycle(level + 1, fcycle(level + 1))
        correct(level, b, e)
        sweep(level, b, a)
        sweep(level, a, b)
        return b

    def coarse_send(k):
        n = zigzag(total - k, total)
        pltpu.make_async_remote_copy(
            src_ref=cbuf.at[me], dst_ref=cbuf.at[me], send_sem=coarse_sems.at[0], recv_sem=coarse_sems.at[1],
            device_id=(wrap(gx, n // gy_count, gx_count), wrap(gy, n % gy_count, gy_count)), device_id_type=MESH,
        ).start()

    def coarse_wait(n):
        others = cbuf.at[pl.ds(0, total - 1)]
        pltpu.make_async_copy(others, others, coarse_sems.at[n]).wait()

    gather_wait(1)
    rows_start((2, 3))
    unpack(1, g2)
    e = fcycle(2)
    e = vcycle(2, e)
    rows_wait((2, 3))
    g1[own_w, :] = gP[own1, :]
    a1[wide1, :] = w1[wide1, :] * g1[wide1, :]
    sweep_block(a1, b1, g1, w1, 1)
    add_level2(e, b1)
    sweep_block(b1, a1, g1, w1, 1)
    sweep_block(a1, b1, g1, w1, 1)
    sweep_block(b1, a1, g1, w1, 1)
    sweep_block(a1, b1, g1, w1, 1)
    residual_block(b1, r1, g1, s1, 1, (base_w - 24, base_w + half_rows + 24))
    source2 = pack_window(r1)
    v2 = sweep_window(2, [w2w[t] * source2[t] for t in range(4)], source2)
    source3 = halved_window(residual_window(2, v2, source2), 32)
    v3 = sweep_window(3, [w3w[t] * source3[t] for t in range(2)], source3)
    left3 = residual_window(3, v3, source3)
    left3 = 0.25 * (left3[0] + left3[1])
    place = lax.rem(gy, 8) * 16
    turns = lax.rem(place + lanes - 8, lanes), lax.rem(place + lanes + half - 8, lanes)
    lane_c = iota((4, lanes), 1)
    upper, lower = (
        pltpu.roll(left3[at : at + 4], turns[0], 1) + pltpu.roll(left3[at : at + 4], turns[1], 1) for at in (4, 8)
    )
    after = (lane_c + lanes - place) % lanes
    cbuf[me] = jnp.where(after < 16, upper, jnp.where((after >= half) & (after < half + 16), lower, 0.0))
    each(total, coarse_send)
    line_sent(0)
    gather_sent(1)
    for n, (dx, dy, source, target) in enumerate(sends):
        @pl.when(inside(dx, dy))
        def _():
            halo_copy(n, dx, dy, source, target).wait_send()
    for n, (dx, _, _) in enumerate(row_moves):
        @pl.when(inside(dx, 0))
        def _():
            row_copy(n, dx).wait_send()
    coarse_wait(1)
    for x in range(gx_count):
        for u in range(gy_count // 8):
            first = x * gy_count + u * 8
            left, right = (
                (cbuf[k] + cbuf[k + 1]) + (cbuf[k + 2] + cbuf[k + 3]) for k in (first, first + 4)
            )
            at = slice(u * lanes, (u + 1) * lanes)
            g4[0, x * 8 : x * 8 + 4, at] = jnp.where(lane_c < half, left, right)
            g4[0, x * 8 + 4 : x * 8 + 8, at] = pltpu.roll(jnp.where(lane_c < half, right, left), half, 1)
    e = coarse()
    e = e[0, pl.ds(pl.multiple_of(gx * 8, 8), 24), :][4 : 4 + window]
    near_e, far_e = (
        pltpu.roll(e, lax.rem(2 * q_count + 8 + k - gy * 16, q_count), 1)[:, 0:lanes] for k in (0, half)
    )
    e = jnp.where(in_domain(half), jnp.where(lane_w < half, near_e, far_e), 0.0)
    v3 = [v3[t] + e for t in range(2)]
    v3 = sweep_window(3, sweep_window(3, v3, source3), source3)
    e = [v3[t] + pltpu.roll(v3[t], 32, 1) for t in range(2)]
    v2 = [v2[t] + e[t // 2] for t in range(4)]
    v2 = sweep_window(2, sweep_window(2, v2, source2), source2)
    raised = exact_dot(jnp.concatenate(v2, 0), up_w[...])
    for t in range(4):
        put_window(t, raised[t * window : (t + 1) * window])
    near_w = (base_w - 8, base_w + half_rows + 8)
    around_w = slice(near_w[0] - 8, near_w[1] + 8)
    b1[around_w, :] = b1[around_w, :] + get_strips(r1, around_w)
    sweep_block(b1, a1, g1, w1, 1, near_w)
    sweep_block(a1, b1, g1, w1, 1, near_w)
    raised = exact_dot(b1[slice(*near_w), :], up0[...])
    put_strips(fine_add, pl.ds(0, ext1, 2), raised)
    put_strips(fine_add, pl.ds(1, ext1, 2), raised)
    for lo in range(ROWS_PAD, ext - ROWS_PAD, 8):
        at = slice(lo, lo + 8)
        vB[at, :] = vB[at, :] + get_strips(fine_add, at)
    sweep_block(vB, vA, gE, wE, 0)
    sweep_block(vA, vB, gE, wE, 0)
    for lo in range(0, rows, 8):
        mid, beside = around(vB, base + lo, 8)
        at = slice(base + lo, base + lo + 8)
        left = gE[at, :] - ((4.0 * mid - beside) + sE[at, :] * mid)
        out_ref[0, lo : lo + 8, :] = mid[:, 0:cols]
        out_ref[1, lo : lo + 8, :] = left[:, 0:cols]

    coarse_wait(0)


def solution(mesh):
    gx_count, gy_count = mesh.shape["gx"], mesh.shape["gy"]
    total = gx_count * gy_count

    def body(right_side, shift):
        rows, cols = right_side.shape
        assert cols == 256 and rows == 128 and gy_count % 8 == 0 and gy_count & (gy_count - 1) == 0
        ext, width = rows + 2 * (HALO + ROWS_PAD), cols + 128
        ext1, width1 = ext // 2 + 2 * ROWS_PAD, 256
        wide1 = rows // 2 + 2 * (ROW_HALO + ROWS_PAD)
        window = rows // 16 + 8
        p, q = rows // 16 * gx_count, cols // 16 * gy_count
        V = pltpu.VMEM
        dma = pltpu.SemaphoreType.DMA
        big = [V((ext, width), F32)] * 5 + [V((width // 128, ext, 128), F32)]
        one = [V((ext1, width1), F32)] * 5
        one += [V((wide1, width1), F32)] * 5 + [V((width1 // 128, wide1, 128), F32)]
        levels = []
        for n in (16, 4, 1):
            levels += [V((n, p, q), F32)] * 3 + [V((n, p + 16, q), F32)] * (2 if n > 1 else 1)
        scratch = (
            [V((rows, cols), F32)] * 2 + [dma((2,))]
            + big + one
            + [V((rows, 128), F32)] * 2 + [V((ext, 128), F32)] * 2
            + [V((width, width1), BF16), V((width1, width), BF16), V((width1, 128), BF16), V((4 * q, width1), BF16)]
            + [V((width1, 128), BF16), V((128, width1), BF16)]
            + [V((2, total, 16, 128), F32), V((total, 4, 128), F32)]
            + levels
            + [V((4, 24, width1), F32)]
            + [V((4, window, 128), F32)] * 2 + [V((2, window, 128), F32)] * 2
            + [V((5, p, q), F32), V((2, p, q), F32), V((20, p + 16, q), F32)]
            + [dma((10,)), dma((10,)), dma((4,)), dma((4,)), dma((2, total)), dma((2, total)), dma((2,))]
            + [pltpu.SemaphoreType.REGULAR((gy_count.bit_length() - 1,))]
        )
        out = pltpu.VMEM((2,) + right_side.shape, F32)
        both = pl.pallas_call(
            functools.partial(kernel, gx_count, gy_count),
            out_shape=out,
            in_specs=[pl.BlockSpec(memory_space=pltpu.HBM)] * 2,
            out_specs=pl.BlockSpec(memory_space=pltpu.VMEM),
            scratch_shapes=scratch,
            compiler_params=pltpu.CompilerParams(
                collective_id=0, has_side_effects=True, vmem_limit_bytes=60*1024*1024
            ),
        )(right_side, shift)
        return both[0], both[1]

    spec = P("gx", "gy")
    return jax.shard_map(body, mesh=mesh, in_specs=(spec, spec), out_specs=(spec, spec), check_vma=False)
```
